256 devices in a mesh: freq: 16 (over y_lo, x, core), base: 16 (over y_hi, z).
Axes of the slice: x: 4, y: 4 (y_hi: 2, y_lo: 2; y = y_hi * 2 + y_lo), z: 8, core: 2. Of those that a mesh axis runs over, the one named last changes fastest.
Arguments:
- visibility: float32 [2, 32, 8192], P(None, 'freq', 'base'), may hold values from -6 to 6
- tile_of: int32 [32, 8192, 1], P('freq', 'base'), may hold values from 0 to 15; in each aligned block of 512 rows (0 to 511, 512 to 1023, ..., all dimensions but the last counted through in order) at most 64 rows name the same one
- u_within: int32 [32, 8192], P('freq', 'base'), may hold values from 0 to 63
- v_cell: int32 [32, 8192], P('freq', 'base'), may hold values from 0 to 1016
- kernel_index: int32 [2, 32, 8192], P(None, 'freq', 'base'), may hold values from 0 to 127
- kernel: float32 [128, 8], replicated, may hold values from 0.1 to 1
- live_count: int32 [32, 16], P('freq', 'base'), may hold values from 64 to 512, as said below
- bin_map: int32 [1024, 1024], P('base'), may hold values from 0 to 511, as said below
Outputs:
- power_map: float32 [1024, 1024], P('freq', 'base')
- spectrum: float32 [512], replicated
The draws below stay inside these ranges and needn't reach their ends.
Inputs may be any that keep to these rules, and one draw needn't show every extreme that they name: `tile_of`: among the visibilities of one channel on one device, at most 64 name the same tile, and in some device's visibilities a tile is named by exactly 64. `live_count`: the first device along base holds 512 used slots in every channel; the used slots of a device are its first ones. `bin_map`: every bin number occurs.
All inputs are finite; a program needn't handle non-finite values.
Results may differ from the reference program's by a relative error of at most 0.0003.
Values sent between devices are 32-bit elements; how exact they have to be, the bound alone decides.
A program may use at most 128 MiB of HBM per device.

```python
import math
import jax
import jax.numpy as jnp
import numpy as np
from jax import lax

G = 1024
NBINS = 512
KW = 8
OVER = 128
VIS_DEV = 512
CH_DEV = 2
TILE = 64
CAP = 64
CH = 32
VIS = 8192
N_FREQ = 16
N_BASE = 16


def draw_visibility(key, part):
    channels = CH_DEV * N_FREQ
    visits = VIS_DEV * N_BASE
    frequency = 100.0 + 60.0 * jnp.arange(channels, dtype=jnp.float32) / max(channels - 1, 1)
    falloff = (frequency / 100.0) ** (-2.6)
    values = jnp.clip(jax.random.normal(key, (2, channels, visits), jnp.float32), -6.0, 6.0)
    return values * falloff[None, :, None]


def draw_live_count(key, part):
    channels = CH_DEV * N_FREQ
    floor_count = VIS_DEV // 8
    device = jnp.arange(N_BASE, dtype=jnp.int32)
    spread = (VIS_DEV - floor_count) * (N_BASE - device) // N_BASE + 1
    additional = jax.random.randint(key, (channels, N_BASE), 0, spread[None, :])
    counts = floor_count + additional
    return jnp.where(device[None, :] == 0, VIS_DEV, counts).astype(jnp.int32)


def draw_bin_map(key, part):
    centre = jax.random.randint(key, (2,), -(G // 8), G // 8 + 1)
    positions = jnp.arange(G, dtype=jnp.int32)
    along_u = (positions - centre[0] + G // 2) % G - G // 2
    along_v = (positions - centre[1] + G // 2) % G - G // 2
    radius_sq = along_u[:, None] * along_u[:, None] + along_v[None, :] * along_v[None, :]
    return jnp.minimum(radius_sq * NBINS // (G // 2 * (G // 2)), NBINS - 1).astype(jnp.int32)


def plant(entries, stream_key, low, high):
    extent = entries.shape
    spot = [jax.random.randint(jax.random.fold_in(stream_key, axis), (), 0, extent[axis]) for axis in range(len(extent))]
    entries = entries.at[tuple(spot)].set(low)
    longest = extent.index(max(extent))
    spot[longest] = (spot[longest] + 1) % extent[longest]
    return entries.at[tuple(spot)].set(high)


def deal_out(key, own, number, rows, number_of, top, bound, slope):
    order = jax.random.permutation(key, number_of)
    heavy_load, usual = shares(number_of, rows * top, bound, slope, True), shares(number_of, rows * top, bound, slope, False)
    places = jnp.arange(number_of)

    def named(tallies, rotation):
        used = int((tallies > 0).sum())
        fixed = max(1, used // 4)
        passed = fixed + (places - fixed + rotation * (used - fixed)) % max(1, number_of - fixed)
        return jnp.zeros((number_of,), jnp.int32).at[order[jnp.where(places < fixed, places, passed)]].set(jnp.asarray(tallies, jnp.int32))

    tallies = jnp.where(number % 4 == 0, named(heavy_load, number // 4), named(usual, number - number // 4 - 1))
    mixed = jax.random.permutation(jax.random.fold_in(own, 3), number_of)
    giver, receiver = mixed[0:number_of // 2 * 2:2], mixed[1:number_of // 2 * 2:2]
    margin = jnp.minimum(tallies[giver] - 1, bound - tallies[receiver]) // 2
    margin = jnp.where((giver == order[0]) | (receiver == order[0]) | (tallies[receiver] == 0), 0, jnp.maximum(margin, 0))
    passed = jax.random.randint(jax.random.fold_in(own, 4), (number_of // 2,), 0, 1 << 20) % (margin + 1)
    tallies = tallies.at[giver].add(-passed).at[receiver].add(passed)
    items = jnp.searchsorted(jnp.cumsum(tallies), jnp.arange(rows * top), side="right").astype(jnp.int32)
    table = items.reshape(top, rows).T
    table = table[jax.random.permutation(jax.random.fold_in(own, 1), rows)]
    rotation = jax.random.randint(jax.random.fold_in(own, 2), (rows, 1), 0, top)
    return jnp.take_along_axis(table, (jnp.arange(top)[None, :] + rotation) % top, axis=1)


def shares(count, total, limit, skew, full):
    loads = [(1 << 20) // math.isqrt(rank ** skew) + 1 for rank in range(1, count + 1)]
    largest = limit if full else min(limit, max(-(-total // count), total * loads[0] // sum(loads)))
    least = 1 if total - largest >= count - 1 else 0
    given, surplus = [largest] + [least] * (count - 1), total - largest - least * (count - 1)
    while surplus > 0:
        free = [i for i in range(1, count) if given[i] < largest] or [i for i in range(1, count) if given[i] < limit]
        pool, remaining = sum([loads[i] for i in free]), surplus
        for i in free:
            more = min(limit - given[i], max(1, remaining * loads[i] // pool), surplus)
            given[i] = given[i] + more
            surplus = surplus - more
    return np.array(given)


def setup_inputs(seed: int = 0) -> dict:
    key_list = jax.random.split(jax.random.key(seed), 9)
    visibility = draw_visibility(jax.random.fold_in(key_list[8], 71), 0)
    tile_of_keys = jax.random.split(jax.random.fold_in(key_list[1], 1), CH * VIS // VIS_DEV)
    tile_of_turns = jax.random.permutation(jax.random.fold_in(key_list[1], 3), CH * VIS // VIS_DEV)
    tile_of = jax.vmap(lambda own, number: deal_out(jax.random.fold_in(key_list[1], 2), own, number, VIS_DEV, N_BASE, 1, CAP, 2))(tile_of_keys, tile_of_turns).reshape((CH, VIS, 1))
    u_within = plant(jax.random.randint(key_list[2], (CH, VIS), 0, TILE), jax.random.fold_in(key_list[2], 1), 0, TILE - 1).astype(jnp.int32)
    v_cell = plant(jax.random.randint(key_list[3], (CH, VIS), 0, G - KW + 1), jax.random.fold_in(key_list[3], 1), 0, G - KW).astype(jnp.int32)
    kernel_index = plant(jax.random.randint(key_list[4], (2, CH, VIS), 0, OVER), jax.random.fold_in(key_list[4], 1), 0, OVER - 1).astype(jnp.int32)
    kernel = jnp.clip(jnp.exp(jax.random.uniform(key_list[5], (OVER, KW), jnp.float32, math.log(0.1), math.log(1.0))), 0.1, 1.0)
    live_count = draw_live_count(jax.random.fold_in(key_list[8], 71), 0)
    bin_map = draw_bin_map(jax.random.fold_in(key_list[8], 71), 0)
    return {"visibility": visibility, "tile_of": tile_of, "u_within": u_within, "v_cell": v_cell, "kernel_index": kernel_index, "kernel": kernel, "live_count": live_count, "bin_map": bin_map}


def channel_power(visibility_re, visibility_im, tile_row, u_within, v_cell, index_u, index_v, used_slots, kernel):
    tile_rows = G // N_BASE
    u_cell = jnp.minimum(tile_row * tile_rows + u_within, G - KW)
    position = jnp.arange(VIS_DEV * N_BASE, dtype=jnp.int32)
    holder = position // VIS_DEV
    is_live = (position % VIS_DEV) < used_slots[holder]
    zeroed = jnp.zeros_like(visibility_re)
    real_part = jnp.where(is_live, visibility_re, zeroed)
    imag_part = jnp.where(is_live, visibility_im, zeroed)
    taps_u = kernel[index_u]
    taps_v = kernel[index_v]
    weight = taps_u[:, :, None] * taps_v[:, None, :]
    offsets = jnp.arange(KW, dtype=jnp.int32)
    row_cells = jnp.broadcast_to(u_cell[:, None, None] + offsets[None, :, None], weight.shape)
    col_cells = jnp.broadcast_to(v_cell[:, None, None] + offsets[None, None, :], weight.shape)
    grid_re = jnp.zeros((G, G), jnp.float32).at[row_cells, col_cells].add(weight * real_part[:, None, None])
    grid_im = jnp.zeros((G, G), jnp.float32).at[row_cells, col_cells].add(weight * imag_part[:, None, None])
    transformed = jnp.fft.fft2(grid_re + 1j * grid_im)
    return transformed.real * transformed.real + transformed.imag * transformed.imag


def reference(visibility, tile_of, u_within, v_cell, kernel_index, kernel, live_count, bin_map):
    def accumulate(running, channel_items):
        vis_re, vis_im, tile_row, within, column, index_u, index_v, used_slots = channel_items
        return running + channel_power(vis_re, vis_im, tile_row, within, column, index_u, index_v, used_slots, kernel), None

    channel_items = (visibility[0], visibility[1], tile_of[:, :, 0], u_within, v_cell, kernel_index[0], kernel_index[1], live_count)
    power_sum, _ = lax.scan(accumulate, jnp.zeros((G, G), jnp.float32), channel_items)
    channels = CH_DEV * N_FREQ
    visits = VIS_DEV * N_BASE
    power_map = power_sum / (channels * visits)
    flat_bins = bin_map.T.reshape(-1)
    totals = jax.ops.segment_sum(power_map.reshape(-1), flat_bins, num_segments=NBINS)
    counts = jax.ops.segment_sum(jnp.ones_like(power_map).reshape(-1), flat_bins, num_segments=NBINS)
    return power_map, totals / counts
```

```python
import functools
import math

import jax
import jax.numpy as jnp
from jax import lax
from jax.experimental import pallas as pl
from jax.experimental.pallas import tpu as pltpu
from jax.sharding import Mesh
from jax.sharding import PartitionSpec as P

G = 1024
NBINS = 512
KW = 8
OVER = 128
SLOTS = 512
TILES = 16
BLOCKS = 128
F32 = jnp.float32
BF16 = jnp.bfloat16
I32 = jnp.int32
AXES = ("freq_0", "freq_1", "freq_2", "base_0", "base_1")
FREQ = AXES[:3]
BASE = AXES[3:]
NORM = 1.0 / (32 * 8192)


def iota(shape, dim):
    return lax.broadcasted_iota(I32, shape, dim)


def cis(phase, period):
    phase = phase & (period - 1)
    phase = jnp.where(phase >= period // 2, phase - period, phase)
    angle = phase.astype(F32) * (2.0 * math.pi / period)
    return jnp.cos(angle), -jnp.sin(angle)


def cmul(ar, ai, br, bi):
    return ar * br - ai * bi, ar * bi + ai * br


def split2(x):
    hi = x.astype(BF16)
    return hi, (x - hi.astype(F32)).astype(BF16)


def dot_nt(a, b):
    return lax.dot_general(a, b, (((1,), (1,)), ((), ())), preferred_element_type=F32)


def dot_nn(a, b):
    return lax.dot_general(a, b, (((1,), (0,)), ((), ())), preferred_element_type=F32)


def take_lanes(table, index):
    return jnp.take_along_axis(table, index, axis=1, mode="promise_in_bounds")


def bin_channel(ch, z, vis_ref, tile_ref, within_ref, vcell_ref, kidx_ref, live, upper):
    tile = tile_ref[ch : ch + 1, :]
    lane = iota((1, SLOTS), 1)
    is_live = lane < live
    member = (tile == iota((TILES, SLOTS), 0)) & is_live
    before = dot_nn(member.astype(BF16), upper)
    rank = jnp.sum(jnp.where(member, before, 0.0), axis=0, keepdims=True).astype(I32)
    block = tile * 4 + (rank >> 4)
    position = (block >> 3) * 128 + (((block & 7) + z) & 7) * 16 + (rank & 15)
    position = jnp.where(is_live, position, -1)
    row = jnp.minimum(within_ref[ch : ch + 1, :], (G - KW) - tile * 64)
    column = vcell_ref[ch : ch + 1, :]
    parts = []
    for part in range(2):
        value = vis_ref[part, ch : ch + 1, :]
        for _ in range(3):
            piece = value.astype(BF16).astype(F32)
            parts.append(piece)
            value = value - piece
    parts += [
        row.astype(F32),
        (column >> 3).astype(F32),
        (column & 7).astype(F32),
        kidx_ref[0, ch : ch + 1, :].astype(F32),
        kidx_ref[1, ch : ch + 1, :].astype(F32),
        jnp.ones((1, SLOTS), F32),
        jnp.zeros((4, SLOTS), F32),
    ]
    payload = jnp.concatenate(parts, axis=0).astype(BF16)
    out = []
    for part in range(4):
        place = (iota((256, SLOTS), 0) + part * 256 == position).astype(F32).astype(BF16)
        got = dot_nt(payload, place)
        out.append(
            jnp.concatenate(
                [
                    got[0:1] + got[1:2] + got[2:3],
                    got[3:4] + got[4:5] + got[5:6],
                    got[6:7],
                    got[7:8] * 8.0 + got[8:9],
                    got[9:10],
                    got[10:11],
                    got[11:12],
                    jnp.zeros((1, 256), F32),
                ],
                axis=0,
            )
        )
    return out


def bin_kernel(live_ref, vis_ref, tile_ref, within_ref, vcell_ref, kidx_ref, out_ref):
    z = lax.axis_index("base_1")
    upper = (iota((SLOTS, SLOTS), 0) < iota((SLOTS, SLOTS), 1)).astype(F32).astype(BF16)
    for ch in range(2):
        parts = bin_channel(
            ch, z, vis_ref, tile_ref, within_ref, vcell_ref, kidx_ref, live_ref[ch, 0], upper
        )
        for index, part in enumerate(parts):
            out_ref[ch, 2 * index] = part[:, :128]
            out_ref[ch, 2 * index + 1] = part[:, 128:]


def image_kernel(
    got_ref,
    kernel_ref,
    out_ref,
    merged,
    ec_ref,
    es_ref,
    pc_ref,
    ps_ref,
    wh_a,
    wl_a,
    rh_a,
    rl_a,
    wh_b,
    wl_b,
    rh_b,
    rl_b,
    grid_ref,
    bh_ref,
    bl_ref,
    mh_ref,
    ml_ref,
    tw_ref,
    count_vmem,
    count_smem,
    order,
    sem,
):
    z = lax.axis_index("base_1")
    group = iota((8, 128), 1) >> 4
    for half in range(2):
        for g in range(8):
            rows = [got_ref[zz, half, g] for zz in range(8)]
            for i in range(8):
                block = rows[(0 - i) % 8]
                for p in range(1, 8):
                    block = jnp.where(group == p, rows[(p - i) % 8], block)
                merged[half * 64 + g * 8 + i] = block
    merged[BLOCKS] = jnp.zeros((8, 128), F32)
    used = merged[0:BLOCKS, 6, :].astype(BF16)
    counts = dot_nt(jnp.ones((8, 128), F32).astype(BF16), used)
    count_vmem[...] = counts.astype(I32)
    copy = pltpu.make_async_copy(count_vmem, count_smem, sem)
    copy.start()

    l_row = iota((128, 128), 0)
    l_val = (l_row & 63) + (l_row >> 6) * 512 + z * 64
    lane = iota((128, 128), 1)
    ec, es = cis(l_val * lane, G)
    ec_ref[...] = ec
    es_ref[...] = es
    zr, zi = cis(l_val, G)
    kern = kernel_ref[...]
    pr = jnp.broadcast_to(kern[7:8], (128, 128))
    pi = jnp.zeros((128, 128), F32)
    for s in range(6, -1, -1):
        pr, pi = cmul(pr, pi, zr, zi)
        pr = pr + kern[s : s + 1]
    pc_ref[...] = pr
    ps_ref[...] = pi
    fc, fs = cis(l_row * lane, 128)
    for quarter, value in ((0, fc), (1, -fs), (2, fs), (3, fc)):
        hi, lo = split2(value)
        at = (slice((quarter >> 1) * 128, (quarter >> 1) * 128 + 128), slice((quarter & 1) * 128, (quarter & 1) * 128 + 128))
        mh_ref[at] = hi
        ml_ref[at] = lo
    tr, ti = cis(l_row, G)
    ar, ai = tr, ti
    for k0 in range(1, 8):
        tw_ref[k0, 0] = ar
        tw_ref[k0, 1] = ai
        if k0 < 7:
            ar, ai = cmul(ar, ai, tr, ti)
    sub = iota((8, 128), 0)
    ct_r, ct_i = cis(sub * iota((8, 128), 1), 8)
    grid_ref[...] = jnp.zeros_like(grid_ref)
    for ref in (wh_b, wl_b, rh_b, rl_b):
        ref[...] = jnp.zeros_like(ref)

    copy.wait()

    def list_step(b, n):
        order[n] = b
        return n + jnp.where(count_smem[0, b] > 0, 1, 0)

    total = lax.fori_loop(0, BLOCKS, list_step, 0, unroll=8)
    order[total] = BLOCKS
    order[total + 1] = BLOCKS

    def build(bid, wh, wl, rh, rl):
        blk = merged[bid]
        ints = blk.astype(I32)

        def spread(row):
            return jnp.broadcast_to(row, (8, 128))

        v = spread(ints[3:4])
        index_d = v & 127
        index_c = v >> 7
        index_u = spread(ints[4:5])
        index_v = spread(ints[5:6])
        w = spread(ints[2:3])
        cr = take_lanes(ct_r, index_c)
        ci = take_lanes(ct_i, index_c)
        cr, ci = cmul(cr, ci, spread(blk[0:1]), spread(blk[1:2]))
        for pair in range(8):
            res, ims = [], []
            for lg in (2 * pair, 2 * pair + 1):
                at = slice(8 * lg, 8 * lg + 8)
                er = take_lanes(ec_ref[at], index_d)
                ei = take_lanes(es_ref[at], index_d)
                qr = take_lanes(pc_ref[at], index_v)
                qi = take_lanes(ps_ref[at], index_v)
                ar, ai = cmul(er, ei, qr, qi)
                ar, ai = cmul(ar, ai, cr, ci)
                res.append(ar)
                ims.append(ai)
            for base, values in ((0, res), (128, ims)):
                hi, lo = split2(jnp.concatenate(values, axis=0))
                at = slice(base + 16 * pair, base + 16 * pair + 16)
                wh[at] = hi
                wl[at] = lo
        taps = take_lanes(kernel_ref[...], index_u)
        turned = jnp.take_along_axis(taps, (sub - w) & 7, axis=0, mode="promise_in_bounds")
        high = turned.astype(BF16).astype(F32)
        low = turned - high
        which = (w - sub + 7) >> 3
        zero = jnp.zeros((8, 128), F32)
        for pair in range(5):
            his, los = [], []
            for k in (2 * pair, 2 * pair + 1):
                hit = which == k
                his.append(jnp.where(hit, high, zero))
                los.append(jnp.where(hit, low, zero))
            rh[16 * pair : 16 * pair + 16] = jnp.concatenate(his, axis=0).astype(BF16)
            rl[16 * pair : 16 * pair + 16] = jnp.concatenate(los, axis=0).astype(BF16)

    def place(bid, wh, wl, rh, rl):
        res = dot_nt(rh[...], wh[...]) + dot_nt(rh[...], wl[...]) + dot_nt(rl[...], wh[...])
        start = pl.multiple_of(((bid >> 2) & 15) * 64, 64)
        grid_ref[pl.ds(start, 80), :] += res

    def step(pair, previous):
        first, second = order[2 * pair], order[2 * pair + 1]
        place(previous, wh_b, wl_b, rh_b, rl_b)
        build(first, wh_a, wl_a, rh_a, rl_a)
        place(first, wh_a, wl_a, rh_a, rl_a)
        build(second, wh_b, wl_b, rh_b, rl_b)
        return second

    last = lax.fori_loop(0, (total + 1) >> 1, step, jnp.int32(BLOCKS))
    place(last, wh_b, wl_b, rh_b, rl_b)

    root = math.sqrt(0.5)
    slot_of = (0, 2, 4, 6, 1, 3, 5, 7)
    for rows in range(8):
        u = [
            (
                grid_ref[128 * a + 16 * rows : 128 * a + 16 * rows + 16, 0:128],
                grid_ref[128 * a + 16 * rows : 128 * a + 16 * rows + 16, 128:256],
            )
            for a in range(8)
        ]

        def add(x, y):
            return x[0] + y[0], x[1] + y[1]

        def sub2(x, y):
            return x[0] - y[0], x[1] - y[1]

        def four(a, b, c, d):
            s, t = add(a, c), sub2(a, c)
            p, q = add(b, d), sub2(b, d)
            mq = (q[1], -q[0])
            return add(s, p), add(t, mq), sub2(s, p), sub2(t, mq)

        even = four(u[0], u[2], u[4], u[6])
        odd = four(u[1], u[3], u[5], u[7])
        o1 = ((odd[1][0] + odd[1][1]) * root, (odd[1][1] - odd[1][0]) * root)
        o2 = (odd[2][1], -odd[2][0])
        o3 = ((odd[3][1] - odd[3][0]) * root, -(odd[3][0] + odd[3][1]) * root)
        odd = (odd[0], o1, o2, o3)
        spectrum = [add(even[k], odd[k]) for k in range(4)] + [sub2(even[k], odd[k]) for k in range(4)]
        at = slice(16 * rows, 16 * rows + 16)
        for k0 in range(8):
            xr, xi = spectrum[k0]
            if k0:
                xr, xi = cmul(xr, xi, tw_ref[k0, 0, at], tw_ref[k0, 1, at])
            col = slice(128 * slot_of[k0], 128 * slot_of[k0] + 128)
            for base, value in ((0, xr), (128, xi)):
                hi, lo = split2(value)
                bh_ref[base + 16 * rows : base + 16 * rows + 16, col] = hi
                bl_ref[base + 16 * rows : base + 16 * rows + 16, col] = lo
    low_half = iota((128, 128), 1) < 64
    for k0 in range(4):
        col = slice(256 * k0, 256 * k0 + 256)
        full = dot_nn(mh_ref[...], bh_ref[:, col]) + dot_nn(mh_ref[...], bl_ref[:, col]) + dot_nn(ml_ref[...], bh_ref[:, col])
        power = (full[:128] * full[:128] + full[128:] * full[128:]) * NORM
        pa, pb = power[:, :128], power[:, 128:]
        ra, rb = pltpu.roll(pa, 64, 1), pltpu.roll(pb, 64, 1)
        out_ref[0, :, k0] = jnp.where(low_half, pa, rb).reshape(16, 8, 128)
        out_ref[1, :, k0] = jnp.where(low_half, ra, pb).reshape(16, 8, 128)


def image_call(got, kernel_t):
    w = pltpu.VMEM((256, 128), BF16)
    r = pltpu.VMEM((80, 128), BF16)
    t = pltpu.VMEM((128, 128), F32)
    return pl.pallas_call(
        image_kernel,
        out_shape=jax.ShapeDtypeStruct((2, 16, 4, 8, 128), F32),
        in_specs=[pl.BlockSpec(memory_space=pltpu.VMEM)] * 2,
        out_specs=pl.BlockSpec(memory_space=pltpu.VMEM),
        scratch_shapes=[
            pltpu.VMEM((BLOCKS + 1, 8, 128), F32),
            t, t, t, t,
            w, w, r, r, w, w, r, r,
            pltpu.VMEM((1040, 256), F32),
            pltpu.VMEM((256, 1024), BF16),
            pltpu.VMEM((256, 1024), BF16),
            pltpu.VMEM((256, 256), BF16),
            pltpu.VMEM((256, 256), BF16),
            pltpu.VMEM((8, 2, 128, 128), F32),
            pltpu.VMEM((8, 128), I32),
            pltpu.SMEM((8, 128), I32),
            pltpu.SMEM((BLOCKS + 2,), I32),
            pltpu.SemaphoreType.DMA,
        ],
    )(got, kernel_t)


def tail_kernel(got_ref, bins_ref, power_ref, sums_ref, onehot, left):
    total = got_ref[0]
    for index in range(1, 32):
        total = total + got_ref[index]
    for k0 in range(8):
        half = (k0 // 4) * 64
        power_ref[pl.ds(k0, 8, stride=8), :] = total[k0 % 4][:, half : half + 64]
    high_row = iota((4, 128), 0)
    for row in range(32):
        bins = bins_ref[row : row + 1, :]
        low = bins & 127
        at = slice(128 * row, 128 * row + 128)
        onehot[:, at] = (iota((128, 128), 0) == low).astype(F32).astype(BF16)
        hit = (bins >> 7) == high_row
        value = total[row // 8][row % 8 : row % 8 + 1]
        p0 = value.astype(BF16).astype(F32)
        p1 = (value - p0).astype(BF16).astype(F32)
        p2 = value - p0 - p1
        zero = jnp.zeros((4, 128), F32)
        pieces = [jnp.where(hit, p, zero) for p in (p0, p1, p2, jnp.ones((1, 128), F32))]
        left[:, at] = jnp.concatenate(pieces, axis=0).astype(BF16)
    got = dot_nt(left[...], onehot[...])
    sums_ref[0:4] = got[0:4] + got[4:8] + got[8:12]
    sums_ref[4:8] = got[12:16]


def tail_call(got, bins):
    return pl.pallas_call(
        tail_kernel,
        out_shape=(jax.ShapeDtypeStruct((64, 64), F32), jax.ShapeDtypeStruct((8, 128), F32)),
        in_specs=[pl.BlockSpec(memory_space=pltpu.VMEM)] * 2,
        out_specs=(pl.BlockSpec(memory_space=pltpu.VMEM),) * 2,
        scratch_shapes=[pltpu.VMEM((128, 4096), BF16), pltpu.VMEM((16, 4096), BF16)],
    )(got, bins)


def per_device(visibility, tile_of, u_within, v_cell, kernel_index, kernel, live_count, bin_map):
    vmem = pl.BlockSpec(memory_space=pltpu.VMEM)
    binned = pl.pallas_call(
        bin_kernel,
        out_shape=jax.ShapeDtypeStruct((2, 8, 8, 128), F32),
        in_specs=[pl.BlockSpec(memory_space=pltpu.SMEM)] + [vmem] * 5,
        out_specs=vmem,
    )(live_count, visibility, tile_of[:, :, 0], u_within, v_cell, kernel_index)
    mine = lax.all_to_all(binned, "base_0", 0, 0, tiled=True)
    got = lax.all_gather(mine, "base_1")
    power = image_call(got, kernel.T)
    pieces = power.reshape(32, 4, 8, 128)
    pieces = lax.all_to_all(pieces, ("base_0",) + FREQ, 0, 0, tiled=True)
    freq = lax.axis_index(FREQ)
    bins = lax.dynamic_slice_in_dim(bin_map, freq * 64, 64, 1)
    bins = bins.T.reshape(8, 2, 4, 64).transpose(2, 0, 1, 3).reshape(32, 128)
    share, sums = tail_call(pieces, bins)
    sums = lax.psum(sums, AXES)
    return share, (sums[:4] / sums[4:]).reshape(NBINS)


def solution(mesh):
    split = Mesh(mesh.devices.reshape(2, 4, 2, 2, 8), AXES)
    return jax.shard_map(
        per_device,
        mesh=split,
        in_specs=(
            P(None, FREQ, BASE),
            P(FREQ, BASE, None),
            P(FREQ, BASE),
            P(FREQ, BASE),
            P(None, FREQ, BASE),
            P(),
            P(FREQ, BASE),
            P(BASE, None),
        ),
        out_specs=(P(FREQ, BASE), P()),
        check_vma=False,
    )
```

```python
import functools
import math

import jax
import jax.numpy as jnp
from jax import lax
from jax.experimental import pallas as pl
from jax.experimental.pallas import tpu as pltpu
from jax.sharding import PartitionSpec as P

G = 1024
NBINS = 512
KW = 8
OVER = 128
SLOTS = 512
TILES = 16
BLOCKS = 128
F32 = jnp.float32
BF16 = jnp.bfloat16
I32 = jnp.int32
MESH = pl.DeviceIdType.MESH
VMEM_SPEC = pl.BlockSpec(memory_space=pltpu.VMEM)
NORM = 1.0 / (32 * 8192)


def iota(shape, dim):
    return lax.broadcasted_iota(I32, shape, dim)


def cis(phase, period):
    phase = phase & (period - 1)
    phase = jnp.where(phase >= period // 2, phase - period, phase)
    angle = phase.astype(F32) * (2.0 * math.pi / period)
    return jnp.cos(angle), -jnp.sin(angle)


def cmul(ar, ai, br, bi):
    return ar * br - ai * bi, ar * bi + ai * br


def split2(x):
    hi = x.astype(BF16)
    return hi, (x - hi.astype(F32)).astype(BF16)


def dot_nt(a, b):
    return lax.dot_general(a, b, (((1,), (1,)), ((), ())), preferred_element_type=F32)


def dot_nn(a, b):
    return lax.dot_general(a, b, (((1,), (0,)), ((), ())), preferred_element_type=F32)


def take_lanes(table, index):
    return jnp.take_along_axis(table, index, axis=1, mode="promise_in_bounds")


def bin_channel(ch, z, vis_ref, tile_ref, within_ref, vcell_ref, kidx_ref, live, upper):
    tile = tile_ref[ch]
    lane = iota((1, SLOTS), 1)
    is_live = lane < live
    member = (tile == iota((TILES, SLOTS), 0)) & is_live
    before = dot_nn(member.astype(BF16), upper)
    rank = jnp.sum(jnp.where(member, before, 0.0), axis=0, keepdims=True).astype(I32)
    block = tile * 4 + (rank >> 4)
    position = (block >> 3) * 128 + (((block & 7) + z) & 7) * 16 + (rank & 15)
    position = jnp.where(is_live, position, -1)
    row = jnp.minimum(within_ref[ch : ch + 1, :], (G - KW) - tile * 64)
    column = vcell_ref[ch : ch + 1, :]
    parts = []
    for part in range(2):
        value = vis_ref[part, ch : ch + 1, :]
        for _ in range(3):
            piece = value.astype(BF16).astype(F32)
            parts.append(piece)
            value = value - piece
    parts += [
        row.astype(F32),
        (column >> 3).astype(F32),
        (column & 7).astype(F32),
        kidx_ref[0, ch : ch + 1, :].astype(F32),
        kidx_ref[1, ch : ch + 1, :].astype(F32),
        jnp.ones((1, SLOTS), F32),
        jnp.zeros((4, SLOTS), F32),
    ]
    payload = jnp.concatenate(parts, axis=0).astype(BF16)
    out = []
    for part in range(4):
        place = (iota((256, SLOTS), 0) + part * 256 == position).astype(F32).astype(BF16)
        got = dot_nt(payload, place)
        out.append(
            jnp.concatenate(
                [
                    got[0:1] + got[1:2] + got[2:3],
                    got[3:4] + got[4:5] + got[5:6],
                    got[6:7],
                    got[7:8] * 8.0 + got[8:9],
                    got[9:10],
                    got[10:11],
                    got[11:12],
                    jnp.zeros((1, 256), F32),
                ],
                axis=0,
            )
        )
    return out


def places():
    base = lax.axis_index("base")
    return base // 8, base % 8


def gather_kernel(
    live_ref, vis_ref, tile_ref, within_ref, vcell_ref, kidx_ref, out_ref, packed, got, send, land, relay, local
):
    h, z = places()
    hops = (1, -1, 2, -2)

    def device(side, step):
        return {"base": side * 8 + (z + step + 8) % 8}

    barrier = pltpu.get_barrier_semaphore()
    for step in hops:
        pl.semaphore_signal(barrier, 1, device_id=device(h, step), device_id_type=MESH)
    for step in (0,) + hops:
        pl.semaphore_signal(barrier, 1, device_id=device(1 - h, step), device_id_type=MESH)

    upper = (iota((SLOTS, SLOTS), 0) < iota((SLOTS, SLOTS), 1)).astype(F32).astype(BF16)
    for ch in range(2):
        parts = bin_channel(
            ch, z, vis_ref, tile_ref, within_ref, vcell_ref, kidx_ref, live_ref[0, ch], upper
        )
        for index, part in enumerate(parts):
            packed[ch, 12 * index : 12 * index + 6] = part[:6, :128]
            packed[ch, 12 * index + 6 : 12 * index + 12] = part[:6, 128:]
    pl.semaphore_wait(barrier, 9)

    def direct(side, step, number):
        return pltpu.make_async_remote_copy(
            src_ref=packed.at[side],
            dst_ref=got.at[z, h],
            send_sem=send.at[number],
            recv_sem=land.at[z, h],
            device_id=device(side, step),
            device_id_type=MESH,
        )

    def arrival(step, side):
        zz = (z + step + 8) % 8
        return pltpu.make_async_remote_copy(
            src_ref=got.at[zz, side],
            dst_ref=got.at[zz, side],
            send_sem=send.at[0],
            recv_sem=land.at[zz, side],
            device_id=device(1 - h, 0),
            device_id_type=MESH,
        )

    copies = []
    for step in (2, -2):
        copies.append(direct(1 - h, step, len(copies)))
        copies.append(direct(h, step, len(copies)))
    for step in (1, -1):
        copies.append(direct(1 - h, step, len(copies)))
        copies.append(direct(h, step, len(copies)))
    copies.append(direct(1 - h, 0, len(copies)))
    for copy in copies:
        copy.start()
    own = pltpu.make_async_copy(packed.at[h], got.at[z, h], local)
    own.start()

    relays = []

    def pass_on(source, side, step):
        zz = (z + source + 8) % 8
        copy = pltpu.make_async_remote_copy(
            src_ref=got.at[zz, side],
            dst_ref=got.at[zz, side],
            send_sem=relay.at[len(relays)],
            recv_sem=land.at[zz, side],
            device_id=device(h, step),
            device_id_type=MESH,
        )
        copy.start()
        relays.append(copy)

    arrival(-2, h).wait_recv()
    pass_on(-2, h, 2)
    pass_on(-2, h, 1)
    arrival(2, h).wait_recv()
    pass_on(2, h, -1)
    arrival(2, 1 - h).wait_recv()
    pass_on(2, 1 - h, -2)
    pass_on(2, 1 - h, -1)
    arrival(-2, 1 - h).wait_recv()
    pass_on(-2, 1 - h, 1)
    for step in (1, -1):
        arrival(step, h).wait_recv()
        arrival(step, 1 - h).wait_recv()
    arrival(0, 1 - h).wait_recv()
    for step in (3, -3, 4):
        arrival(step, h).wait_recv()
        arrival(step, 1 - h).wait_recv()
    own.wait()
    for copy in copies + relays:
        copy.wait_send()
    group = iota((48, 128), 1) >> 4
    for half in range(2):
        for i in range(8):
            block = got[(0 - i) % 8, half]
            for p in range(1, 8):
                block = jnp.where(group == p, got[(p - i) % 8, half], block)
            out_ref[half * 8 + i] = block


def gather_call(live, visibility, tile, within, column, kernel_index):
    return pl.pallas_call(
        gather_kernel,
        out_shape=jax.ShapeDtypeStruct((16, 48, 128), F32),
        in_specs=[pl.BlockSpec(memory_space=pltpu.SMEM)] + [VMEM_SPEC] * 5,
        out_specs=VMEM_SPEC,
        scratch_shapes=[
            pltpu.VMEM((2, 48, 128), F32),
            pltpu.VMEM((8, 2, 48, 128), F32),
            pltpu.SemaphoreType.DMA((9,)),
            pltpu.SemaphoreType.DMA((8, 2)),
            pltpu.SemaphoreType.DMA((6,)),
            pltpu.SemaphoreType.DMA,
        ],
        compiler_params=pltpu.CompilerParams(collective_id=0, has_side_effects=True),
    )(live, visibility, tile, within, column, kernel_index)


def grid_kernel(
    merged,
    kernel_ref,
    grid_ref,
    ec_ref,
    es_ref,
    pc_ref,
    ps_ref,
    wh_a,
    wl_a,
    rh_a,
    rl_a,
    wh_b,
    wl_b,
    rh_b,
    rl_b,
    count_vmem,
    count_smem,
    order,
    sem,
):
    _, z = places()
    used = (merged[...].reshape(768, 128) != 0.0).astype(F32).astype(BF16)
    counts = dot_nt(jnp.ones((8, 128), F32).astype(BF16), used)
    count_vmem[...] = counts.astype(I32)
    copy = pltpu.make_async_copy(count_vmem, count_smem, sem)
    copy.start()

    l_row = iota((128, 128), 0)
    l_val = (l_row & 63) + (l_row >> 6) * 512 + z * 64
    lane = iota((128, 128), 1)
    ec, es = cis(l_val * lane, G)
    ec_ref[...] = ec
    es_ref[...] = es
    zr, zi = cis(l_val, G)
    kern = kernel_ref[...]
    pr = jnp.broadcast_to(kern[7:8], (128, 128))
    pi = jnp.zeros((128, 128), F32)
    for s in range(6, -1, -1):
        pr, pi = cmul(pr, pi, zr, zi)
        pr = pr + kern[s : s + 1]
    pc_ref[...] = pr
    ps_ref[...] = pi
    sub = iota((8, 128), 0)
    ct_r, ct_i = cis(sub * iota((8, 128), 1), 8)
    grid_ref[...] = jnp.zeros_like(grid_ref)
    for ref in (wh_b, wl_b, rh_b, rl_b):
        ref[...] = jnp.zeros_like(ref)

    copy.wait()

    def list_step(b, n):
        order[n] = b
        first = ((b >> 6) * 8 + (b & 7)) * 48 + ((b >> 3) & 7) * 6
        found = count_smem[0, first] + count_smem[0, first + 1]
        return n + jnp.where(found > 0, 1, 0)

    total = lax.fori_loop(0, BLOCKS, list_step, 0, unroll=8)
    order[total] = BLOCKS
    order[total + 1] = BLOCKS

    def build(bid, wh, wl, rh, rl):
        which = ((bid >> 6) & 1) * 8 + (bid & 7)
        first = ((bid >> 3) & 7) * 6
        keep = jnp.where(bid < BLOCKS, 1.0, 0.0)

        def field(index):
            return jnp.broadcast_to(merged[which, pl.ds(first + index, 1), :], (8, 128))

        v = field(3).astype(I32)
        index_d = v & 127
        index_c = v >> 7
        index_u = field(4).astype(I32)
        index_v = field(5).astype(I32)
        w = field(2).astype(I32)
        cr = take_lanes(ct_r, index_c)
        ci = take_lanes(ct_i, index_c)
        cr, ci = cmul(cr, ci, field(0) * keep, field(1) * keep)
        for pair in range(8):
            res, ims = [], []
            for lg in (2 * pair, 2 * pair + 1):
                at = slice(8 * lg, 8 * lg + 8)
                er = take_lanes(ec_ref[at], index_d)
                ei = take_lanes(es_ref[at], index_d)
                qr = take_lanes(pc_ref[at], index_v)
                qi = take_lanes(ps_ref[at], index_v)
                ar, ai = cmul(er, ei, qr, qi)
                ar, ai = cmul(ar, ai, cr, ci)
                res.append(ar)
                ims.append(ai)
            for base, values in ((0, res), (128, ims)):
                hi, lo = split2(jnp.concatenate(values, axis=0))
                at = slice(base + 16 * pair, base + 16 * pair + 16)
                wh[at] = hi
                wl[at] = lo
        taps = take_lanes(kernel_ref[...], index_u)
        turned = jnp.take_along_axis(taps, (sub - w) & 7, axis=0, mode="promise_in_bounds")
        high = turned.astype(BF16).astype(F32)
        low = turned - high
        down = (w - sub + 7) >> 3
        zero = jnp.zeros((8, 128), F32)
        for pair in range(5):
            his, los = [], []
            for k in (2 * pair, 2 * pair + 1):
                hit = down == k
                his.append(jnp.where(hit, high, zero))
                los.append(jnp.where(hit, low, zero))
            rh[16 * pair : 16 * pair + 16] = jnp.concatenate(his, axis=0).astype(BF16)
            rl[16 * pair : 16 * pair + 16] = jnp.concatenate(los, axis=0).astype(BF16)

    def place(bid, wh, wl, rh, rl):
        res = dot_nt(rh[...], wh[...]) + dot_nt(rh[...], wl[...]) + dot_nt(rl[...], wh[...])
        start = pl.multiple_of(((bid >> 2) & 15) * 64, 64)
        grid_ref[pl.ds(start, 80), :] += res

    def step(pair, previous):
        first, second = order[2 * pair], order[2 * pair + 1]
        place(previous, wh_b, wl_b, rh_b, rl_b)
        build(first, wh_a, wl_a, rh_a, rl_a)
        place(first, wh_a, wl_a, rh_a, rl_a)
        build(second, wh_b, wl_b, rh_b, rl_b)
        return second

    last = lax.fori_loop(0, (total + 1) >> 1, step, jnp.int32(BLOCKS))
    place(last, wh_b, wl_b, rh_b, rl_b)

def grid_call(merged, kernel_t):
    w = pltpu.VMEM((256, 128), BF16)
    r = pltpu.VMEM((80, 128), BF16)
    t = pltpu.VMEM((128, 128), F32)
    return pl.pallas_call(
        grid_kernel,
        out_shape=jax.ShapeDtypeStruct((1040, 256), F32),
        in_specs=[VMEM_SPEC] * 2,
        out_specs=VMEM_SPEC,
        scratch_shapes=[
            t, t, t, t,
            w, w, r, r, w, w, r, r,
            pltpu.VMEM((8, 768), I32),
            pltpu.SMEM((8, 768), I32),
            pltpu.SMEM((BLOCKS + 2,), I32),
            pltpu.SemaphoreType.DMA,
        ],
    )(merged, kernel_t)


def tail_kernel(
    grid_ref, bins_ref, power_ref, spectrum_ref,
    bh_ref, bl_ref, mh_ref, ml_ref, tw_ref, turned, onehot, left,
    piece, partner, summed, landed, counts, counts_in, counts_z, counts_plane, totals, totals_in, totals_z, totals_plane,
    s_pair, r_pair, s_sum, r_sum, s_count, r_count, s_total, r_total, s_countz, r_countz, s_totalz, r_totalz,
):
    h, z = places()
    freq = lax.axis_index("freq")
    quad, core = freq // 2, freq % 2
    me = h * 16 + freq
    me_pair = h * 8 + quad

    def plane_device(index):
        return {"freq": index % 16, "base": (index // 16) * 8 + z}

    def column_device(index):
        return {"freq": freq, "base": h * 8 + index}

    barrier = pltpu.get_barrier_semaphore()

    def greet_plane(k, _):
        pl.semaphore_signal(barrier, 1, device_id=plane_device((me + k) % 32), device_id_type=MESH)
        return 0

    def greet_column(k, _):
        pl.semaphore_signal(barrier, 1, device_id=column_device((z + k) % 8), device_id_type=MESH)
        return 0

    lax.fori_loop(1, 32, greet_plane, 0)
    lax.fori_loop(1, 8, greet_column, 0)

    row128, lane128 = iota((128, 128), 0), iota((128, 128), 1)
    fc, fs = cis(row128 * lane128, 128)
    for quarter, value in ((0, fc), (1, -fs), (2, fs), (3, fc)):
        hi, lo = split2(value)
        at = (
            slice((quarter >> 1) * 128, (quarter >> 1) * 128 + 128),
            slice((quarter & 1) * 128, (quarter & 1) * 128 + 128),
        )
        mh_ref[at] = hi
        ml_ref[at] = lo
    tr, ti = cis(row128, G)
    ar, ai = tr, ti
    for k0 in range(1, 8):
        tw_ref[k0, 0] = ar
        tw_ref[k0, 1] = ai
        if k0 < 7:
            ar, ai = cmul(ar, ai, tr, ti)

    at = pl.multiple_of((freq // 2) * 128, 128)
    bins = bins_ref[:, pl.ds(at, 128)].astype(F32)
    bins = jnp.concatenate([bins, jnp.zeros((64, 128), F32)], axis=0)
    bins = pltpu.roll(bins, core * 64, 1)
    turned[...] = bins.T
    high_row = iota((4, 128), 0)
    lane8 = iota((8, 128), 1)
    hits = []
    for k0 in range(4):
        ours = turned[pl.ds(k0, 8, stride=8), :]
        other = turned[pl.ds(k0 + 4, 8, stride=8), :]
        both = jnp.where(lane8 < 64, ours, pltpu.roll(other, 64, 1)).astype(I32)
        for sub in range(8):
            row = 8 * k0 + sub
            found = both[sub : sub + 1]
            at = slice(128 * row, 128 * row + 128)
            onehot[:, at] = (row128 == (found & 127)).astype(F32).astype(BF16)
            hit = ((found >> 7) == high_row).astype(F32)
            left[12:16, at] = hit
            left[0:4, at] = hit
            left[4:8, at] = hit
            left[8:12, at] = hit
    got = dot_nt(left[...].astype(BF16), onehot[...])
    counts[...] = got[12:16]

    root = math.sqrt(0.5)
    slot_of = (0, 2, 4, 6, 1, 3, 5, 7)
    for rows in range(8):
        u = [
            (
                grid_ref[128 * a + 16 * rows : 128 * a + 16 * rows + 16, 0:128],
                grid_ref[128 * a + 16 * rows : 128 * a + 16 * rows + 16, 128:256],
            )
            for a in range(8)
        ]

        def add(x, y):
            return x[0] + y[0], x[1] + y[1]

        def sub2(x, y):
            return x[0] - y[0], x[1] - y[1]

        def four(a, b, c, d):
            s, t = add(a, c), sub2(a, c)
            p, q = add(b, d), sub2(b, d)
            mq = (q[1], -q[0])
            return add(s, p), add(t, mq), sub2(s, p), sub2(t, mq)

        even = four(u[0], u[2], u[4], u[6])
        odd = four(u[1], u[3], u[5], u[7])
        o1 = ((odd[1][0] + odd[1][1]) * root, (odd[1][1] - odd[1][0]) * root)
        o2 = (odd[2][1], -odd[2][0])
        o3 = ((odd[3][1] - odd[3][0]) * root, -(odd[3][0] + odd[3][1]) * root)
        odd = (odd[0], o1, o2, o3)
        spectrum = [add(even[k], odd[k]) for k in range(4)] + [sub2(even[k], odd[k]) for k in range(4)]
        at = slice(16 * rows, 16 * rows + 16)
        for k0 in range(8):
            xr, xi = spectrum[k0]
            if k0:
                xr, xi = cmul(xr, xi, tw_ref[k0, 0, at], tw_ref[k0, 1, at])
            col = slice(128 * slot_of[k0], 128 * slot_of[k0] + 128)
            for base, value in ((0, xr), (128, xi)):
                hi, lo = split2(value)
                bh_ref[base + 16 * rows : base + 16 * rows + 16, col] = hi
                bl_ref[base + 16 * rows : base + 16 * rows + 16, col] = lo
    pl.semaphore_wait(barrier, 38)

    def plane_copy(k, buf, slots, s, r):
        peer = (me + k) % 32
        return pltpu.make_async_remote_copy(
            src_ref=buf, dst_ref=slots.at[me], send_sem=s.at[k], recv_sem=r.at[me],
            device_id=plane_device(peer), device_id_type=MESH,
        )

    def column_copy(k, buf, slots, s, r):
        peer = (z + k) % 8
        return pltpu.make_async_remote_copy(
            src_ref=buf, dst_ref=slots.at[z], send_sem=s.at[k], recv_sem=r.at[z],
            device_id=column_device(peer), device_id_type=MESH,
        )

    def start_all(count, make, *args):
        def body(k, _):
            make(k, *args).start()
            return 0

        lax.fori_loop(1, count, body, 0)

    def wait_plane(buf, slots, s, r):
        def body(k, total):
            source = (me + k) % 32
            pltpu.make_async_remote_copy(
                src_ref=buf, dst_ref=slots.at[source], send_sem=s.at[k], recv_sem=r.at[source],
                device_id=plane_device(source), device_id_type=MESH,
            ).wait_recv()
            return total + slots[source]

        return lax.fori_loop(1, 32, body, buf[...])

    def wait_column(buf, slots, s, r):
        def body(k, total):
            source = (z + k) % 8
            pltpu.make_async_remote_copy(
                src_ref=buf, dst_ref=slots.at[source], send_sem=s.at[k], recv_sem=r.at[source],
                device_id=column_device(source), device_id_type=MESH,
            ).wait_recv()
            return total + slots[source]

        return lax.fori_loop(1, 8, body, buf[...])

    def sent_all(count, make, *args):
        def body(k, _):
            make(k, *args).wait_send()
            return 0

        lax.fori_loop(1, count, body, 0)

    plane_counts = (counts, counts_in, s_count, r_count)
    start_all(32, plane_copy, *plane_counts)

    def pair_copy(k0):
        return pltpu.make_async_remote_copy(
            src_ref=piece.at[1 - core, k0], dst_ref=partner.at[k0], send_sem=s_pair.at[k0], recv_sem=r_pair.at[k0],
            device_id={"freq": quad * 2 + 1 - core}, device_id_type=MESH,
        )

    low_half = iota((128, 128), 1) < 64
    for k0 in range(4):
        col = slice(256 * k0, 256 * k0 + 256)
        full = dot_nn(mh_ref[...], bh_ref[:, col]) + dot_nn(mh_ref[...], bl_ref[:, col]) + dot_nn(ml_ref[...], bh_ref[:, col])
        power = (full[:128] * full[:128] + full[128:] * full[128:]) * NORM
        pa, pb = power[:, :128], power[:, 128:]
        ra, rb = pltpu.roll(pa, 64, 1), pltpu.roll(pb, 64, 1)
        for side, block in ((0, jnp.where(low_half, pa, rb)), (1, jnp.where(low_half, ra, pb))):
            block = block.reshape(8, 2, 8, 128)
            for cc in range(2):
                piece[cc, k0, side] = block[:, cc]
        pair_copy(k0).start()
    for k0 in range(4):
        pair_copy(k0).wait_recv()
        for side in range(2):
            for q in range(8):
                summed[side * 8 + q, k0] = piece[core, k0, side, q] + partner[k0, side, q]

    def sum_copy(k):
        peer = (me_pair + k) % 16
        return pltpu.make_async_remote_copy(
            src_ref=summed.at[peer], dst_ref=landed.at[me_pair], send_sem=s_sum.at[k], recv_sem=r_sum.at[me_pair],
            device_id={"freq": (peer % 8) * 2 + core, "base": (peer // 8) * 8 + z}, device_id_type=MESH,
        )

    start_all(16, sum_copy)
    counts_plane[...] = wait_plane(*plane_counts)
    column_counts = (counts_plane, counts_z, s_countz, r_countz)
    start_all(8, column_copy, *column_counts)

    def wait_sum(k, total):
        source = (me_pair + k) % 16
        pltpu.make_async_remote_copy(
            src_ref=summed.at[source], dst_ref=landed.at[source], send_sem=s_sum.at[k], recv_sem=r_sum.at[source],
            device_id={"freq": (source % 8) * 2 + core, "base": (source // 8) * 8 + z}, device_id_type=MESH,
        ).wait_recv()
        return total + landed[source]

    total = lax.fori_loop(1, 16, wait_sum, summed[me_pair])
    for k0 in range(4):
        for sub in range(8):
            at = slice(128 * (8 * k0 + sub), 128 * (8 * k0 + sub) + 128)
            hit = left[12:16, at]
            value = total[k0][sub : sub + 1]
            p0 = value.astype(BF16).astype(F32)
            p1 = (value - p0).astype(BF16).astype(F32)
            left[0:4, at] = hit * p0
            left[4:8, at] = hit * p1
            left[8:12, at] = hit * (value - p0 - p1)
    got = dot_nt(left[...].astype(BF16), onehot[...])
    totals[...] = got[0:4] + got[4:8] + got[8:12]
    plane_totals = (totals, totals_in, s_total, r_total)
    start_all(32, plane_copy, *plane_totals)
    for k0 in range(8):
        half = (k0 // 4) * 64
        power_ref[pl.ds(k0, 8, stride=8), :] = total[k0 % 4][:, half : half + 64]
    all_counts = wait_column(*column_counts)
    totals_plane[...] = wait_plane(*plane_totals)
    column_totals = (totals_plane, totals_z, s_totalz, r_totalz)
    start_all(8, column_copy, *column_totals)
    sent_all(32, plane_copy, *plane_counts)
    sent_all(8, column_copy, *column_counts)
    sent_all(16, sum_copy)
    sent_all(32, plane_copy, *plane_totals)
    for k0 in range(4):
        pair_copy(k0).wait_send()
    spectrum_ref[...] = wait_column(*column_totals) / all_counts
    sent_all(8, column_copy, *column_totals)


def tail_call(grid, bins):
    dma = pltpu.SemaphoreType.DMA
    small = (4, 128)
    return pl.pallas_call(
        tail_kernel,
        out_shape=(jax.ShapeDtypeStruct((64, 64), F32), jax.ShapeDtypeStruct((4, 128), F32)),
        in_specs=[VMEM_SPEC] * 2,
        out_specs=(VMEM_SPEC,) * 2,
        scratch_shapes=[
            pltpu.VMEM((256, 1024), BF16),
            pltpu.VMEM((256, 1024), BF16),
            pltpu.VMEM((256, 256), BF16),
            pltpu.VMEM((256, 256), BF16),
            pltpu.VMEM((8, 2, 128, 128), F32),
            pltpu.VMEM((128, 128), F32),
            pltpu.VMEM((128, 4096), BF16),
            pltpu.VMEM((16, 4096), F32),
            pltpu.VMEM((2, 4, 2, 8, 8, 128), F32),
            pltpu.VMEM((4, 2, 8, 8, 128), F32),
            pltpu.VMEM((16, 4, 8, 128), F32),
            pltpu.VMEM((16, 4, 8, 128), F32),
            pltpu.VMEM(small, F32),
            pltpu.VMEM((32,) + small, F32),
            pltpu.VMEM((8,) + small, F32),
            pltpu.VMEM(small, F32),
            pltpu.VMEM(small, F32),
            pltpu.VMEM((32,) + small, F32),
            pltpu.VMEM((8,) + small, F32),
            pltpu.VMEM(small, F32),
            dma((4,)), dma((4,)), dma((16,)), dma((16,)),
            dma((32,)), dma((32,)), dma((32,)), dma((32,)),
            dma((8,)), dma((8,)), dma((8,)), dma((8,)),
        ],
        compiler_params=pltpu.CompilerParams(collective_id=1, has_side_effects=True),
    )(grid, bins)


def per_device(visibility, tile_of, u_within, v_cell, kernel_index, kernel, live_count, bin_map):
    merged = gather_call(
        live_count.T, visibility, tile_of.transpose(0, 2, 1), u_within, v_cell, kernel_index
    )
    grid = grid_call(merged, kernel.T)
    power, spectrum = tail_call(grid, bin_map)
    return power, spectrum.reshape(NBINS)


def solution(mesh):
    return jax.shard_map(
        per_device,
        mesh=mesh,
        in_specs=(
            P(None, "freq", "base"),
            P("freq", "base", None),
            P("freq", "base"),
            P("freq", "base"),
            P(None, "freq", "base"),
            P(),
            P("freq", "base"),
            P("base", None),
        ),
        out_specs=(P("freq", "base"), P()),
        check_vma=False,
    )
```

```python
import functools
import math

import jax
import jax.numpy as jnp
from jax import lax
from jax.experimental import pallas as pl
from jax.experimental.pallas import tpu as pltpu
from jax.sharding import PartitionSpec as P

G = 1024
NBINS = 512
KW = 8
OVER = 128
SLOTS = 512
TILES = 16
BLOCKS = 128
GROUP = 4
F32 = jnp.float32
BF16 = jnp.bfloat16
I32 = jnp.int32
MESH = pl.DeviceIdType.MESH
VMEM_SPEC = pl.BlockSpec(memory_space=pltpu.VMEM)
LIMIT = 16 * 1024 * 1024
NORM = 1.0 / (32 * 8192)


def iota(shape, dim):
    return lax.broadcasted_iota(I32, shape, dim)


def cis(phase, period):
    phase = phase & (period - 1)
    phase = jnp.where(phase >= period // 2, phase - period, phase)
    angle = phase.astype(F32) * (2.0 * math.pi / period)
    return jnp.cos(angle), -jnp.sin(angle)


def cmul(ar, ai, br, bi):
    return ar * br - ai * bi, ar * bi + ai * br


def split2(x):
    hi = x.astype(BF16)
    return hi, (x - hi.astype(F32)).astype(BF16)


def dot_nt(a, b):
    return lax.dot_general(a, b, (((1,), (1,)), ((), ())), preferred_element_type=F32)


def dot_nn(a, b):
    return lax.dot_general(a, b, (((1,), (0,)), ((), ())), preferred_element_type=F32)


def take_lanes(table, index):
    return jnp.take_along_axis(table, index, axis=1, mode="promise_in_bounds")


def bin_channel(ch, z, vis_ref, tile_ref, within_ref, vcell_ref, kidx_ref, live, upper):
    tile = tile_ref[ch]
    lane = iota((1, SLOTS), 1)
    is_live = lane < live
    member = (tile == iota((TILES, SLOTS), 0)) & is_live
    before = dot_nn(member.astype(BF16), upper)
    rank = jnp.sum(jnp.where(member, before, 0.0), axis=0, keepdims=True).astype(I32)
    block = tile * 4 + (rank >> 4)
    position = (block >> 3) * 128 + (((block & 7) + z) & 7) * 16 + (rank & 15)
    position = jnp.where(is_live, position, -1)
    row = jnp.minimum(within_ref[ch : ch + 1, :], (G - KW) - tile * 64)
    column = vcell_ref[ch : ch + 1, :]
    parts = []
    for part in range(2):
        value = vis_ref[part, ch : ch + 1, :]
        for _ in range(3):
            piece = value.astype(BF16).astype(F32)
            parts.append(piece)
            value = value - piece
    parts += [
        row.astype(F32),
        (column >> 3).astype(F32),
        (column & 7).astype(F32),
        kidx_ref[0, ch : ch + 1, :].astype(F32),
        kidx_ref[1, ch : ch + 1, :].astype(F32),
        jnp.ones((1, SLOTS), F32),
        jnp.zeros((4, SLOTS), F32),
    ]
    payload = jnp.concatenate(parts, axis=0).astype(BF16)
    out = []
    for part in range(4):
        place = (iota((256, SLOTS), 0) + part * 256 == position).astype(F32).astype(BF16)
        got = dot_nt(payload, place)
        out.append(
            jnp.concatenate(
                [
                    got[0:1] + got[1:2] + got[2:3],
                    got[3:4] + got[4:5] + got[5:6],
                    got[6:7],
                    got[7:8] * 8.0 + got[8:9],
                    got[9:10],
                    got[10:11],
                    got[11:12],
                    jnp.zeros((1, 256), F32),
                ],
                axis=0,
            )
        )
    return out


def places():
    base = lax.axis_index("base")
    return base // 8, base % 8


def gather_kernel(
    live_hbm,
    vis_hbm,
    tile_hbm,
    within_hbm,
    vcell_hbm,
    kidx_hbm,
    kernel_hbm,
    bins_ref,
    out_ref,
    kernel_ref,
    used_ref,
    phase_ref,
    matrix_ref,
    twiddle_ref,
    onehot_ref,
    hit_ref,
    counts_ref,
    packed,
    got,
    bins,
    turned,
    live_ref,
    vis_ref,
    tile_ref,
    within_ref,
    vcell_ref,
    kidx_ref,
    send,
    land,
    relay,
    local,
    fetched,
):
    inputs = (
        (live_hbm, live_ref),
        (tile_hbm, tile_ref),
        (vis_hbm, vis_ref),
        (within_hbm, within_ref),
        (vcell_hbm, vcell_ref),
        (kidx_hbm, kidx_ref),
        (kernel_hbm, kernel_ref),
    )
    loads = [
        pltpu.make_async_copy(source, place, fetched.at[index])
        for index, (source, place) in enumerate(inputs)
    ]
    for load in loads:
        load.start()
    h, z = places()
    freq = lax.axis_index("freq")
    at = pl.multiple_of((freq // 2) * 128, 128)
    fetch = pltpu.make_async_copy(bins_ref.at[:, pl.ds(at, 128)], bins, fetched.at[7])
    fetch.start()
    hops = (1, -1, 2, -2)

    def device(side, step):
        return {"base": side * 8 + (z + step + 8) % 8}

    barrier = pltpu.get_barrier_semaphore()
    for step in hops:
        pl.semaphore_signal(barrier, 1, device_id=device(h, step), device_id_type=MESH)
    for step in (0,) + hops:
        pl.semaphore_signal(barrier, 1, device_id=device(1 - h, step), device_id_type=MESH)

    upper = (iota((SLOTS, SLOTS), 0) < iota((SLOTS, SLOTS), 1)).astype(F32).astype(BF16)
    for load in loads:
        load.wait()
    for ch in range(2):
        live = live_ref[0:1, ch : ch + 1]
        parts = bin_channel(
            ch, z, vis_ref, tile_ref, within_ref, vcell_ref, kidx_ref, live, upper
        )
        for index, part in enumerate(parts):
            packed[ch, 12 * index : 12 * index + 6] = part[:6, :128]
            packed[ch, 12 * index + 6 : 12 * index + 12] = part[:6, 128:]
    pl.semaphore_wait(barrier, 9)

    def direct(side, step, number):
        return pltpu.make_async_remote_copy(
            src_ref=packed.at[side],
            dst_ref=got.at[z, h],
            send_sem=send.at[number],
            recv_sem=land.at[z, h],
            device_id=device(side, step),
            device_id_type=MESH,
        )

    def arrival(step, side):
        zz = (z + step + 8) % 8
        return pltpu.make_async_remote_copy(
            src_ref=got.at[zz, side],
            dst_ref=got.at[zz, side],
            send_sem=send.at[0],
            recv_sem=land.at[zz, side],
            device_id=device(1 - h, 0),
            device_id_type=MESH,
        )

    copies = []
    for step in (2, -2):
        copies.append(direct(1 - h, step, len(copies)))
        copies.append(direct(h, step, len(copies)))
    for step in (1, -1):
        copies.append(direct(1 - h, step, len(copies)))
        copies.append(direct(h, step, len(copies)))
    copies.append(direct(1 - h, 0, len(copies)))
    for copy in copies:
        copy.start()
    own = pltpu.make_async_copy(packed.at[h], got.at[z, h], local)
    own.start()

    column_tables(z, kernel_ref, phase_ref)
    row_tables(matrix_ref, twiddle_ref)
    fetch.wait()
    bin_tables(freq % 2, bins, turned, onehot_ref, hit_ref, counts_ref)

    relays = []

    def pass_on(source, side, step):
        zz = (z + source + 8) % 8
        copy = pltpu.make_async_remote_copy(
            src_ref=got.at[zz, side],
            dst_ref=got.at[zz, side],
            send_sem=relay.at[len(relays)],
            recv_sem=land.at[zz, side],
            device_id=device(h, step),
            device_id_type=MESH,
        )
        copy.start()
        relays.append(copy)

    arrival(-2, h).wait_recv()
    pass_on(-2, h, 2)
    pass_on(-2, h, 1)
    arrival(2, h).wait_recv()
    pass_on(2, h, -1)
    arrival(2, 1 - h).wait_recv()
    pass_on(2, 1 - h, -2)
    pass_on(2, 1 - h, -1)
    arrival(-2, 1 - h).wait_recv()
    pass_on(-2, 1 - h, 1)
    for step in (1, -1):
        arrival(step, h).wait_recv()
        arrival(step, 1 - h).wait_recv()
    arrival(0, 1 - h).wait_recv()
    for step in (3, -3, 4):
        arrival(step, h).wait_recv()
        arrival(step, 1 - h).wait_recv()
    own.wait()
    for copy in copies + relays:
        copy.wait_send()
    group = iota((48, 128), 1) >> 4
    for half in range(2):
        for i in range(8):
            block = got[(0 - i) % 8, half]
            for p in range(1, 8):
                block = jnp.where(group == p, got[(p - i) % 8, half], block)
            out_ref[half * 8 + i] = block
    nonzero = (out_ref[...].reshape(768, 128) != 0.0).astype(F32).astype(BF16)
    found = dot_nt(jnp.ones((8, 128), F32).astype(BF16), nonzero).astype(BF16)
    row, block = iota((768, 128), 0), iota((768, 128), 1)
    first = ((block >> 6) * 8 + (block & 7)) * 48 + ((block >> 3) & 7) * 6
    pick = ((row == first) | (row == first + 1)).astype(F32).astype(BF16)
    used_ref[...] = dot_nn(found, pick).astype(I32)


def column_tables(z, kernel_ref, phase_ref):
    l_row, lane = iota((128, 128), 0), iota((128, 128), 1)
    l_val = (l_row & 63) + (l_row >> 6) * 512 + z * 64
    phase_ref[0], phase_ref[1] = cis(l_val * lane, G)
    zr, zi = cis(l_val, G)
    kern = kernel_ref[...]
    pr = jnp.broadcast_to(kern[7:8], (128, 128))
    pi = jnp.zeros((128, 128), F32)
    for s in range(6, -1, -1):
        pr, pi = cmul(pr, pi, zr, zi)
        pr = pr + kern[s : s + 1]
    phase_ref[2] = pr
    phase_ref[3] = pi


def row_tables(matrix_ref, twiddle_ref):
    row, lane = iota((128, 128), 0), iota((128, 128), 1)
    fc, fs = cis(row * lane, 128)
    for quarter, value in ((0, fc), (1, -fs), (2, fs), (3, fc)):
        down, right = (quarter >> 1) * 128, (quarter & 1) * 128
        for part, half in enumerate(split2(value)):
            matrix_ref[part, down : down + 128, right : right + 128] = half
    tr, ti = cis(row, G)
    ar, ai = tr, ti
    for k0 in range(1, 8):
        twiddle_ref[k0 - 1, 0] = ar
        twiddle_ref[k0 - 1, 1] = ai
        if k0 < 7:
            ar, ai = cmul(ar, ai, tr, ti)


def bin_tables(core, bins, turned, onehot_ref, hit_ref, counts_ref):
    full = jnp.concatenate([bins[...].astype(F32), jnp.zeros((64, 128), F32)], axis=0)
    turned[...] = pltpu.roll(full, core * 64, 1).T
    row128, high_row, lane8 = iota((128, 128), 0), iota((4, 128), 0), iota((8, 128), 1)
    for k0 in range(4):
        ours = turned[pl.ds(k0, 8, stride=8), :]
        other = turned[pl.ds(k0 + 4, 8, stride=8), :]
        both = jnp.where(lane8 < 64, ours, pltpu.roll(other, 64, 1)).astype(I32)
        for sub in range(8):
            found = both[sub : sub + 1]
            at = slice(128 * (8 * k0 + sub), 128 * (8 * k0 + sub) + 128)
            onehot_ref[:, at] = (row128 == (found & 127)).astype(F32).astype(BF16)
            hit_ref[:, at] = ((found >> 7) == high_row).astype(F32)
    counts_ref[...] = dot_nt(hit_ref[...].astype(BF16), onehot_ref[...])


def gather_call(*args):
    return pl.pallas_call(
        gather_kernel,
        out_shape=(
            jax.ShapeDtypeStruct((16, 48, 128), F32),
            jax.ShapeDtypeStruct((8, 128), F32),
            jax.ShapeDtypeStruct((8, 128), I32),
            jax.ShapeDtypeStruct((4, 128, 128), F32),
            jax.ShapeDtypeStruct((2, 256, 256), BF16),
            jax.ShapeDtypeStruct((7, 2, 128, 128), F32),
            jax.ShapeDtypeStruct((128, 4096), BF16),
            jax.ShapeDtypeStruct((4, 4096), F32),
            jax.ShapeDtypeStruct((4, 128), F32),
        ),
        in_specs=[pl.BlockSpec(memory_space=pltpu.HBM)] * 8,
        out_specs=(VMEM_SPEC,) * 9,
        scratch_shapes=[
            pltpu.VMEM((2, 48, 128), F32),
            pltpu.VMEM((8, 2, 48, 128), F32),
            pltpu.VMEM((64, 128), I32),
            pltpu.VMEM((128, 128), F32),
            pltpu.VMEM((1, 2), I32),
            pltpu.VMEM((2, 2, SLOTS), F32),
            pltpu.VMEM((2, 1, SLOTS), I32),
            pltpu.VMEM((2, SLOTS), I32),
            pltpu.VMEM((2, SLOTS), I32),
            pltpu.VMEM((2, 2, SLOTS), I32),
            pltpu.SemaphoreType.DMA((9,)),
            pltpu.SemaphoreType.DMA((8, 2)),
            pltpu.SemaphoreType.DMA((6,)),
            pltpu.SemaphoreType.DMA,
            pltpu.SemaphoreType.DMA((8,)),
        ],
        compiler_params=pltpu.CompilerParams(
            collective_id=0, has_side_effects=True, vmem_limit_bytes=LIMIT
        ),
    )(*(pltpu.with_memory_space_constraint(x, pltpu.HBM) for x in args))


def grid_kernel(merged, used_ref, phase_ref, kernel_ref, grid_ref, wbuf, rbuf, used, order, sem):
    copy = pltpu.make_async_copy(used_ref, used, sem)
    copy.start()
    sub = iota((8, 128), 0)
    ct_r, ct_i = cis(sub * iota((8, 128), 1), 8)
    grid_ref[...] = jnp.zeros_like(grid_ref)
    for slot in range(2):
        for i in range(GROUP):
            rbuf[slot, i, 80:160, 128:256] = jnp.zeros((80, 128), BF16)
    copy.wait()

    def list_step(b, n):
        order[n] = b
        return n + jnp.where(used[0, b] > 0, 1, 0)

    total = lax.fori_loop(0, BLOCKS, list_step, 0, unroll=16)
    for i in range(GROUP):
        order[total + i] = BLOCKS

    def build(bid, slot, i):
        which = ((bid >> 6) & 1) * 8 + (bid & 7)
        first = ((bid >> 3) & 7) * 6
        keep = jnp.where(bid < BLOCKS, 1.0, 0.0)

        def field(index):
            return jnp.broadcast_to(merged[which, pl.ds(first + index, 1), :], (8, 128))

        v = field(3).astype(I32)
        index_d = v & 127
        index_c = v >> 7
        index_u = field(4).astype(I32)
        index_v = field(5).astype(I32)
        w = field(2).astype(I32)
        cr = take_lanes(ct_r, index_c)
        ci = take_lanes(ct_i, index_c)
        cr, ci = cmul(cr, ci, field(0) * keep, field(1) * keep)
        for pair in range(8):
            res, ims = [], []
            for lg in (2 * pair, 2 * pair + 1):
                at = slice(8 * lg, 8 * lg + 8)
                er = take_lanes(phase_ref[0, at], index_d)
                ei = take_lanes(phase_ref[1, at], index_d)
                qr = take_lanes(phase_ref[2, at], index_v)
                qi = take_lanes(phase_ref[3, at], index_v)
                ar, ai = cmul(er, ei, qr, qi)
                ar, ai = cmul(ar, ai, cr, ci)
                res.append(ar)
                ims.append(ai)
            for base, values in ((0, res), (128, ims)):
                hi, lo = split2(jnp.concatenate(values, axis=0))
                at = slice(base + 16 * pair, base + 16 * pair + 16)
                wbuf[slot, i, at, 0:128] = hi
                wbuf[slot, i, at, 128:256] = lo
        taps = take_lanes(kernel_ref[...], index_u)
        turned = jnp.take_along_axis(taps, (sub - w) & 7, axis=0, mode="promise_in_bounds")
        high = turned.astype(BF16).astype(F32)
        low = turned - high
        down = (w - sub + 7) >> 3
        zero = jnp.zeros((8, 128), F32)
        for pair in range(5):
            his, los = [], []
            for k in (2 * pair, 2 * pair + 1):
                hit = down == k
                his.append(jnp.where(hit, high, zero))
                los.append(jnp.where(hit, low, zero))
            hi = jnp.concatenate(his, axis=0).astype(BF16)
            at = slice(16 * pair, 16 * pair + 16)
            rbuf[slot, i, at, 0:128] = hi
            rbuf[slot, i, at, 128:256] = hi
            at = slice(80 + 16 * pair, 80 + 16 * pair + 16)
            rbuf[slot, i, at, 0:128] = jnp.concatenate(los, axis=0).astype(BF16)

    def place(bid, slot, i):
        res = dot_nt(rbuf[slot, i], wbuf[slot, i])
        start = pl.multiple_of(((bid >> 2) & 15) * 64, 64)
        grid_ref[pl.ds(start, 80), :] += res[:80] + res[80:]

    def fill(it, slot):
        bids = tuple(order[GROUP * it + i] for i in range(GROUP))
        for i in range(GROUP):
            build(bids[i], slot, i)
        return bids

    def step(it, before):
        slot = it & 1
        for i in range(GROUP):
            place(before[i], 1 - slot, i)
        return fill(it, slot)

    rounds = (total + GROUP - 1) // GROUP
    last = lax.fori_loop(1, rounds, step, fill(0, 0))
    slot = jnp.where(rounds > 0, (rounds - 1) & 1, 0)
    for i in range(GROUP):
        place(last[i], slot, i)


def grid_call(merged, used, phase, kernel_t):
    return pl.pallas_call(
        grid_kernel,
        out_shape=jax.ShapeDtypeStruct((1040, 256), F32),
        in_specs=[VMEM_SPEC] * 4,
        out_specs=VMEM_SPEC,
        scratch_shapes=[
            pltpu.VMEM((2, GROUP, 256, 256), BF16),
            pltpu.VMEM((2, GROUP, 160, 256), BF16),
            pltpu.SMEM((8, 128), I32),
            pltpu.SMEM((BLOCKS + GROUP,), I32),
            pltpu.SemaphoreType.DMA,
        ],
        compiler_params=pltpu.CompilerParams(vmem_limit_bytes=LIMIT),
    )(merged, used, phase, kernel_t)


def tail_kernel(
    grid_ref, matrix_ref, tw_ref, onehot, hit_ref, counts, power_ref, spectrum_ref,
    bh_ref, bl_ref, left, piece, partner, summed, landed, counts_in, counts_z, counts_plane, totals, totals_in, totals_z, totals_plane,
    s_pair, r_pair, s_sum, r_sum, s_count, r_count, s_total, r_total, s_countz, r_countz, s_totalz, r_totalz,
):
    h, z = places()
    freq = lax.axis_index("freq")
    quad, core = freq // 2, freq % 2
    me = h * 16 + freq
    me_pair = h * 8 + quad

    def plane_device(index):
        return {"freq": index % 16, "base": (index // 16) * 8 + z}

    def column_device(index):
        return {"freq": freq, "base": h * 8 + index}

    barrier = pltpu.get_barrier_semaphore()

    def greet_plane(k, _):
        pl.semaphore_signal(barrier, 1, device_id=plane_device((me + k) % 32), device_id_type=MESH)
        return 0

    def greet_column(k, _):
        pl.semaphore_signal(barrier, 1, device_id=column_device((z + k) % 8), device_id_type=MESH)
        return 0

    lax.fori_loop(1, 32, greet_plane, 0)
    lax.fori_loop(1, 8, greet_column, 0)

    root = math.sqrt(0.5)
    slot_of = (0, 2, 4, 6, 1, 3, 5, 7)
    for rows in range(8):
        u = [
            (
                grid_ref[128 * a + 16 * rows : 128 * a + 16 * rows + 16, 0:128],
                grid_ref[128 * a + 16 * rows : 128 * a + 16 * rows + 16, 128:256],
            )
            for a in range(8)
        ]

        def add(x, y):
            return x[0] + y[0], x[1] + y[1]

        def sub2(x, y):
            return x[0] - y[0], x[1] - y[1]

        def four(a, b, c, d):
            s, t = add(a, c), sub2(a, c)
            p, q = add(b, d), sub2(b, d)
            mq = (q[1], -q[0])
            return add(s, p), add(t, mq), sub2(s, p), sub2(t, mq)

        even = four(u[0], u[2], u[4], u[6])
        odd = four(u[1], u[3], u[5], u[7])
        o1 = ((odd[1][0] + odd[1][1]) * root, (odd[1][1] - odd[1][0]) * root)
        o2 = (odd[2][1], -odd[2][0])
        o3 = ((odd[3][1] - odd[3][0]) * root, -(odd[3][0] + odd[3][1]) * root)
        odd = (odd[0], o1, o2, o3)
        spectrum = [add(even[k], odd[k]) for k in range(4)] + [sub2(even[k], odd[k]) for k in range(4)]
        at = slice(16 * rows, 16 * rows + 16)
        for k0 in range(8):
            xr, xi = spectrum[k0]
            if k0:
                xr, xi = cmul(xr, xi, tw_ref[k0 - 1, 0, at], tw_ref[k0 - 1, 1, at])
            col = slice(128 * slot_of[k0], 128 * slot_of[k0] + 128)
            for base, value in ((0, xr), (128, xi)):
                hi, lo = split2(value)
                bh_ref[base + 16 * rows : base + 16 * rows + 16, col] = hi
                bl_ref[base + 16 * rows : base + 16 * rows + 16, col] = lo
    pl.semaphore_wait(barrier, 38)

    def plane_copy(k, buf, slots, s, r):
        peer = (me + k) % 32
        return pltpu.make_async_remote_copy(
            src_ref=buf, dst_ref=slots.at[me], send_sem=s.at[k], recv_sem=r.at[me],
            device_id=plane_device(peer), device_id_type=MESH,
        )

    def column_copy(k, buf, slots, s, r):
        peer = (z + k) % 8
        return pltpu.make_async_remote_copy(
            src_ref=buf, dst_ref=slots.at[z], send_sem=s.at[k], recv_sem=r.at[z],
            device_id=column_device(peer), device_id_type=MESH,
        )

    def start_all(count, make, *args):
        def body(k, _):
            make(k, *args).start()
            return 0

        lax.fori_loop(1, count, body, 0)

    def wait_plane(buf, slots, s, r):
        def body(k, total):
            source = (me + k) % 32
            pltpu.make_async_remote_copy(
                src_ref=buf, dst_ref=slots.at[source], send_sem=s.at[k], recv_sem=r.at[source],
                device_id=plane_device(source), device_id_type=MESH,
            ).wait_recv()
            return total + slots[source]

        return lax.fori_loop(1, 32, body, buf[...])

    def wait_column(buf, slots, s, r):
        def body(k, total):
            source = (z + k) % 8
            pltpu.make_async_remote_copy(
                src_ref=buf, dst_ref=slots.at[source], send_sem=s.at[k], recv_sem=r.at[source],
                device_id=column_device(source), device_id_type=MESH,
            ).wait_recv()
            return total + slots[source]

        return lax.fori_loop(1, 8, body, buf[...])

    def sent_all(count, make, *args):
        def body(k, _):
            make(k, *args).wait_send()
            return 0

        lax.fori_loop(1, count, body, 0)

    plane_counts = (counts, counts_in, s_count, r_count)
    start_all(32, plane_copy, *plane_counts)

    def pair_copy(k0):
        return pltpu.make_async_remote_copy(
            src_ref=piece.at[1 - core, k0], dst_ref=partner.at[k0], send_sem=s_pair.at[k0], recv_sem=r_pair.at[k0],
            device_id={"freq": quad * 2 + 1 - core}, device_id_type=MESH,
        )

    low_half = iota((128, 128), 1) < 64
    for k0 in range(4):
        col = slice(256 * k0, 256 * k0 + 256)
        full = dot_nn(matrix_ref[0], bh_ref[:, col]) + dot_nn(matrix_ref[0], bl_ref[:, col]) + dot_nn(matrix_ref[1], bh_ref[:, col])
        power = (full[:128] * full[:128] + full[128:] * full[128:]) * NORM
        pa, pb = power[:, :128], power[:, 128:]
        ra, rb = pltpu.roll(pa, 64, 1), pltpu.roll(pb, 64, 1)
        for side, block in ((0, jnp.where(low_half, pa, rb)), (1, jnp.where(low_half, ra, pb))):
            block = block.reshape(8, 2, 8, 128)
            for cc in range(2):
                piece[cc, k0, side] = block[:, cc]
        pair_copy(k0).start()
    for k0 in range(4):
        pair_copy(k0).wait_recv()
        for side in range(2):
            for q in range(8):
                summed[side * 8 + q, k0] = piece[core, k0, side, q] + partner[k0, side, q]

    def sum_copy(k):
        peer = (me_pair + k) % 16
        return pltpu.make_async_remote_copy(
            src_ref=summed.at[peer], dst_ref=landed.at[me_pair], send_sem=s_sum.at[k], recv_sem=r_sum.at[me_pair],
            device_id={"freq": (peer % 8) * 2 + core, "base": (peer // 8) * 8 + z}, device_id_type=MESH,
        )

    start_all(16, sum_copy)
    counts_plane[...] = wait_plane(*plane_counts)
    column_counts = (counts_plane, counts_z, s_countz, r_countz)
    start_all(8, column_copy, *column_counts)

    def wait_sum(k, total):
        source = (me_pair + k) % 16
        pltpu.make_async_remote_copy(
            src_ref=summed.at[source], dst_ref=landed.at[source], send_sem=s_sum.at[k], recv_sem=r_sum.at[source],
            device_id={"freq": (source % 8) * 2 + core, "base": (source // 8) * 8 + z}, device_id_type=MESH,
        ).wait_recv()
        return total + landed[source]

    total = lax.fori_loop(1, 16, wait_sum, summed[me_pair])
    for k0 in range(4):
        for sub in range(8):
            at = slice(128 * (8 * k0 + sub), 128 * (8 * k0 + sub) + 128)
            hit = hit_ref[:, at]
            value = total[k0][sub : sub + 1]
            p0 = value.astype(BF16).astype(F32)
            p1 = (value - p0).astype(BF16).astype(F32)
            left[0:4, at] = hit * p0
            left[4:8, at] = hit * p1
            left[8:12, at] = hit * (value - p0 - p1)
    got = dot_nt(left[...].astype(BF16), onehot[...])
    totals[...] = got[0:4] + got[4:8] + got[8:12]
    plane_totals = (totals, totals_in, s_total, r_total)
    start_all(32, plane_copy, *plane_totals)
    for k0 in range(8):
        half = (k0 // 4) * 64
        power_ref[pl.ds(k0, 8, stride=8), :] = total[k0 % 4][:, half : half + 64]
    all_counts = wait_column(*column_counts)
    totals_plane[...] = wait_plane(*plane_totals)
    column_totals = (totals_plane, totals_z, s_totalz, r_totalz)
    start_all(8, column_copy, *column_totals)
    sent_all(32, plane_copy, *plane_counts)
    sent_all(8, column_copy, *column_counts)
    sent_all(16, sum_copy)
    sent_all(32, plane_copy, *plane_totals)
    for k0 in range(4):
        pair_copy(k0).wait_send()
    spectrum_ref[...] = wait_column(*column_totals) / all_counts
    sent_all(8, column_copy, *column_totals)


def tail_call(grid, matrix, twiddle, onehot, hit, counts):
    dma = pltpu.SemaphoreType.DMA
    small = (4, 128)
    return pl.pallas_call(
        tail_kernel,
        out_shape=(jax.ShapeDtypeStruct((64, 64), F32), jax.ShapeDtypeStruct((4, 128), F32)),
        in_specs=[VMEM_SPEC] * 6,
        out_specs=(VMEM_SPEC,) * 2,
        scratch_shapes=[
            pltpu.VMEM((256, 1024), BF16),
            pltpu.VMEM((256, 1024), BF16),
            pltpu.VMEM((16, 4096), F32),
            pltpu.VMEM((2, 4, 2, 8, 8, 128), F32),
            pltpu.VMEM((4, 2, 8, 8, 128), F32),
            pltpu.VMEM((16, 4, 8, 128), F32),
            pltpu.VMEM((16, 4, 8, 128), F32),
            pltpu.VMEM((32,) + small, F32),
            pltpu.VMEM((8,) + small, F32),
            pltpu.VMEM(small, F32),
            pltpu.VMEM(small, F32),
            pltpu.VMEM((32,) + small, F32),
            pltpu.VMEM((8,) + small, F32),
            pltpu.VMEM(small, F32),
            dma((4,)), dma((4,)), dma((16,)), dma((16,)),
            dma((32,)), dma((32,)), dma((32,)), dma((32,)),
            dma((8,)), dma((8,)), dma((8,)), dma((8,)),
        ],
        compiler_params=pltpu.CompilerParams(
            collective_id=1, has_side_effects=True, vmem_limit_bytes=LIMIT
        ),
    )(grid, matrix, twiddle, onehot, hit, counts)


def per_device(visibility, tile_of, u_within, v_cell, kernel_index, kernel, live_count, bin_map):
    merged, kernel_rows, used, phase, matrix, twiddle, onehot, hit, counts = gather_call(
        live_count.T,
        visibility,
        tile_of.transpose(0, 2, 1),
        u_within,
        v_cell,
        kernel_index,
        kernel.T,
        bin_map,
    )
    grid = grid_call(merged, used, phase, kernel_rows)
    power, spectrum = tail_call(grid, matrix, twiddle, onehot, hit, counts)
    return power, spectrum.reshape(NBINS)


def solution(mesh):
    return jax.shard_map(
        per_device,
        mesh=mesh,
        in_specs=(
            P(None, "freq", "base"),
            P("freq", "base", None),
            P("freq", "base"),
            P("freq", "base"),
            P(None, "freq", "base"),
            P(),
            P("freq", "base"),
            P("base", None),
        ),
        out_specs=(P("freq", "base"), P()),
        check_vma=False,
    )
```

```python
import functools
import math

import jax
import jax.numpy as jnp
from jax import lax
from jax.experimental import pallas as pl
from jax.experimental.pallas import tpu as pltpu
from jax.sharding import PartitionSpec as P

G = 1024
NBINS = 512
KW = 8
OVER = 128
SLOTS = 512
TILES = 16
BLOCKS = 128
GROUP = 4
CHUNK = 16
F32 = jnp.float32
BF16 = jnp.bfloat16
I32 = jnp.int32
MESH = pl.DeviceIdType.MESH
VMEM_SPEC = pl.BlockSpec(memory_space=pltpu.VMEM)
LIMIT = 16 * 1024 * 1024
NORM = 1.0 / (32 * 8192)


def iota(shape, dim):
    return lax.broadcasted_iota(I32, shape, dim)


def cis(phase, period):
    phase = phase & (period - 1)
    phase = jnp.where(phase >= period // 2, phase - period, phase)
    angle = phase.astype(F32) * (2.0 * math.pi / period)
    return jnp.cos(angle), -jnp.sin(angle)


def cmul(ar, ai, br, bi):
    return ar * br - ai * bi, ar * bi + ai * br


def split2(x):
    hi = x.astype(BF16)
    return hi, (x - hi.astype(F32)).astype(BF16)


def dot_nt(a, b):
    return lax.dot_general(a, b, (((1,), (1,)), ((), ())), preferred_element_type=F32)


def dot_nn(a, b):
    return lax.dot_general(a, b, (((1,), (0,)), ((), ())), preferred_element_type=F32)


def take_lanes(table, index):
    return jnp.take_along_axis(table, index, axis=1, mode="promise_in_bounds")


def bin_channel(ch, z, vis_ref, tile_ref, within_ref, vcell_ref, kidx_ref, live, upper):
    tile = tile_ref[ch]
    lane = iota((1, SLOTS), 1)
    is_live = lane < live
    member = (tile == iota((TILES, SLOTS), 0)) & is_live
    before = dot_nn(member.astype(BF16), upper)
    rank = jnp.sum(jnp.where(member, before, 0.0), axis=0, keepdims=True).astype(I32)
    block = tile * 4 + (rank >> 4)
    position = (block >> 3) * 128 + (((block & 7) + z) & 7) * 16 + (rank & 15)
    position = jnp.where(is_live, position, -1)
    row = jnp.minimum(within_ref[ch : ch + 1, :], (G - KW) - tile * 64)
    column = vcell_ref[ch : ch + 1, :]
    parts = []
    for part in range(2):
        value = vis_ref[part, ch : ch + 1, :]
        for _ in range(3):
            piece = value.astype(BF16).astype(F32)
            parts.append(piece)
            value = value - piece
    parts += [
        row.astype(F32),
        (column >> 3).astype(F32),
        (column & 7).astype(F32),
        kidx_ref[0, ch : ch + 1, :].astype(F32),
        kidx_ref[1, ch : ch + 1, :].astype(F32),
        jnp.ones((1, SLOTS), F32),
        jnp.zeros((4, SLOTS), F32),
    ]
    payload = jnp.concatenate(parts, axis=0).astype(BF16)
    out = []
    for part in range(4):
        place = (iota((256, SLOTS), 0) + part * 256 == position).astype(F32).astype(BF16)
        got = dot_nt(payload, place)
        out.append(
            jnp.concatenate(
                [
                    got[0:1] + got[1:2] + got[2:3],
                    got[3:4] + got[4:5] + got[5:6],
                    got[6:7],
                    got[7:8] * 8.0 + got[8:9],
                    got[9:10],
                    got[10:11],
                    got[11:12],
                    jnp.zeros((1, 256), F32),
                ],
                axis=0,
            )
        )
    return out


def places():
    base = lax.axis_index("base")
    return base // 8, base % 8


def gather_kernel(
    live_hbm,
    vis_hbm,
    tile_hbm,
    within_hbm,
    vcell_hbm,
    kidx_hbm,
    kernel_hbm,
    bins_ref,
    out_ref,
    kernel_ref,
    used_ref,
    phase_ref,
    matrix_ref,
    twiddle_ref,
    onehot_ref,
    hit_ref,
    counts_ref,
    packed,
    got,
    bins,
    turned,
    live_ref,
    vis_ref,
    tile_ref,
    within_ref,
    vcell_ref,
    kidx_ref,
    send,
    land,
    relay,
    local,
    fetched,
):
    inputs = (
        (live_hbm, live_ref),
        (tile_hbm, tile_ref),
        (vis_hbm, vis_ref),
        (within_hbm, within_ref),
        (vcell_hbm, vcell_ref),
        (kidx_hbm, kidx_ref),
        (kernel_hbm, kernel_ref),
    )
    loads = [
        pltpu.make_async_copy(source, place, fetched.at[index])
        for index, (source, place) in enumerate(inputs)
    ]
    for load in loads:
        load.start()
    h, z = places()
    freq = lax.axis_index("freq")
    at = pl.multiple_of((freq // 2) * 128, 128)
    fetch = pltpu.make_async_copy(bins_ref.at[:, pl.ds(at, 128)], bins, fetched.at[7])
    fetch.start()
    hops = (1, -1, 2, -2)

    def device(side, step):
        return {"base": side * 8 + (z + step + 8) % 8}

    barrier = pltpu.get_barrier_semaphore()
    for step in hops:
        pl.semaphore_signal(barrier, 1, device_id=device(h, step), device_id_type=MESH)
    for step in (0,) + hops:
        pl.semaphore_signal(barrier, 1, device_id=device(1 - h, step), device_id_type=MESH)

    upper = (iota((SLOTS, SLOTS), 0) < iota((SLOTS, SLOTS), 1)).astype(F32).astype(BF16)
    for load in loads:
        load.wait()
    for ch in range(2):
        live = live_ref[0:1, ch : ch + 1]
        parts = bin_channel(
            ch, z, vis_ref, tile_ref, within_ref, vcell_ref, kidx_ref, live, upper
        )
        for index, part in enumerate(parts):
            packed[ch, 12 * index : 12 * index + 6] = part[:6, :128]
            packed[ch, 12 * index + 6 : 12 * index + 12] = part[:6, 128:]
    pl.semaphore_wait(barrier, 9)

    def direct(side, step, number):
        return pltpu.make_async_remote_copy(
            src_ref=packed.at[side],
            dst_ref=got.at[z, h],
            send_sem=send.at[number],
            recv_sem=land.at[z, h],
            device_id=device(side, step),
            device_id_type=MESH,
        )

    def arrival(step, side):
        zz = (z + step + 8) % 8
        return pltpu.make_async_remote_copy(
            src_ref=got.at[zz, side],
            dst_ref=got.at[zz, side],
            send_sem=send.at[0],
            recv_sem=land.at[zz, side],
            device_id=device(1 - h, 0),
            device_id_type=MESH,
        )

    copies = []
    for step in (2, -2):
        copies.append(direct(1 - h, step, len(copies)))
        copies.append(direct(h, step, len(copies)))
    for step in (1, -1):
        copies.append(direct(1 - h, step, len(copies)))
        copies.append(direct(h, step, len(copies)))
    copies.append(direct(1 - h, 0, len(copies)))
    for copy in copies:
        copy.start()
    own = pltpu.make_async_copy(packed.at[h], got.at[z, h], local)
    own.start()

    column_tables(z, kernel_ref, phase_ref)
    row_tables(matrix_ref, twiddle_ref)
    fetch.wait()
    bin_tables(freq % 2, bins, turned, onehot_ref, hit_ref, counts_ref)

    relays = []

    def pass_on(source, side, step):
        zz = (z + source + 8) % 8
        copy = pltpu.make_async_remote_copy(
            src_ref=got.at[zz, side],
            dst_ref=got.at[zz, side],
            send_sem=relay.at[len(relays)],
            recv_sem=land.at[zz, side],
            device_id=device(h, step),
            device_id_type=MESH,
        )
        copy.start()
        relays.append(copy)

    arrival(-2, h).wait_recv()
    pass_on(-2, h, 2)
    pass_on(-2, h, 1)
    arrival(2, h).wait_recv()
    pass_on(2, h, -1)
    arrival(2, 1 - h).wait_recv()
    pass_on(2, 1 - h, -2)
    pass_on(2, 1 - h, -1)
    arrival(-2, 1 - h).wait_recv()
    pass_on(-2, 1 - h, 1)
    for step in (1, -1):
        arrival(step, h).wait_recv()
        arrival(step, 1 - h).wait_recv()
    arrival(0, 1 - h).wait_recv()
    for step in (3, -3, 4):
        arrival(step, h).wait_recv()
        arrival(step, 1 - h).wait_recv()
    own.wait()
    for copy in copies + relays:
        copy.wait_send()
    group = iota((48, 128), 1) >> 4
    for half in range(2):
        for i in range(8):
            block = got[(0 - i) % 8, half]
            for p in range(1, 8):
                block = jnp.where(group == p, got[(p - i) % 8, half], block)
            out_ref[half * 8 + i] = block
    nonzero = (out_ref[...].reshape(768, 128) != 0.0).astype(F32).astype(BF16)
    found = dot_nt(jnp.ones((8, 128), F32).astype(BF16), nonzero).astype(BF16)
    row, block = iota((768, 128), 0), iota((768, 128), 1)
    first = ((block >> 6) * 8 + (block & 7)) * 48 + ((block >> 3) & 7) * 6
    pick = ((row == first) | (row == first + 1)).astype(F32).astype(BF16)
    used_ref[...] = dot_nn(found, pick).astype(I32)


def column_tables(z, kernel_ref, phase_ref):
    l_row, lane = iota((128, 128), 0), iota((128, 128), 1)
    l_val = (l_row & 63) + (l_row >> 6) * 512 + z * 64
    phase_ref[0], phase_ref[1] = cis(l_val * lane, G)
    zr, zi = cis(l_val, G)
    kern = kernel_ref[...]
    pr = jnp.broadcast_to(kern[7:8], (128, 128))
    pi = jnp.zeros((128, 128), F32)
    for s in range(6, -1, -1):
        pr, pi = cmul(pr, pi, zr, zi)
        pr = pr + kern[s : s + 1]
    phase_ref[2] = pr
    phase_ref[3] = pi


def row_tables(matrix_ref, twiddle_ref):
    row, lane = iota((128, 128), 0), iota((128, 128), 1)
    fc, fs = cis(row * lane, 128)
    for quarter, value in ((0, fc), (1, -fs), (2, fs), (3, fc)):
        down, right = (quarter >> 1) * 128, (quarter & 1) * 128
        for part, half in enumerate(split2(value)):
            matrix_ref[part, down : down + 128, right : right + 128] = half
    tr, ti = cis(row, G)
    ar, ai = tr, ti
    for k0 in range(1, 8):
        twiddle_ref[k0 - 1, 0] = ar
        twiddle_ref[k0 - 1, 1] = ai
        if k0 < 7:
            ar, ai = cmul(ar, ai, tr, ti)


def bin_tables(core, bins, turned, onehot_ref, hit_ref, counts_ref):
    full = jnp.concatenate([bins[...].astype(F32), jnp.zeros((64, 128), F32)], axis=0)
    turned[...] = pltpu.roll(full, core * 64, 1).T
    row128, high_row, lane8 = iota((128, 128), 0), iota((4, 128), 0), iota((8, 128), 1)
    for k0 in range(4):
        ours = turned[pl.ds(k0, 8, stride=8), :]
        other = turned[pl.ds(k0 + 4, 8, stride=8), :]
        both = jnp.where(lane8 < 64, ours, pltpu.roll(other, 64, 1)).astype(I32)
        for sub in range(8):
            found = both[sub : sub + 1]
            at = slice(128 * (8 * k0 + sub), 128 * (8 * k0 + sub) + 128)
            onehot_ref[:, at] = (row128 == (found & 127)).astype(F32).astype(BF16)
            hit_ref[:, at] = ((found >> 7) == high_row).astype(F32)
    counts_ref[...] = dot_nt(hit_ref[...].astype(BF16), onehot_ref[...])


def gather_call(*args):
    return pl.pallas_call(
        gather_kernel,
        out_shape=(
            jax.ShapeDtypeStruct((16, 48, 128), F32),
            jax.ShapeDtypeStruct((8, 128), F32),
            jax.ShapeDtypeStruct((8, 128), I32),
            jax.ShapeDtypeStruct((4, 128, 128), F32),
            jax.ShapeDtypeStruct((2, 256, 256), BF16),
            jax.ShapeDtypeStruct((7, 2, 128, 128), F32),
            jax.ShapeDtypeStruct((128, 4096), BF16),
            jax.ShapeDtypeStruct((4, 4096), F32),
            jax.ShapeDtypeStruct((4, 128), F32),
        ),
        in_specs=[pl.BlockSpec(memory_space=pltpu.HBM)] * 8,
        out_specs=(VMEM_SPEC,) * 9,
        scratch_shapes=[
            pltpu.VMEM((2, 48, 128), F32),
            pltpu.VMEM((8, 2, 48, 128), F32),
            pltpu.VMEM((64, 128), I32),
            pltpu.VMEM((128, 128), F32),
            pltpu.VMEM((1, 2), I32),
            pltpu.VMEM((2, 2, SLOTS), F32),
            pltpu.VMEM((2, 1, SLOTS), I32),
            pltpu.VMEM((2, SLOTS), I32),
            pltpu.VMEM((2, SLOTS), I32),
            pltpu.VMEM((2, 2, SLOTS), I32),
            pltpu.SemaphoreType.DMA((9,)),
            pltpu.SemaphoreType.DMA((8, 2)),
            pltpu.SemaphoreType.DMA((6,)),
            pltpu.SemaphoreType.DMA,
            pltpu.SemaphoreType.DMA((8,)),
        ],
        compiler_params=pltpu.CompilerParams(
            collective_id=0, has_side_effects=True, vmem_limit_bytes=LIMIT
        ),
    )(*(pltpu.with_memory_space_constraint(x, pltpu.HBM) for x in args))


def grid_kernel(merged, used_ref, phase_ref, kernel_ref, grid_ref, wbuf, rbuf, used, order, sem):
    copy = pltpu.make_async_copy(used_ref, used, sem)
    copy.start()
    sub = iota((8, 128), 0)
    ct_r, ct_i = cis(sub * iota((8, 128), 1), 8)
    grid_ref[...] = jnp.zeros_like(grid_ref)
    for slot in range(2):
        for i in range(GROUP):
            rbuf[slot, i, 80:160, 128:256] = jnp.zeros((80, 128), BF16)
    copy.wait()

    def list_step(b, n):
        order[n] = b
        return n + jnp.where(used[0, b] > 0, 1, 0)

    total = lax.fori_loop(0, BLOCKS, list_step, 0, unroll=16)
    for i in range(GROUP):
        order[total + i] = BLOCKS

    def build(bid, slot, i):
        which = ((bid >> 6) & 1) * 8 + (bid & 7)
        first = ((bid >> 3) & 7) * 6
        keep = jnp.where(bid < BLOCKS, 1.0, 0.0)

        def field(index):
            return jnp.broadcast_to(merged[which, pl.ds(first + index, 1), :], (8, 128))

        v = field(3).astype(I32)
        index_d = v & 127
        index_c = v >> 7
        index_u = field(4).astype(I32)
        index_v = field(5).astype(I32)
        w = field(2).astype(I32)
        cr = take_lanes(ct_r, index_c)
        ci = take_lanes(ct_i, index_c)
        cr, ci = cmul(cr, ci, field(0) * keep, field(1) * keep)
        for chunk in range(0, 16, CHUNK):
            rows = [slice(8 * lg, 8 * lg + 8) for lg in range(chunk, chunk + CHUNK)]
            phase = [(take_lanes(phase_ref[0, at], index_d), take_lanes(phase_ref[1, at], index_d)) for at in rows]
            taps = [(take_lanes(phase_ref[2, at], index_v), take_lanes(phase_ref[3, at], index_v)) for at in rows]
            done = [cmul(*cmul(*a, *b), cr, ci) for a, b in zip(phase, taps)]
            for pair in range(CHUNK // 2):
                for part in range(2):
                    hi, lo = split2(jnp.concatenate([done[2 * pair][part], done[2 * pair + 1][part]], axis=0))
                    start = part * 128 + 8 * chunk + 16 * pair
                    wbuf[slot, i, start : start + 16, 0:128] = hi
                    wbuf[slot, i, start : start + 16, 128:256] = lo
        taps = take_lanes(kernel_ref[...], index_u)
        turned = jnp.take_along_axis(taps, (sub - w) & 7, axis=0, mode="promise_in_bounds")
        high = turned.astype(BF16).astype(F32)
        low = turned - high
        down = (w - sub + 7) >> 3
        zero = jnp.zeros((8, 128), F32)
        for pair in range(5):
            his, los = [], []
            for k in (2 * pair, 2 * pair + 1):
                hit = down == k
                his.append(jnp.where(hit, high, zero))
                los.append(jnp.where(hit, low, zero))
            hi = jnp.concatenate(his, axis=0).astype(BF16)
            at = slice(16 * pair, 16 * pair + 16)
            rbuf[slot, i, at, 0:128] = hi
            rbuf[slot, i, at, 128:256] = hi
            at = slice(80 + 16 * pair, 80 + 16 * pair + 16)
            rbuf[slot, i, at, 0:128] = jnp.concatenate(los, axis=0).astype(BF16)

    def place(bid, slot, i):
        res = dot_nt(rbuf[slot, i], wbuf[slot, i])
        start = pl.multiple_of(((bid >> 2) & 15) * 64, 64)
        grid_ref[pl.ds(start, 80), :] += res[:80] + res[80:]

    def fill(it, slot):
        bids = tuple(order[GROUP * it + i] for i in range(GROUP))
        for i in range(GROUP):
            build(bids[i], slot, i)
        return bids

    def step(it, before):
        slot = it & 1
        for i in range(GROUP):
            place(before[i], 1 - slot, i)
        return fill(it, slot)

    rounds = (total + GROUP - 1) // GROUP
    last = lax.fori_loop(1, rounds, step, fill(0, 0))
    slot = jnp.where(rounds > 0, (rounds - 1) & 1, 0)
    for i in range(GROUP):
        place(last[i], slot, i)


def grid_call(merged, used, phase, kernel_t):
    return pl.pallas_call(
        grid_kernel,
        out_shape=jax.ShapeDtypeStruct((1040, 256), F32),
        in_specs=[VMEM_SPEC] * 4,
        out_specs=VMEM_SPEC,
        scratch_shapes=[
            pltpu.VMEM((2, GROUP, 256, 256), BF16),
            pltpu.VMEM((2, GROUP, 160, 256), BF16),
            pltpu.SMEM((8, 128), I32),
            pltpu.SMEM((BLOCKS + GROUP,), I32),
            pltpu.SemaphoreType.DMA,
        ],
        compiler_params=pltpu.CompilerParams(vmem_limit_bytes=LIMIT),
    )(merged, used, phase, kernel_t)


def tail_kernel(
    grid_ref, matrix_ref, tw_ref, onehot, hit_ref, counts, power_ref, spectrum_ref,
    bh_ref, bl_ref, left, piece, partner, summed, landed, counts_in, counts_z, counts_plane,
    totals, totals_in, totals_z, totals_plane, sems,
):
    h, z = places()
    freq = lax.axis_index("freq")
    quad, core = freq // 2, freq % 2
    me = h * 16 + freq
    me_pair = h * 8 + quad
    far_first = (4, 3, 5, 2, 6, 1, 7)

    def chip(index, to_core):
        return {"freq": (index % 8) * 2 + to_core, "base": (index // 8) * 8 + z}

    def column(step, to_core):
        return {"freq": quad * 2 + to_core, "base": h * 8 + (z + step) % 8}

    barrier = pltpu.get_barrier_semaphore()

    def greet(device):
        pl.semaphore_signal(barrier, 1, device_id=device, device_id_type=MESH)

    for step in far_first:
        for to_core in range(2):
            greet(column(step, to_core))
    for k in range(1, 16):
        for to_core in range(2):
            greet(chip((me_pair + k) % 16, to_core))
    greet(chip(me_pair, 1 - core))

    root = math.sqrt(0.5)
    slot_of = (0, 2, 4, 6, 1, 3, 5, 7)
    for rows in range(8):
        u = [
            (
                grid_ref[128 * a + 16 * rows : 128 * a + 16 * rows + 16, 0:128],
                grid_ref[128 * a + 16 * rows : 128 * a + 16 * rows + 16, 128:256],
            )
            for a in range(8)
        ]

        def add(x, y):
            return x[0] + y[0], x[1] + y[1]

        def sub2(x, y):
            return x[0] - y[0], x[1] - y[1]

        def four(a, b, c, d):
            s, t = add(a, c), sub2(a, c)
            p, q = add(b, d), sub2(b, d)
            mq = (q[1], -q[0])
            return add(s, p), add(t, mq), sub2(s, p), sub2(t, mq)

        even = four(u[0], u[2], u[4], u[6])
        odd = four(u[1], u[3], u[5], u[7])
        o1 = ((odd[1][0] + odd[1][1]) * root, (odd[1][1] - odd[1][0]) * root)
        o2 = (odd[2][1], -odd[2][0])
        o3 = ((odd[3][1] - odd[3][0]) * root, -(odd[3][0] + odd[3][1]) * root)
        odd = (odd[0], o1, o2, o3)
        spectrum = [add(even[k], odd[k]) for k in range(4)] + [sub2(even[k], odd[k]) for k in range(4)]
        at = slice(16 * rows, 16 * rows + 16)
        for k0 in range(8):
            xr, xi = spectrum[k0]
            if k0:
                xr, xi = cmul(xr, xi, tw_ref[k0 - 1, 0, at], tw_ref[k0 - 1, 1, at])
            col = slice(128 * slot_of[k0], 128 * slot_of[k0] + 128)
            for base, value in ((0, xr), (128, xi)):
                hi, lo = split2(value)
                bh_ref[base + 16 * rows : base + 16 * rows + 16, col] = hi
                bl_ref[base + 16 * rows : base + 16 * rows + 16, col] = lo
    low_half = iota((128, 128), 1) < 64
    for k0 in range(4):
        col = slice(256 * k0, 256 * k0 + 256)
        full = dot_nn(matrix_ref[0], bh_ref[:, col]) + dot_nn(matrix_ref[0], bl_ref[:, col]) + dot_nn(matrix_ref[1], bh_ref[:, col])
        power = (full[:128] * full[:128] + full[128:] * full[128:]) * NORM
        pa, pb = power[:, :128], power[:, 128:]
        ra, rb = pltpu.roll(pa, 64, 1), pltpu.roll(pb, 64, 1)
        for side, block in ((0, jnp.where(low_half, pa, rb)), (1, jnp.where(low_half, ra, pb))):
            block = block.reshape(8, 2, 8, 128)
            for cc in range(2):
                piece[cc, k0, side] = block[:, cc]

    pl.semaphore_wait(barrier, 45)

    def remote(source, target, number, device):
        return pltpu.make_async_remote_copy(
            src_ref=source, dst_ref=target, send_sem=sems.at[2 * number], recv_sem=sems.at[2 * number + 1],
            device_id=device, device_id_type=MESH,
        )

    def whole(ref, count, number):
        return remote(ref.at[0:count], ref.at[0:count], number, chip(me_pair, 1 - core))

    pair = remote(piece.at[1 - core], partner, 0, chip(me_pair, 1 - core))
    pair.start()

    def plane_send(buf, slots, number):
        @pl.when(core == 0)
        def _():
            remote(buf, slots.at[me], number, chip(me_pair, 1)).start()

        for k in range(1, 16):
            remote(buf, slots.at[me], number, chip((me_pair + k) % 16, 1)).start()

    def plane_sum(buf, slots, result, number):
        slots[me] = buf[...]
        whole(slots, 31, number).wait_recv()
        total = slots[0]
        for index in range(1, 32):
            total = total + slots[index]
        result[...] = total

    def column_send(buf, slots, number):
        for step in far_first:
            for to_core in range(2):
                remote(buf, slots.at[z], number, column(step, to_core)).start()
        remote(buf, slots.at[z], number, chip(me_pair, 0)).start()

    def column_sum(buf, slots, number):
        @pl.when(core == 0)
        def _():
            whole(slots, 8, number).wait_recv()

        @pl.when(core == 1)
        def _():
            slots[z] = buf[...]
            whole(slots, 7, number).wait_recv()

        total = slots[0]
        for index in range(1, 8):
            total = total + slots[index]
        return total

    def plane_sent(slots, number):
        @pl.when(core == 0)
        def _():
            whole(slots, 16, number).wait_send()

        @pl.when(core == 1)
        def _():
            whole(slots, 15, number).wait_send()

    plane_send(counts, counts_in, 2)
    pair.wait_recv()
    for k0 in range(4):
        for side in range(2):
            for q in range(8):
                summed[side * 8 + q, k0] = piece[core, k0, side, q] + partner[k0, side, q]
    for k in range(1, 16):
        peer = (me_pair + k) % 16
        remote(summed.at[peer], landed.at[me_pair], 1, chip(peer, core)).start()
    landed[me_pair] = summed[me_pair]

    @pl.when(core == 1)
    def _():
        plane_sum(counts, counts_in, counts_plane, 2)
        column_send(counts_plane, counts_z, 3)

    whole(landed, 15, 1).wait_recv()
    total = landed[0]
    for index in range(1, 16):
        total = total + landed[index]
    for k0 in range(4):
        for sub in range(8):
            at = slice(128 * (8 * k0 + sub), 128 * (8 * k0 + sub) + 128)
            hit = hit_ref[:, at]
            value = total[k0][sub : sub + 1]
            p0 = value.astype(BF16).astype(F32)
            p1 = (value - p0).astype(BF16).astype(F32)
            left[0:4, at] = hit * p0
            left[4:8, at] = hit * p1
            left[8:12, at] = hit * (value - p0 - p1)
            left[12:16, at] = jnp.zeros((4, 128), F32)
    got = dot_nt(left[...].astype(BF16), onehot[...])
    totals[...] = got[0:4] + got[4:8] + got[8:12]
    plane_send(totals, totals_in, 4)
    for k0 in range(8):
        half = (k0 // 4) * 64
        power_ref[pl.ds(k0, 8, stride=8), :] = total[k0 % 4][:, half : half + 64]
    all_counts = column_sum(counts_plane, counts_z, 3)

    @pl.when(core == 1)
    def _():
        plane_sum(totals, totals_in, totals_plane, 4)
        column_send(totals_plane, totals_z, 5)

    pair.wait_send()
    whole(landed, 15, 1).wait_send()
    plane_sent(counts_in, 2)
    plane_sent(totals_in, 4)

    @pl.when(core == 1)
    def _():
        whole(counts_in, 15, 3).wait_send()

    spectrum_ref[...] = column_sum(totals_plane, totals_z, 5) / all_counts

    @pl.when(core == 1)
    def _():
        whole(totals_in, 15, 5).wait_send()


def tail_call(grid, matrix, twiddle, onehot, hit, counts):
    small = (4, 128)
    return pl.pallas_call(
        tail_kernel,
        out_shape=(jax.ShapeDtypeStruct((64, 64), F32), jax.ShapeDtypeStruct((4, 128), F32)),
        in_specs=[VMEM_SPEC] * 6,
        out_specs=(VMEM_SPEC,) * 2,
        scratch_shapes=[
            pltpu.VMEM((256, 1024), BF16),
            pltpu.VMEM((256, 1024), BF16),
            pltpu.VMEM((16, 4096), F32),
            pltpu.VMEM((2, 4, 2, 8, 8, 128), F32),
            pltpu.VMEM((4, 2, 8, 8, 128), F32),
            pltpu.VMEM((16, 4, 8, 128), F32),
            pltpu.VMEM((16, 4, 8, 128), F32),
            pltpu.VMEM((32,) + small, F32),
            pltpu.VMEM((8,) + small, F32),
            pltpu.VMEM(small, F32),
            pltpu.VMEM(small, F32),
            pltpu.VMEM((32,) + small, F32),
            pltpu.VMEM((8,) + small, F32),
            pltpu.VMEM(small, F32),
            pltpu.SemaphoreType.DMA((12,)),
        ],
        compiler_params=pltpu.CompilerParams(
            collective_id=1, has_side_effects=True, vmem_limit_bytes=LIMIT
        ),
    )(grid, matrix, twiddle, onehot, hit, counts)


def per_device(visibility, tile_of, u_within, v_cell, kernel_index, kernel, live_count, bin_map):
    merged, kernel_rows, used, phase, matrix, twiddle, onehot, hit, counts = gather_call(
        live_count.T,
        visibility,
        tile_of.transpose(0, 2, 1),
        u_within,
        v_cell,
        kernel_index,
        kernel.T,
        bin_map,
    )
    grid = grid_call(merged, used, phase, kernel_rows)
    power, spectrum = tail_call(grid, matrix, twiddle, onehot, hit, counts)
    return power, spectrum.reshape(NBINS)


def solution(mesh):
    return jax.shard_map(
        per_device,
        mesh=mesh,
        in_specs=(
            P(None, "freq", "base"),
            P("freq", "base", None),
            P("freq", "base"),
            P("freq", "base"),
            P(None, "freq", "base"),
            P(),
            P("freq", "base"),
            P("base", None),
        ),
        out_specs=(P("freq", "base"), P()),
        check_vma=False,
    )
```

```python
import functools
import math

import jax
import jax.numpy as jnp
from jax import lax
from jax.experimental import pallas as pl
from jax.experimental.pallas import tpu as pltpu
from jax.sharding import PartitionSpec as P

G = 1024
NBINS = 512
KW = 8
OVER = 128
SLOTS = 512
TILES = 16
BLOCKS = 128
GROUP = 4
F32 = jnp.float32
BF16 = jnp.bfloat16
I32 = jnp.int32
MESH = pl.DeviceIdType.MESH
VMEM_SPEC = pl.BlockSpec(memory_space=pltpu.VMEM)
LIMIT = 16 * 1024 * 1024
NORM = 1.0 / (32 * 8192)


def iota(shape, dim):
    return lax.broadcasted_iota(I32, shape, dim)


def cis(phase, period):
    phase = phase & (period - 1)
    phase = jnp.where(phase >= period // 2, phase - period, phase)
    angle = phase.astype(F32) * (2.0 * math.pi / period)
    return jnp.cos(angle), -jnp.sin(angle)


def cmul(ar, ai, br, bi):
    return ar * br - ai * bi, ar * bi + ai * br


def split2(x):
    hi = x.astype(BF16)
    return hi, (x - hi.astype(F32)).astype(BF16)


def dot_nt(a, b):
    return lax.dot_general(a, b, (((1,), (1,)), ((), ())), preferred_element_type=F32)


def dot_nn(a, b):
    return lax.dot_general(a, b, (((1,), (0,)), ((), ())), preferred_element_type=F32)


def take_lanes(table, index):
    return jnp.take_along_axis(table, index, axis=1, mode="promise_in_bounds")


def bin_channel(ch, z, vis_ref, tile_ref, within_ref, vcell_ref, kidx_ref, live, upper):
    tile = tile_ref[ch]
    lane = iota((1, SLOTS), 1)
    is_live = lane < live
    member = (tile == iota((TILES, SLOTS), 0)) & is_live
    before = dot_nn(member.astype(BF16), upper)
    rank = jnp.sum(jnp.where(member, before, 0.0), axis=0, keepdims=True).astype(I32)
    block = tile * 4 + (rank >> 4)
    position = (block >> 3) * 128 + (((block & 7) + z) & 7) * 16 + (rank & 15)
    position = jnp.where(is_live, position, -1)
    row = jnp.minimum(within_ref[ch : ch + 1, :], (G - KW) - tile * 64)
    column = vcell_ref[ch : ch + 1, :]
    parts = []
    for part in range(2):
        value = vis_ref[part, ch : ch + 1, :]
        for _ in range(3):
            piece = value.astype(BF16).astype(F32)
            parts.append(piece)
            value = value - piece
    parts += [
        row.astype(F32),
        (column >> 3).astype(F32),
        (column & 7).astype(F32),
        kidx_ref[0, ch : ch + 1, :].astype(F32),
        kidx_ref[1, ch : ch + 1, :].astype(F32),
        jnp.ones((1, SLOTS), F32),
        jnp.zeros((4, SLOTS), F32),
    ]
    payload = jnp.concatenate(parts, axis=0).astype(BF16)
    out = []
    for part in range(4):
        place = (iota((256, SLOTS), 0) + part * 256 == position).astype(F32).astype(BF16)
        got = dot_nt(payload, place)
        out.append(
            jnp.concatenate(
                [
                    got[0:1] + got[1:2] + got[2:3],
                    got[3:4] + got[4:5] + got[5:6],
                    got[6:7],
                    got[7:8] * 8.0 + got[8:9],
                    got[9:10],
                    got[10:11],
                    got[11:12],
                    jnp.zeros((1, 256), F32),
                ],
                axis=0,
            )
        )
    return out


def places():
    base = lax.axis_index("base")
    return base // 8, base % 8


def gather_kernel(
    live_hbm,
    vis_hbm,
    tile_hbm,
    within_hbm,
    vcell_hbm,
    kidx_hbm,
    kernel_hbm,
    bins_ref,
    out_ref,
    kernel_ref,
    used_ref,
    phase_ref,
    matrix_ref,
    twiddle_ref,
    onehot_ref,
    hit_ref,
    counts_ref,
    packed,
    got,
    bins,
    turned,
    live_ref,
    vis_ref,
    tile_ref,
    within_ref,
    vcell_ref,
    kidx_ref,
    send,
    land,
    relay,
    local,
    fetched,
):
    inputs = (
        (live_hbm, live_ref),
        (tile_hbm, tile_ref),
        (vis_hbm, vis_ref),
        (within_hbm, within_ref),
        (vcell_hbm, vcell_ref),
        (kidx_hbm, kidx_ref),
        (kernel_hbm, kernel_ref),
    )
    loads = [
        pltpu.make_async_copy(source, place, fetched.at[index])
        for index, (source, place) in enumerate(inputs)
    ]
    for load in loads:
        load.start()
    h, z = places()
    freq = lax.axis_index("freq")
    at = pl.multiple_of((freq // 2) * 128, 128)
    fetch = pltpu.make_async_copy(bins_ref.at[:, pl.ds(at, 128)], bins, fetched.at[7])
    fetch.start()
    hops = (1, -1, 2, -2)

    def device(side, step):
        return {"base": side * 8 + (z + step + 8) % 8}

    barrier = pltpu.get_barrier_semaphore()
    for step in hops:
        pl.semaphore_signal(barrier, 1, device_id=device(h, step), device_id_type=MESH)
    for step in (0, 2, -2):
        pl.semaphore_signal(barrier, 1, device_id=device(1 - h, step), device_id_type=MESH)

    upper = (iota((SLOTS, SLOTS), 0) < iota((SLOTS, SLOTS), 1)).astype(F32).astype(BF16)
    for load in loads:
        load.wait()
    for ch in range(2):
        live = live_ref[0:1, ch : ch + 1]
        parts = bin_channel(
            ch, z, vis_ref, tile_ref, within_ref, vcell_ref, kidx_ref, live, upper
        )
        for index, part in enumerate(parts):
            packed[ch, 12 * index : 12 * index + 6] = part[:6, :128]
            packed[ch, 12 * index + 6 : 12 * index + 12] = part[:6, 128:]
    pl.semaphore_wait(barrier, 7)

    def direct(side, step, number):
        return pltpu.make_async_remote_copy(
            src_ref=packed.at[side],
            dst_ref=got.at[z, h],
            send_sem=send.at[number],
            recv_sem=land.at[z, h],
            device_id=device(side, step),
            device_id_type=MESH,
        )

    def arrival(step, side):
        zz = (z + step + 8) % 8
        return pltpu.make_async_remote_copy(
            src_ref=got.at[zz, side],
            dst_ref=got.at[zz, side],
            send_sem=send.at[0],
            recv_sem=land.at[zz, side],
            device_id=device(1 - h, 0),
            device_id_type=MESH,
        )

    copies = []
    for step in (2, -2):
        copies.append(direct(1 - h, step, len(copies)))
        copies.append(direct(h, step, len(copies)))
    copies.insert(2, direct(1 - h, 0, 4))
    for step in (1, -1):
        copies.append(direct(h, step, len(copies)))
    for copy in copies:
        copy.start()
    own = pltpu.make_async_copy(packed.at[h], got.at[z, h], local)
    own.start()

    column_tables(z, kernel_ref, phase_ref)
    row_tables(matrix_ref, twiddle_ref)
    fetch.wait()
    bin_tables(freq % 2, bins, turned, onehot_ref, hit_ref, counts_ref)

    relays = []

    def pass_on(source, side, step):
        zz = (z + source + 8) % 8
        copy = pltpu.make_async_remote_copy(
            src_ref=got.at[zz, side],
            dst_ref=got.at[zz, side],
            send_sem=relay.at[len(relays)],
            recv_sem=land.at[zz, side],
            device_id=device(h, step),
            device_id_type=MESH,
        )
        copy.start()
        relays.append(copy)

    arrival(0, 1 - h).wait_recv()
    pass_on(0, 1 - h, 1)
    pass_on(0, 1 - h, -1)
    arrival(-2, h).wait_recv()
    pass_on(-2, h, 2)
    pass_on(-2, h, 1)
    arrival(2, h).wait_recv()
    pass_on(2, h, -1)
    arrival(2, 1 - h).wait_recv()
    pass_on(2, 1 - h, -2)
    pass_on(2, 1 - h, -1)
    arrival(-2, 1 - h).wait_recv()
    pass_on(-2, 1 - h, 1)
    for step in (1, -1):
        arrival(step, h).wait_recv()
        arrival(step, 1 - h).wait_recv()
    for step in (3, -3, 4):
        arrival(step, h).wait_recv()
        arrival(step, 1 - h).wait_recv()
    own.wait()
    for copy in copies + relays:
        copy.wait_send()
    group = iota((48, 128), 1) >> 4
    for half in range(2):
        for i in range(8):
            block = got[(0 - i) % 8, half]
            for p in range(1, 8):
                block = jnp.where(group == p, got[(p - i) % 8, half], block)
            out_ref[half * 8 + i] = block
    nonzero = (out_ref[...].reshape(768, 128) != 0.0).astype(F32).astype(BF16)
    found = dot_nt(jnp.ones((8, 128), F32).astype(BF16), nonzero).astype(BF16)
    row, block = iota((768, 128), 0), iota((768, 128), 1)
    first = ((block >> 6) * 8 + (block & 7)) * 48 + ((block >> 3) & 7) * 6
    pick = ((row == first) | (row == first + 1)).astype(F32).astype(BF16)
    used_ref[...] = dot_nn(found, pick).astype(I32)


def column_tables(z, kernel_ref, phase_ref):
    l_row = iota((128, 128), 0)
    zr, zi = cis((l_row & 63) + (l_row >> 6) * 512 + z * 64, G)
    kern = kernel_ref[...]
    pr = jnp.broadcast_to(kern[7:8], (128, 128))
    pi = jnp.zeros((128, 128), F32)
    for s in range(6, -1, -1):
        pr, pi = cmul(pr, pi, zr, zi)
        pr = pr + kern[s : s + 1]
    phase_ref[0] = pr
    phase_ref[1] = pi


def row_tables(matrix_ref, twiddle_ref):
    row, lane = iota((128, 128), 0), iota((128, 128), 1)
    fc, fs = cis(row * lane, 128)
    for quarter, value in ((0, fc), (1, -fs), (2, fs), (3, fc)):
        down, right = (quarter >> 1) * 128, (quarter & 1) * 128
        for part, half in enumerate(split2(value)):
            matrix_ref[part, down : down + 128, right : right + 128] = half
    tr, ti = cis(row, G)
    ar, ai = tr, ti
    for k0 in range(1, 8):
        twiddle_ref[k0 - 1, 0] = ar
        twiddle_ref[k0 - 1, 1] = ai
        if k0 < 7:
            ar, ai = cmul(ar, ai, tr, ti)


def bin_tables(core, bins, turned, onehot_ref, hit_ref, counts_ref):
    full = jnp.concatenate([bins[...].astype(F32), jnp.zeros((64, 128), F32)], axis=0)
    turned[...] = pltpu.roll(full, core * 64, 1).T
    row128, high_row, lane8 = iota((128, 128), 0), iota((4, 128), 0), iota((8, 128), 1)
    for k0 in range(4):
        ours = turned[pl.ds(k0, 8, stride=8), :]
        other = turned[pl.ds(k0 + 4, 8, stride=8), :]
        both = jnp.where(lane8 < 64, ours, pltpu.roll(other, 64, 1)).astype(I32)
        for sub in range(8):
            found = both[sub : sub + 1]
            at = slice(128 * (8 * k0 + sub), 128 * (8 * k0 + sub) + 128)
            onehot_ref[:, at] = (row128 == (found & 127)).astype(F32).astype(BF16)
            hit_ref[:, at] = ((found >> 7) == high_row).astype(F32)
    counts_ref[...] = dot_nt(hit_ref[...].astype(BF16), onehot_ref[...])


def gather_call(*args):
    return pl.pallas_call(
        gather_kernel,
        out_shape=(
            jax.ShapeDtypeStruct((16, 48, 128), F32),
            jax.ShapeDtypeStruct((8, 128), F32),
            jax.ShapeDtypeStruct((8, 128), I32),
            jax.ShapeDtypeStruct((2, 128, 128), F32),
            jax.ShapeDtypeStruct((2, 256, 256), BF16),
            jax.ShapeDtypeStruct((7, 2, 128, 128), F32),
            jax.ShapeDtypeStruct((128, 4096), BF16),
            jax.ShapeDtypeStruct((4, 4096), F32),
            jax.ShapeDtypeStruct((4, 128), F32),
        ),
        in_specs=[pl.BlockSpec(memory_space=pltpu.HBM)] * 8,
        out_specs=(VMEM_SPEC,) * 9,
        scratch_shapes=[
            pltpu.VMEM((2, 48, 128), F32),
            pltpu.VMEM((8, 2, 48, 128), F32),
            pltpu.VMEM((64, 128), I32),
            pltpu.VMEM((128, 128), F32),
            pltpu.VMEM((1, 2), I32),
            pltpu.VMEM((2, 2, SLOTS), F32),
            pltpu.VMEM((2, 1, SLOTS), I32),
            pltpu.VMEM((2, SLOTS), I32),
            pltpu.VMEM((2, SLOTS), I32),
            pltpu.VMEM((2, 2, SLOTS), I32),
            pltpu.SemaphoreType.DMA((7,)),
            pltpu.SemaphoreType.DMA((8, 2)),
            pltpu.SemaphoreType.DMA((8,)),
            pltpu.SemaphoreType.DMA,
            pltpu.SemaphoreType.DMA((8,)),
        ],
        compiler_params=pltpu.CompilerParams(
            collective_id=0, has_side_effects=True, vmem_limit_bytes=LIMIT
        ),
    )(*(pltpu.with_memory_space_constraint(x, pltpu.HBM) for x in args))


def grid_kernel(merged, used_ref, taps_ref, kernel_ref, grid_ref, wbuf_a, rbuf_a, wbuf_b, rbuf_b, rows, used, order, sem):
    copy = pltpu.make_async_copy(used_ref, used, sem)
    copy.start()
    sub = iota((8, 128), 0)
    lane = iota((8, 128), 1)
    _, z = places()
    sd_r, sd_i = cis(sub * lane, G)
    sc_r, sc_i = cis(sub * lane, 8)
    gd_r, gd_i = cis((z * 64 + sub * 8) * lane, G)
    gc_r, gc_i = cis((z * 64 + sub * 8) * lane, 8)
    grid_ref[...] = jnp.zeros_like(grid_ref)
    wbufs, rbufs = (wbuf_a, wbuf_b), (rbuf_a, rbuf_b)
    for i in range(GROUP):
        for ref in rbufs:
            ref[i, 80:160, 128:256] = jnp.zeros((80, 128), BF16)
    copy.wait()

    def list_step(b, n):
        order[n] = b
        return n + jnp.where(used[0, b] > 0, 1, 0)

    total = lax.fori_loop(0, BLOCKS, list_step, 0, unroll=16)
    for i in range(2 * GROUP):
        order[total + i] = BLOCKS

    def build(bid, slot, i):
        which = ((bid >> 6) & 1) * 8 + (bid & 7)
        first = ((bid >> 3) & 7) * 6
        keep = jnp.where(bid < BLOCKS, 1.0, 0.0)

        def field(index):
            return jnp.broadcast_to(merged[which, pl.ds(first + index, 1), :], (8, 128))

        v = field(3).astype(I32)
        index_d = v & 127
        index_c = v >> 7
        index_u = field(4).astype(I32)
        index_v = field(5).astype(I32)
        w = field(2).astype(I32)
        near = [take_lanes(t, index_d) for t in (gd_r, gd_i, sd_r, sd_i)]
        wide = [take_lanes(t, index_c) for t in (gc_r, gc_i, sc_r, sc_i)]
        group = cmul(*near[:2], *wide[:2])
        inner = cmul(*cmul(*near[2:], *wide[2:]), field(0) * keep, field(1) * keep)
        sign = (1 - 2 * (v & 1)).astype(F32)
        rows[i, 0] = group[0]
        rows[i, 1] = group[1]
        for pair in range(4):
            done = []
            for g in (2 * pair, 2 * pair + 1):
                ar, ai = cmul(jnp.broadcast_to(rows[i, 0, g : g + 1], (8, 128)), jnp.broadcast_to(rows[i, 1, g : g + 1], (8, 128)), *inner)
                low, high = slice(8 * g, 8 * g + 8), slice(64 + 8 * g, 72 + 8 * g)
                one = cmul(ar, ai, take_lanes(taps_ref[0, low], index_v), take_lanes(taps_ref[1, low], index_v))
                two = cmul(ar * sign, ai * sign, take_lanes(taps_ref[0, high], index_v), take_lanes(taps_ref[1, high], index_v))
                done.append(one + two)
            for part, start in enumerate((0, 128, 64, 192)):
                hi, lo = split2(jnp.concatenate([done[0][part], done[1][part]], axis=0))
                at = slice(start + 16 * pair, start + 16 * pair + 16)
                wbufs[slot][i, at, 0:128] = hi
                wbufs[slot][i, at, 128:256] = lo
        taps = take_lanes(kernel_ref[...], index_u)
        turned = jnp.take_along_axis(taps, (sub - w) & 7, axis=0, mode="promise_in_bounds")
        high = turned.astype(BF16).astype(F32)
        low = turned - high
        down = (w - sub + 7) >> 3
        zero = jnp.zeros((8, 128), F32)
        for pair in range(5):
            his, los = [], []
            for k in (2 * pair, 2 * pair + 1):
                hit = down == k
                his.append(jnp.where(hit, high, zero))
                los.append(jnp.where(hit, low, zero))
            hi = jnp.concatenate(his, axis=0).astype(BF16)
            at = slice(16 * pair, 16 * pair + 16)
            rbufs[slot][i, at, 0:128] = hi
            rbufs[slot][i, at, 128:256] = hi
            at = slice(80 + 16 * pair, 80 + 16 * pair + 16)
            rbufs[slot][i, at, 0:128] = jnp.concatenate(los, axis=0).astype(BF16)

    def place(bid, slot, i):
        res = dot_nt(rbufs[slot][i], wbufs[slot][i])
        start = pl.multiple_of(((bid >> 2) & 15) * 64, 64)
        grid_ref[pl.ds(start, 80), :] += res[:80] + res[80:]

    def fill(it, slot):
        bids = tuple(order[GROUP * it + i] for i in range(GROUP))
        for i in range(GROUP):
            build(bids[i], slot, i)
        return bids

    def step(it, before):
        first = tuple(order[2 * GROUP * it + i] for i in range(GROUP))
        second = tuple(order[2 * GROUP * it + GROUP + i] for i in range(GROUP))
        for i in range(GROUP):
            place(before[i], 1, i)
            build(first[i], 0, i)
        for i in range(GROUP):
            place(first[i], 0, i)
            build(second[i], 1, i)
        return second

    rounds = (total + 2 * GROUP - 1) // (2 * GROUP)
    for i in range(GROUP):
        rbufs[1][i, 0:80, 0:256] = jnp.zeros((80, 256), BF16)
        rbufs[1][i, 80:160, 0:128] = jnp.zeros((80, 128), BF16)
        wbufs[1][i] = jnp.zeros((256, 256), BF16)
    last = lax.fori_loop(0, rounds, step, (jnp.int32(BLOCKS),) * GROUP)
    for i in range(GROUP):
        place(last[i], 1, i)


def grid_call(merged, used, phase, kernel_t):
    return pl.pallas_call(
        grid_kernel,
        out_shape=jax.ShapeDtypeStruct((1040, 256), F32),
        in_specs=[VMEM_SPEC] * 4,
        out_specs=VMEM_SPEC,
        scratch_shapes=[
            pltpu.VMEM((GROUP, 256, 256), BF16),
            pltpu.VMEM((GROUP, 160, 256), BF16),
            pltpu.VMEM((GROUP, 256, 256), BF16),
            pltpu.VMEM((GROUP, 160, 256), BF16),
            pltpu.VMEM((GROUP, 2, 8, 128), F32),
            pltpu.SMEM((8, 128), I32),
            pltpu.SMEM((BLOCKS + 2 * GROUP,), I32),
            pltpu.SemaphoreType.DMA,
        ],
        compiler_params=pltpu.CompilerParams(vmem_limit_bytes=LIMIT),
    )(merged, used, phase, kernel_t)


def tail_kernel(
    grid_ref, matrix_ref, tw_ref, onehot, hit_ref, counts, power_ref, spectrum_ref,
    bh_ref, bl_ref, left, piece, partner, summed, landed, counts_in, counts_z, counts_plane,
    totals, totals_in, totals_z, totals_plane, sems,
):
    h, z = places()
    freq = lax.axis_index("freq")
    quad, core = freq // 2, freq % 2
    me = h * 16 + freq
    me_pair = h * 8 + quad
    far_first = (4, 3, 5, 2, 6, 1, 7)

    def chip(index, to_core):
        return {"freq": (index % 8) * 2 + to_core, "base": (index // 8) * 8 + z}

    def column(step, to_core):
        return {"freq": quad * 2 + to_core, "base": h * 8 + (z + step) % 8}

    barrier = pltpu.get_barrier_semaphore()

    def greet(device):
        pl.semaphore_signal(barrier, 1, device_id=device, device_id_type=MESH)

    for step in far_first:
        for to_core in range(2):
            greet(column(step, to_core))
    for k in range(1, 16):
        for to_core in range(2):
            greet(chip((me_pair + k) % 16, to_core))
    greet(chip(me_pair, 1 - core))

    root = math.sqrt(0.5)
    slot_of = (0, 2, 4, 6, 1, 3, 5, 7)
    for rows in range(8):
        u = [
            (
                grid_ref[128 * a + 16 * rows : 128 * a + 16 * rows + 16, 0:128],
                grid_ref[128 * a + 16 * rows : 128 * a + 16 * rows + 16, 128:256],
            )
            for a in range(8)
        ]

        def add(x, y):
            return x[0] + y[0], x[1] + y[1]

        def sub2(x, y):
            return x[0] - y[0], x[1] - y[1]

        def four(a, b, c, d):
            s, t = add(a, c), sub2(a, c)
            p, q = add(b, d), sub2(b, d)
            mq = (q[1], -q[0])
            return add(s, p), add(t, mq), sub2(s, p), sub2(t, mq)

        even = four(u[0], u[2], u[4], u[6])
        odd = four(u[1], u[3], u[5], u[7])
        o1 = ((odd[1][0] + odd[1][1]) * root, (odd[1][1] - odd[1][0]) * root)
        o2 = (odd[2][1], -odd[2][0])
        o3 = ((odd[3][1] - odd[3][0]) * root, -(odd[3][0] + odd[3][1]) * root)
        odd = (odd[0], o1, o2, o3)
        spectrum = [add(even[k], odd[k]) for k in range(4)] + [sub2(even[k], odd[k]) for k in range(4)]
        at = slice(16 * rows, 16 * rows + 16)
        for k0 in range(8):
            xr, xi = spectrum[k0]
            if k0:
                xr, xi = cmul(xr, xi, tw_ref[k0 - 1, 0, at], tw_ref[k0 - 1, 1, at])
            col = slice(128 * slot_of[k0], 128 * slot_of[k0] + 128)
            for base, value in ((0, xr), (128, xi)):
                hi, lo = split2(value)
                bh_ref[base + 16 * rows : base + 16 * rows + 16, col] = hi
                bl_ref[base + 16 * rows : base + 16 * rows + 16, col] = lo
    low_half = iota((128, 128), 1) < 64
    for k0 in range(4):
        col = slice(256 * k0, 256 * k0 + 256)
        full = dot_nn(matrix_ref[0], bh_ref[:, col]) + dot_nn(matrix_ref[0], bl_ref[:, col]) + dot_nn(matrix_ref[1], bh_ref[:, col])
        power = (full[:128] * full[:128] + full[128:] * full[128:]) * NORM
        pa, pb = power[:, :128], power[:, 128:]
        ra, rb = pltpu.roll(pa, 64, 1), pltpu.roll(pb, 64, 1)
        for side, block in ((0, jnp.where(low_half, pa, rb)), (1, jnp.where(low_half, ra, pb))):
            block = block.reshape(8, 2, 8, 128)
            for cc in range(2):
                piece[cc, k0, side] = block[:, cc]

    pl.semaphore_wait(barrier, 45)

    def remote(source, target, number, device):
        return pltpu.make_async_remote_copy(
            src_ref=source, dst_ref=target, send_sem=sems.at[2 * number], recv_sem=sems.at[2 * number + 1],
            device_id=device, device_id_type=MESH,
        )

    def whole(ref, count, number):
        return remote(ref.at[0:count], ref.at[0:count], number, chip(me_pair, 1 - core))

    pair = remote(piece.at[1 - core], partner, 0, chip(me_pair, 1 - core))
    pair.start()

    def plane_send(buf, slots, number):
        @pl.when(core == 0)
        def _():
            remote(buf, slots.at[me], number, chip(me_pair, 1)).start()

        for k in range(1, 16):
            remote(buf, slots.at[me], number, chip((me_pair + k) % 16, 1)).start()

    def plane_sum(buf, slots, result, number):
        slots[me] = buf[...]
        whole(slots, 31, number).wait_recv()
        total = slots[0]
        for index in range(1, 32):
            total = total + slots[index]
        result[...] = total

    def column_send(buf, slots, number):
        for step in far_first:
            for to_core in range(2):
                remote(buf, slots.at[z], number, column(step, to_core)).start()
        remote(buf, slots.at[z], number, chip(me_pair, 0)).start()

    def column_sum(buf, slots, number):
        @pl.when(core == 0)
        def _():
            whole(slots, 8, number).wait_recv()

        @pl.when(core == 1)
        def _():
            slots[z] = buf[...]
            whole(slots, 7, number).wait_recv()

        total = slots[0]
        for index in range(1, 8):
            total = total + slots[index]
        return total

    def plane_sent(slots, number):
        @pl.when(core == 0)
        def _():
            whole(slots, 16, number).wait_send()

        @pl.when(core == 1)
        def _():
            whole(slots, 15, number).wait_send()

    plane_send(counts, counts_in, 2)
    pair.wait_recv()
    for k0 in range(4):
        for side in range(2):
            for q in range(8):
                summed[side * 8 + q, k0] = piece[core, k0, side, q] + partner[k0, side, q]
    for k in range(1, 16):
        peer = (me_pair + k) % 16
        remote(summed.at[peer], landed.at[me_pair], 1, chip(peer, core)).start()
    landed[me_pair] = summed[me_pair]

    @pl.when(core == 1)
    def _():
        plane_sum(counts, counts_in, counts_plane, 2)
        column_send(counts_plane, counts_z, 3)

    whole(landed, 15, 1).wait_recv()
    total = landed[0]
    for index in range(1, 16):
        total = total + landed[index]
    for k0 in range(4):
        for sub in range(8):
            at = slice(128 * (8 * k0 + sub), 128 * (8 * k0 + sub) + 128)
            hit = hit_ref[:, at]
            value = total[k0][sub : sub + 1]
            p0 = value.astype(BF16).astype(F32)
            p1 = (value - p0).astype(BF16).astype(F32)
            left[0:4, at] = hit * p0
            left[4:8, at] = hit * p1
            left[8:12, at] = hit * (value - p0 - p1)
            left[12:16, at] = jnp.zeros((4, 128), F32)
    got = dot_nt(left[...].astype(BF16), onehot[...])
    totals[...] = got[0:4] + got[4:8] + got[8:12]
    plane_send(totals, totals_in, 4)
    for k0 in range(8):
        half = (k0 // 4) * 64
        power_ref[pl.ds(k0, 8, stride=8), :] = total[k0 % 4][:, half : half + 64]
    all_counts = column_sum(counts_plane, counts_z, 3)

    @pl.when(core == 1)
    def _():
        plane_sum(totals, totals_in, totals_plane, 4)
        column_send(totals_plane, totals_z, 5)

    pair.wait_send()
    whole(landed, 15, 1).wait_send()
    plane_sent(counts_in, 2)
    plane_sent(totals_in, 4)

    @pl.when(core == 1)
    def _():
        whole(counts_in, 15, 3).wait_send()

    spectrum_ref[...] = column_sum(totals_plane, totals_z, 5) / all_counts

    @pl.when(core == 1)
    def _():
        whole(totals_in, 15, 5).wait_send()


def tail_call(grid, matrix, twiddle, onehot, hit, counts):
    small = (4, 128)
    return pl.pallas_call(
        tail_kernel,
        out_shape=(jax.ShapeDtypeStruct((64, 64), F32), jax.ShapeDtypeStruct((4, 128), F32)),
        in_specs=[VMEM_SPEC] * 6,
        out_specs=(VMEM_SPEC,) * 2,
        scratch_shapes=[
            pltpu.VMEM((256, 1024), BF16),
            pltpu.VMEM((256, 1024), BF16),
            pltpu.VMEM((16, 4096), F32),
            pltpu.VMEM((2, 4, 2, 8, 8, 128), F32),
            pltpu.VMEM((4, 2, 8, 8, 128), F32),
            pltpu.VMEM((16, 4, 8, 128), F32),
            pltpu.VMEM((16, 4, 8, 128), F32),
            pltpu.VMEM((32,) + small, F32),
            pltpu.VMEM((8,) + small, F32),
            pltpu.VMEM(small, F32),
            pltpu.VMEM(small, F32),
            pltpu.VMEM((32,) + small, F32),
            pltpu.VMEM((8,) + small, F32),
            pltpu.VMEM(small, F32),
            pltpu.SemaphoreType.DMA((12,)),
        ],
        compiler_params=pltpu.CompilerParams(
            collective_id=1, has_side_effects=True, vmem_limit_bytes=LIMIT
        ),
    )(grid, matrix, twiddle, onehot, hit, counts)


def per_device(visibility, tile_of, u_within, v_cell, kernel_index, kernel, live_count, bin_map):
    merged, kernel_rows, used, phase, matrix, twiddle, onehot, hit, counts = gather_call(
        live_count.T,
        visibility,
        tile_of.transpose(0, 2, 1),
        u_within,
        v_cell,
        kernel_index,
        kernel.T,
        bin_map,
    )
    grid = grid_call(merged, used, phase, kernel_rows)
    power, spectrum = tail_call(grid, matrix, twiddle, onehot, hit, counts)
    return power, spectrum.reshape(NBINS)


def solution(mesh):
    return jax.shard_map(
        per_device,
        mesh=mesh,
        in_specs=(
            P(None, "freq", "base"),
            P("freq", "base", None),
            P("freq", "base"),
            P("freq", "base"),
            P(None, "freq", "base"),
            P(),
            P("freq", "base"),
            P("base", None),
        ),
        out_specs=(P("freq", "base"), P()),
        check_vma=False,
    )
```

```python
import functools
import math

import jax
import jax.numpy as jnp
from jax import lax
from jax.experimental import pallas as pl
from jax.experimental.pallas import tpu as pltpu
from jax.sharding import PartitionSpec as P

G = 1024
NBINS = 512
KW = 8
OVER = 128
SLOTS = 512
TILES = 16
BLOCKS = 128
GROUP = 4
F32 = jnp.float32
BF16 = jnp.bfloat16
I32 = jnp.int32
MESH = pl.DeviceIdType.MESH
VMEM_SPEC = pl.BlockSpec(memory_space=pltpu.VMEM)
LIMIT = 16 * 1024 * 1024
NORM = 1.0 / (32 * 8192)


def iota(shape, dim):
    return lax.broadcasted_iota(I32, shape, dim)


def cis(phase, period):
    phase = phase & (period - 1)
    phase = jnp.where(phase >= period // 2, phase - period, phase)
    angle = phase.astype(F32) * (2.0 * math.pi / period)
    return jnp.cos(angle), -jnp.sin(angle)


def cmul(ar, ai, br, bi):
    return ar * br - ai * bi, ar * bi + ai * br


def split2(x):
    hi = x.astype(BF16)
    return hi, (x - hi.astype(F32)).astype(BF16)


def dot_nt(a, b):
    return lax.dot_general(a, b, (((1,), (1,)), ((), ())), preferred_element_type=F32)


def dot_nn(a, b):
    return lax.dot_general(a, b, (((1,), (0,)), ((), ())), preferred_element_type=F32)


def take_lanes(table, index):
    return jnp.take_along_axis(table, index, axis=1, mode="promise_in_bounds")


def bin_channel(ch, z, vis_ref, tile_ref, within_ref, vcell_ref, kidx_ref, live, upper):
    tile = tile_ref[ch]
    lane = iota((1, SLOTS), 1)
    is_live = lane < live
    member = (tile == iota((TILES, SLOTS), 0)) & is_live
    before = dot_nn(member.astype(BF16), upper)
    rank = jnp.sum(jnp.where(member, before, 0.0), axis=0, keepdims=True).astype(I32)
    block = tile * 4 + (rank >> 4)
    position = (block >> 3) * 128 + (((block & 7) + z) & 7) * 16 + (rank & 15)
    position = jnp.where(is_live, position, -1)
    row = jnp.minimum(within_ref[ch : ch + 1, :], (G - KW) - tile * 64)
    column = vcell_ref[ch : ch + 1, :]
    parts = []
    for part in range(2):
        value = vis_ref[part, ch : ch + 1, :]
        for _ in range(3):
            piece = value.astype(BF16).astype(F32)
            parts.append(piece)
            value = value - piece
    parts += [
        row.astype(F32),
        (column >> 3).astype(F32),
        (column & 7).astype(F32),
        kidx_ref[0, ch : ch + 1, :].astype(F32),
        kidx_ref[1, ch : ch + 1, :].astype(F32),
        jnp.ones((1, SLOTS), F32),
        jnp.zeros((4, SLOTS), F32),
    ]
    payload = jnp.concatenate(parts, axis=0).astype(BF16)
    out = []
    for part in range(4):
        place = (iota((256, SLOTS), 0) + part * 256 == position).astype(F32).astype(BF16)
        got = dot_nt(payload, place)
        out.append(
            jnp.concatenate(
                [
                    got[0:1] + got[1:2] + got[2:3],
                    got[3:4] + got[4:5] + got[5:6],
                    got[6:7],
                    got[7:8] * 8.0 + got[8:9],
                    got[9:10],
                    got[10:11],
                    got[11:12],
                    jnp.zeros((1, 256), F32),
                ],
                axis=0,
            )
        )
    return out


def places():
    base = lax.axis_index("base")
    return base // 8, base % 8


def gather_kernel(
    live_hbm,
    vis_hbm,
    tile_hbm,
    within_hbm,
    vcell_hbm,
    kidx_hbm,
    kernel_hbm,
    bins_ref,
    out_ref,
    kernel_ref,
    used_ref,
    phase_ref,
    matrix_ref,
    twiddle_ref,
    onehot_ref,
    hit_ref,
    counts_ref,
    packed,
    got,
    bins,
    turned,
    live_ref,
    vis_ref,
    tile_ref,
    within_ref,
    vcell_ref,
    kidx_ref,
    send,
    land,
    relay,
    local,
    fetched,
):
    inputs = (
        (live_hbm, live_ref),
        (tile_hbm, tile_ref),
        (vis_hbm, vis_ref),
        (within_hbm, within_ref),
        (vcell_hbm, vcell_ref),
        (kidx_hbm, kidx_ref),
        (kernel_hbm, kernel_ref),
    )
    loads = [
        pltpu.make_async_copy(source, place, fetched.at[index])
        for index, (source, place) in enumerate(inputs)
    ]
    for load in loads:
        load.start()
    h, z = places()
    freq = lax.axis_index("freq")
    at = pl.multiple_of((freq // 2) * 128, 128)
    fetch = pltpu.make_async_copy(bins_ref.at[:, pl.ds(at, 128)], bins, fetched.at[7])
    fetch.start()
    hops = (1, -1, 2, -2)

    def device(side, step):
        return {"base": side * 8 + (z + step + 8) % 8}

    barrier = pltpu.get_barrier_semaphore()
    for step in hops:
        pl.semaphore_signal(barrier, 1, device_id=device(h, step), device_id_type=MESH)
    for step in (0, 2, -2):
        pl.semaphore_signal(barrier, 1, device_id=device(1 - h, step), device_id_type=MESH)

    upper = (iota((SLOTS, SLOTS), 0) < iota((SLOTS, SLOTS), 1)).astype(F32).astype(BF16)
    for load in loads:
        load.wait()
    for ch in range(2):
        live = live_ref[0:1, ch : ch + 1]
        parts = bin_channel(
            ch, z, vis_ref, tile_ref, within_ref, vcell_ref, kidx_ref, live, upper
        )
        for index, part in enumerate(parts):
            packed[ch, 12 * index : 12 * index + 6] = part[:6, :128]
            packed[ch, 12 * index + 6 : 12 * index + 12] = part[:6, 128:]
    pl.semaphore_wait(barrier, 7)

    def direct(side, step, number):
        return pltpu.make_async_remote_copy(
            src_ref=packed.at[side],
            dst_ref=got.at[z, h],
            send_sem=send.at[number],
            recv_sem=land.at[z, h],
            device_id=device(side, step),
            device_id_type=MESH,
        )

    def arrival(step, side):
        zz = (z + step + 8) % 8
        return pltpu.make_async_remote_copy(
            src_ref=got.at[zz, side],
            dst_ref=got.at[zz, side],
            send_sem=send.at[0],
            recv_sem=land.at[zz, side],
            device_id=device(1 - h, 0),
            device_id_type=MESH,
        )

    copies = []
    for step in (2, -2):
        copies.append(direct(1 - h, step, len(copies)))
        copies.append(direct(h, step, len(copies)))
    copies.insert(2, direct(1 - h, 0, 4))
    for step in (1, -1):
        copies.append(direct(h, step, len(copies)))
    for copy in copies:
        copy.start()
    own = pltpu.make_async_copy(packed.at[h], got.at[z, h], local)
    own.start()

    column_tables(z, kernel_ref, phase_ref)
    row_tables(matrix_ref, twiddle_ref)
    fetch.wait()
    bin_tables(freq % 2, bins, turned, onehot_ref, hit_ref, counts_ref)

    relays = []

    def pass_on(source, side, step):
        zz = (z + source + 8) % 8
        copy = pltpu.make_async_remote_copy(
            src_ref=got.at[zz, side],
            dst_ref=got.at[zz, side],
            send_sem=relay.at[len(relays)],
            recv_sem=land.at[zz, side],
            device_id=device(h, step),
            device_id_type=MESH,
        )
        copy.start()
        relays.append(copy)

    arrival(0, 1 - h).wait_recv()
    pass_on(0, 1 - h, 1)
    pass_on(0, 1 - h, -1)
    arrival(-2, h).wait_recv()
    pass_on(-2, h, 2)
    pass_on(-2, h, 1)
    arrival(2, h).wait_recv()
    pass_on(2, h, -1)
    arrival(2, 1 - h).wait_recv()
    pass_on(2, 1 - h, -2)
    pass_on(2, 1 - h, -1)
    arrival(-2, 1 - h).wait_recv()
    pass_on(-2, 1 - h, 1)
    for step in (1, -1):
        arrival(step, h).wait_recv()
        arrival(step, 1 - h).wait_recv()
    for step in (3, -3, 4):
        arrival(step, h).wait_recv()
        arrival(step, 1 - h).wait_recv()
    own.wait()
    for copy in copies + relays:
        copy.wait_send()
    group = iota((48, 128), 1) >> 4
    for half in range(2):
        for i in range(8):
            block = got[(0 - i) % 8, half]
            for p in range(1, 8):
                block = jnp.where(group == p, got[(p - i) % 8, half], block)
            out_ref[half * 8 + i] = block
    nonzero = (out_ref[...].reshape(768, 128) != 0.0).astype(F32).astype(BF16)
    found = dot_nt(jnp.ones((8, 128), F32).astype(BF16), nonzero).astype(BF16)
    row, block = iota((768, 128), 0), iota((768, 128), 1)
    first = ((block >> 6) * 8 + (block & 7)) * 48 + ((block >> 3) & 7) * 6
    pick = ((row == first) | (row == first + 1)).astype(F32).astype(BF16)
    used_ref[...] = dot_nn(found, pick).astype(I32)


def column_tables(z, kernel_ref, phase_ref):
    l_row = iota((128, 128), 0)
    zr, zi = cis((l_row & 63) + (l_row >> 6) * 512 + z * 64, G)
    kern = kernel_ref[...]
    pr = jnp.broadcast_to(kern[7:8], (128, 128))
    pi = jnp.zeros((128, 128), F32)
    for s in range(6, -1, -1):
        pr, pi = cmul(pr, pi, zr, zi)
        pr = pr + kern[s : s + 1]
    phase_ref[0] = pr
    phase_ref[1] = pi


def row_tables(matrix_ref, twiddle_ref):
    row, lane = iota((128, 128), 0), iota((128, 128), 1)
    fc, fs = cis(row * lane, 128)
    for quarter, value in ((0, fc), (1, -fs), (2, fs), (3, fc)):
        down, right = (quarter >> 1) * 128, (quarter & 1) * 128
        for part, half in enumerate(split2(value)):
            matrix_ref[part, down : down + 128, right : right + 128] = half
    tr, ti = cis(row, G)
    ar, ai = tr, ti
    for k0 in range(1, 8):
        twiddle_ref[k0 - 1, 0] = ar
        twiddle_ref[k0 - 1, 1] = ai
        if k0 < 7:
            ar, ai = cmul(ar, ai, tr, ti)


def bin_tables(core, bins, turned, onehot_ref, hit_ref, counts_ref):
    full = jnp.concatenate([bins[...].astype(F32), jnp.zeros((64, 128), F32)], axis=0)
    turned[...] = pltpu.roll(full, core * 64, 1).T
    row128, high_row, lane8 = iota((128, 128), 0), iota((4, 128), 0), iota((8, 128), 1)
    for k0 in range(4):
        ours = turned[pl.ds(k0, 8, stride=8), :]
        other = turned[pl.ds(k0 + 4, 8, stride=8), :]
        both = jnp.where(lane8 < 64, ours, pltpu.roll(other, 64, 1)).astype(I32)
        for sub in range(8):
            found = both[sub : sub + 1]
            at = slice(128 * (8 * k0 + sub), 128 * (8 * k0 + sub) + 128)
            onehot_ref[:, at] = (row128 == (found & 127)).astype(F32).astype(BF16)
            hit_ref[:, at] = ((found >> 7) == high_row).astype(F32)
    counts_ref[...] = dot_nt(hit_ref[...].astype(BF16), onehot_ref[...])


def gather_call(*args):
    return pl.pallas_call(
        gather_kernel,
        out_shape=(
            jax.ShapeDtypeStruct((16, 48, 128), F32),
            jax.ShapeDtypeStruct((8, 128), F32),
            jax.ShapeDtypeStruct((8, 128), I32),
            jax.ShapeDtypeStruct((2, 128, 128), F32),
            jax.ShapeDtypeStruct((2, 256, 256), BF16),
            jax.ShapeDtypeStruct((7, 2, 128, 128), F32),
            jax.ShapeDtypeStruct((128, 4096), BF16),
            jax.ShapeDtypeStruct((4, 4096), F32),
            jax.ShapeDtypeStruct((4, 128), F32),
        ),
        in_specs=[pl.BlockSpec(memory_space=pltpu.HBM)] * 8,
        out_specs=(VMEM_SPEC,) * 9,
        scratch_shapes=[
            pltpu.VMEM((2, 48, 128), F32),
            pltpu.VMEM((8, 2, 48, 128), F32),
            pltpu.VMEM((64, 128), I32),
            pltpu.VMEM((128, 128), F32),
            pltpu.VMEM((1, 2), I32),
            pltpu.VMEM((2, 2, SLOTS), F32),
            pltpu.VMEM((2, 1, SLOTS), I32),
            pltpu.VMEM((2, SLOTS), I32),
            pltpu.VMEM((2, SLOTS), I32),
            pltpu.VMEM((2, 2, SLOTS), I32),
            pltpu.SemaphoreType.DMA((7,)),
            pltpu.SemaphoreType.DMA((8, 2)),
            pltpu.SemaphoreType.DMA((8,)),
            pltpu.SemaphoreType.DMA,
            pltpu.SemaphoreType.DMA((8,)),
        ],
        compiler_params=pltpu.CompilerParams(
            collective_id=0, has_side_effects=True, vmem_limit_bytes=LIMIT
        ),
    )(*(pltpu.with_memory_space_constraint(x, pltpu.HBM) for x in args))


def gridder(merged, taps_ref, kernel_ref, grid_ref, wbufs, rbufs, rows):
    sub = iota((8, 128), 0)
    lane = iota((8, 128), 1)
    _, z = places()
    sd_r, sd_i = cis(sub * lane, G)
    sc_r, sc_i = cis(sub * lane, 8)
    gd_r, gd_i = cis((z * 64 + sub * 8) * lane, G)
    gc_r, gc_i = cis((z * 64 + sub * 8) * lane, 8)
    grid_ref[...] = jnp.zeros_like(grid_ref)
    for i in range(GROUP):
        for ref in rbufs:
            ref[i, 80:160, 128:256] = jnp.zeros((80, 128), BF16)
    for i in range(GROUP):
        rbufs[1][i, 0:80, 0:256] = jnp.zeros((80, 256), BF16)
        rbufs[1][i, 80:160, 0:128] = jnp.zeros((80, 128), BF16)
        wbufs[1][i] = jnp.zeros((256, 256), BF16)

    def build(bid, slot, i):
        which = lax.rem(lax.div(bid, 64), 2) * 8 + lax.rem(bid, 8)
        first = lax.rem(lax.div(bid, 8), 8) * 6
        keep = jnp.where(bid < BLOCKS, 1.0, 0.0)

        def field(index):
            return jnp.broadcast_to(merged[which, pl.ds(first + index, 1), :], (8, 128))

        v = field(3).astype(I32)
        index_d = v & 127
        index_c = v >> 7
        index_u = field(4).astype(I32)
        index_v = field(5).astype(I32)
        w = field(2).astype(I32)
        near = [take_lanes(t, index_d) for t in (gd_r, gd_i, sd_r, sd_i)]
        wide = [take_lanes(t, index_c) for t in (gc_r, gc_i, sc_r, sc_i)]
        group = cmul(*near[:2], *wide[:2])
        inner = cmul(*cmul(*near[2:], *wide[2:]), field(0) * keep, field(1) * keep)
        sign = (1 - 2 * (v & 1)).astype(F32)
        rows[i, 0] = group[0]
        rows[i, 1] = group[1]
        for pair in range(4):
            done = []
            for g in (2 * pair, 2 * pair + 1):
                ar, ai = cmul(jnp.broadcast_to(rows[i, 0, g : g + 1], (8, 128)), jnp.broadcast_to(rows[i, 1, g : g + 1], (8, 128)), *inner)
                low, high = slice(8 * g, 8 * g + 8), slice(64 + 8 * g, 72 + 8 * g)
                one = cmul(ar, ai, take_lanes(taps_ref[0, low], index_v), take_lanes(taps_ref[1, low], index_v))
                two = cmul(ar * sign, ai * sign, take_lanes(taps_ref[0, high], index_v), take_lanes(taps_ref[1, high], index_v))
                done.append(one + two)
            for part, start in enumerate((0, 128, 64, 192)):
                hi, lo = split2(jnp.concatenate([done[0][part], done[1][part]], axis=0))
                at = slice(start + 16 * pair, start + 16 * pair + 16)
                wbufs[slot][i, at, 0:128] = hi
                wbufs[slot][i, at, 128:256] = lo
        taps = take_lanes(kernel_ref[...], index_u)
        turned = jnp.take_along_axis(taps, (sub - w) & 7, axis=0, mode="promise_in_bounds")
        high = turned.astype(BF16).astype(F32)
        low = turned - high
        down = (w - sub + 7) >> 3
        zero = jnp.zeros((8, 128), F32)
        for pair in range(5):
            his, los = [], []
            for k in (2 * pair, 2 * pair + 1):
                hit = down == k
                his.append(jnp.where(hit, high, zero))
                los.append(jnp.where(hit, low, zero))
            hi = jnp.concatenate(his, axis=0).astype(BF16)
            at = slice(16 * pair, 16 * pair + 16)
            rbufs[slot][i, at, 0:128] = hi
            rbufs[slot][i, at, 128:256] = hi
            at = slice(80 + 16 * pair, 80 + 16 * pair + 16)
            rbufs[slot][i, at, 0:128] = jnp.concatenate(los, axis=0).astype(BF16)

    def place(bid, slot, i):
        res = dot_nt(rbufs[slot][i], wbufs[slot][i])
        start = pl.multiple_of(lax.rem(lax.div(bid, 4), 16) * 64, 64)
        grid_ref[pl.ds(start, 80), :] += res[:80] + res[80:]

    return build, place


def grid_kernel(
    merged, used_ref, taps_ref, kernel_ref, grid_ref, wbuf_a, rbuf_a, wbuf_b, rbuf_b, rows, used, order, sem
):
    copy = pltpu.make_async_copy(used_ref, used, sem)
    copy.start()
    build, place = gridder(
        merged, taps_ref, kernel_ref, grid_ref, (wbuf_a, wbuf_b), (rbuf_a, rbuf_b), rows
    )
    copy.wait()

    def list_step(four, n):
        for extra in range(1, 4):
            b = 4 * four + extra
            order[n] = b
            n = n + jnp.where(used[0, b] > 0, 1, 0)
        return n

    total = lax.fori_loop(0, BLOCKS // 4, list_step, 0, unroll=8)
    for i in range(2 * GROUP):
        order[total + i] = BLOCKS

    def step(it, before):
        first = tuple(order[2 * GROUP * it + i] for i in range(GROUP))
        second = tuple(order[2 * GROUP * it + GROUP + i] for i in range(GROUP))
        for i in range(GROUP):
            place(before[i], 1, i)
            build(first[i], 0, i)
        for i in range(GROUP):
            place(first[i], 0, i)
            build(second[i], 1, i)
        return second

    rounds = (total + 2 * GROUP - 1) // (2 * GROUP)
    last = lax.fori_loop(0, rounds, step, (jnp.int32(BLOCKS),) * GROUP)
    for i in range(GROUP):
        place(last[i], 1, i)


def grid_call(merged, used, phase, kernel_t):
    return pl.pallas_call(
        grid_kernel,
        out_shape=jax.ShapeDtypeStruct((1040, 256), F32),
        in_specs=[VMEM_SPEC] * 4,
        out_specs=VMEM_SPEC,
        scratch_shapes=[
            pltpu.VMEM((GROUP, 256, 256), BF16),
            pltpu.VMEM((GROUP, 160, 256), BF16),
            pltpu.VMEM((GROUP, 256, 256), BF16),
            pltpu.VMEM((GROUP, 160, 256), BF16),
            pltpu.VMEM((GROUP, 2, 8, 128), F32),
            pltpu.SMEM((8, 128), I32),
            pltpu.SMEM((BLOCKS + 2 * GROUP,), I32),
            pltpu.SemaphoreType.DMA,
        ],
        compiler_params=pltpu.CompilerParams(vmem_limit_bytes=LIMIT),
    )(merged, used, phase, kernel_t)


def tail_kernel(
    grid_ref, merged, taps_ref, kernel_ref, matrix_ref, tw_ref, onehot, hit_ref, counts, power_ref, spectrum_ref,
    first_ref, wbuf_a, rbuf_a, wbuf_b, rbuf_b, rows_ref, bh_ref, bl_ref, left, piece, partner, summed, landed, counts_in, counts_z, counts_plane,
    totals, totals_in, totals_z, totals_plane, sems,
):
    h, z = places()
    freq = lax.axis_index("freq")
    quad, core = freq // 2, freq % 2
    me = h * 16 + freq
    me_pair = h * 8 + quad
    far_first = (4, 3, 5, 2, 6, 1, 7)

    def chip(index, to_core):
        return {"freq": (index % 8) * 2 + to_core, "base": (index // 8) * 8 + z}

    def column(step, to_core):
        return {"freq": quad * 2 + to_core, "base": h * 8 + (z + step) % 8}

    barrier = pltpu.get_barrier_semaphore()

    def greet(device):
        pl.semaphore_signal(barrier, 1, device_id=device, device_id_type=MESH)

    for step in far_first:
        for to_core in range(2):
            greet(column(step, to_core))
    for k in range(1, 16):
        for to_core in range(2):
            greet(chip((me_pair + k) % 16, to_core))
    greet(chip(me_pair, 1 - core))

    build, place = gridder(
        merged, taps_ref, kernel_ref, first_ref, (wbuf_a, wbuf_b), (rbuf_a, rbuf_b), rows_ref
    )

    def step(it, _):
        for i in range(GROUP):
            place(4 * ((2 * GROUP * it + 32 - GROUP + i) % 32), 1, i)
            build(4 * (2 * GROUP * it + i), 0, i)
        for i in range(GROUP):
            place(4 * (2 * GROUP * it + i), 0, i)
            build(4 * (2 * GROUP * it + GROUP + i), 1, i)
        return 0

    lax.fori_loop(0, 32 // (2 * GROUP), step, 0)
    for i in range(GROUP):
        place(4 * (32 - GROUP + i), 1, i)

    root = math.sqrt(0.5)
    slot_of = (0, 2, 4, 6, 1, 3, 5, 7)
    for rows in range(8):
        u = [
            (
                grid_ref[128 * a + 16 * rows : 128 * a + 16 * rows + 16, 0:128]
                + first_ref[128 * a + 16 * rows : 128 * a + 16 * rows + 16, 0:128],
                grid_ref[128 * a + 16 * rows : 128 * a + 16 * rows + 16, 128:256]
                + first_ref[128 * a + 16 * rows : 128 * a + 16 * rows + 16, 128:256],
            )
            for a in range(8)
        ]

        def add(x, y):
            return x[0] + y[0], x[1] + y[1]

        def sub2(x, y):
            return x[0] - y[0], x[1] - y[1]

        def four(a, b, c, d):
            s, t = add(a, c), sub2(a, c)
            p, q = add(b, d), sub2(b, d)
            mq = (q[1], -q[0])
            return add(s, p), add(t, mq), sub2(s, p), sub2(t, mq)

        even = four(u[0], u[2], u[4], u[6])
        odd = four(u[1], u[3], u[5], u[7])
        o1 = ((odd[1][0] + odd[1][1]) * root, (odd[1][1] - odd[1][0]) * root)
        o2 = (odd[2][1], -odd[2][0])
        o3 = ((odd[3][1] - odd[3][0]) * root, -(odd[3][0] + odd[3][1]) * root)
        odd = (odd[0], o1, o2, o3)
        spectrum = [add(even[k], odd[k]) for k in range(4)] + [sub2(even[k], odd[k]) for k in range(4)]
        at = slice(16 * rows, 16 * rows + 16)
        for k0 in range(8):
            xr, xi = spectrum[k0]
            if k0:
                xr, xi = cmul(xr, xi, tw_ref[k0 - 1, 0, at], tw_ref[k0 - 1, 1, at])
            col = slice(128 * slot_of[k0], 128 * slot_of[k0] + 128)
            for base, value in ((0, xr), (128, xi)):
                hi, lo = split2(value)
                bh_ref[base + 16 * rows : base + 16 * rows + 16, col] = hi
                bl_ref[base + 16 * rows : base + 16 * rows + 16, col] = lo
    low_half = iota((128, 128), 1) < 64
    for k0 in range(4):
        col = slice(256 * k0, 256 * k0 + 256)
        full = dot_nn(matrix_ref[0], bh_ref[:, col]) + dot_nn(matrix_ref[0], bl_ref[:, col]) + dot_nn(matrix_ref[1], bh_ref[:, col])
        power = (full[:128] * full[:128] + full[128:] * full[128:]) * NORM
        pa, pb = power[:, :128], power[:, 128:]
        ra, rb = pltpu.roll(pa, 64, 1), pltpu.roll(pb, 64, 1)
        for side, block in ((0, jnp.where(low_half, pa, rb)), (1, jnp.where(low_half, ra, pb))):
            block = block.reshape(8, 2, 8, 128)
            for cc in range(2):
                piece[cc, k0, side] = block[:, cc]

    pl.semaphore_wait(barrier, 45)

    def remote(source, target, number, device):
        return pltpu.make_async_remote_copy(
            src_ref=source, dst_ref=target, send_sem=sems.at[2 * number], recv_sem=sems.at[2 * number + 1],
            device_id=device, device_id_type=MESH,
        )

    def whole(ref, count, number):
        return remote(ref.at[0:count], ref.at[0:count], number, chip(me_pair, 1 - core))

    pair = remote(piece.at[1 - core], partner, 0, chip(me_pair, 1 - core))
    pair.start()

    def plane_send(buf, slots, number):
        @pl.when(core == 0)
        def _():
            remote(buf, slots.at[me], number, chip(me_pair, 1)).start()

        for k in range(1, 16):
            remote(buf, slots.at[me], number, chip((me_pair + k) % 16, 1)).start()

    def plane_sum(buf, slots, result, number):
        slots[me] = buf[...]
        whole(slots, 31, number).wait_recv()
        total = slots[0]
        for index in range(1, 32):
            total = total + slots[index]
        result[...] = total

    def column_send(buf, slots, number):
        for step in far_first:
            for to_core in range(2):
                remote(buf, slots.at[z], number, column(step, to_core)).start()
        remote(buf, slots.at[z], number, chip(me_pair, 0)).start()

    def column_sum(buf, slots, number):
        @pl.when(core == 0)
        def _():
            whole(slots, 8, number).wait_recv()

        @pl.when(core == 1)
        def _():
            slots[z] = buf[...]
            whole(slots, 7, number).wait_recv()

        total = slots[0]
        for index in range(1, 8):
            total = total + slots[index]
        return total

    def plane_sent(slots, number):
        @pl.when(core == 0)
        def _():
            whole(slots, 16, number).wait_send()

        @pl.when(core == 1)
        def _():
            whole(slots, 15, number).wait_send()

    plane_send(counts, counts_in, 2)
    pair.wait_recv()
    for k0 in range(4):
        for side in range(2):
            for q in range(8):
                summed[side * 8 + q, k0] = piece[core, k0, side, q] + partner[k0, side, q]
    for k in range(1, 16):
        peer = (me_pair + k) % 16
        remote(summed.at[peer], landed.at[me_pair], 1, chip(peer, core)).start()
    landed[me_pair] = summed[me_pair]

    @pl.when(core == 1)
    def _():
        plane_sum(counts, counts_in, counts_plane, 2)
        column_send(counts_plane, counts_z, 3)

    whole(landed, 15, 1).wait_recv()
    total = landed[0]
    for index in range(1, 16):
        total = total + landed[index]
    for k0 in range(4):
        for sub in range(8):
            at = slice(128 * (8 * k0 + sub), 128 * (8 * k0 + sub) + 128)
            hit = hit_ref[:, at]
            value = total[k0][sub : sub + 1]
            p0 = value.astype(BF16).astype(F32)
            p1 = (value - p0).astype(BF16).astype(F32)
            left[0:4, at] = hit * p0
            left[4:8, at] = hit * p1
            left[8:12, at] = hit * (value - p0 - p1)
            left[12:16, at] = jnp.zeros((4, 128), F32)
    got = dot_nt(left[...].astype(BF16), onehot[...])
    totals[...] = got[0:4] + got[4:8] + got[8:12]
    plane_send(totals, totals_in, 4)
    for k0 in range(8):
        half = (k0 // 4) * 64
        power_ref[pl.ds(k0, 8, stride=8), :] = total[k0 % 4][:, half : half + 64]
    all_counts = column_sum(counts_plane, counts_z, 3)

    @pl.when(core == 1)
    def _():
        plane_sum(totals, totals_in, totals_plane, 4)
        column_send(totals_plane, totals_z, 5)

    pair.wait_send()
    whole(landed, 15, 1).wait_send()
    plane_sent(counts_in, 2)
    plane_sent(totals_in, 4)

    @pl.when(core == 1)
    def _():
        whole(counts_in, 15, 3).wait_send()

    spectrum_ref[...] = column_sum(totals_plane, totals_z, 5) / all_counts

    @pl.when(core == 1)
    def _():
        whole(totals_in, 15, 5).wait_send()


def tail_call(*args):
    small = (4, 128)
    return pl.pallas_call(
        tail_kernel,
        out_shape=(jax.ShapeDtypeStruct((64, 64), F32), jax.ShapeDtypeStruct((4, 128), F32)),
        in_specs=[VMEM_SPEC] * 9,
        out_specs=(VMEM_SPEC,) * 2,
        scratch_shapes=[
            pltpu.VMEM((1040, 256), F32),
            pltpu.VMEM((GROUP, 256, 256), BF16),
            pltpu.VMEM((GROUP, 160, 256), BF16),
            pltpu.VMEM((GROUP, 256, 256), BF16),
            pltpu.VMEM((GROUP, 160, 256), BF16),
            pltpu.VMEM((GROUP, 2, 8, 128), F32),
            pltpu.VMEM((256, 1024), BF16),
            pltpu.VMEM((256, 1024), BF16),
            pltpu.VMEM((16, 4096), F32),
            pltpu.VMEM((2, 4, 2, 8, 8, 128), F32),
            pltpu.VMEM((4, 2, 8, 8, 128), F32),
            pltpu.VMEM((16, 4, 8, 128), F32),
            pltpu.VMEM((16, 4, 8, 128), F32),
            pltpu.VMEM((32,) + small, F32),
            pltpu.VMEM((8,) + small, F32),
            pltpu.VMEM(small, F32),
            pltpu.VMEM(small, F32),
            pltpu.VMEM((32,) + small, F32),
            pltpu.VMEM((8,) + small, F32),
            pltpu.VMEM(small, F32),
            pltpu.SemaphoreType.DMA((12,)),
        ],
        compiler_params=pltpu.CompilerParams(
            collective_id=1, has_side_effects=True, vmem_limit_bytes=LIMIT
        ),
    )(*args)


def store_kernel(power_ref, spectrum_ref, power_out, spectrum_out, sems):
    first = pltpu.make_async_copy(power_ref, power_out, sems.at[0])
    second = pltpu.make_async_copy(spectrum_ref, spectrum_out, sems.at[1])
    first.start()
    second.start()
    first.wait()
    second.wait()


def store_call(power, spectrum):
    return pl.pallas_call(
        store_kernel,
        out_shape=(jax.ShapeDtypeStruct((64, 64), F32), jax.ShapeDtypeStruct((4, 128), F32)),
        in_specs=[VMEM_SPEC] * 2,
        out_specs=(pl.BlockSpec(memory_space=pltpu.HBM),) * 2,
        scratch_shapes=[pltpu.SemaphoreType.DMA((2,))],
        compiler_params=pltpu.CompilerParams(vmem_limit_bytes=LIMIT),
    )(power, spectrum)


def per_device(visibility, tile_of, u_within, v_cell, kernel_index, kernel, live_count, bin_map):
    merged, kernel_rows, used, phase, matrix, twiddle, onehot, hit, counts = gather_call(
        live_count.T,
        visibility,
        tile_of.transpose(0, 2, 1),
        u_within,
        v_cell,
        kernel_index,
        kernel.T,
        bin_map,
    )
    grid = grid_call(merged, used, phase, kernel_rows)
    power, spectrum = tail_call(grid, merged, phase, kernel_rows, matrix, twiddle, onehot, hit, counts)
    power, spectrum = store_call(power, spectrum)
    return power, spectrum.reshape(NBINS)


def solution(mesh):
    return jax.shard_map(
        per_device,
        mesh=mesh,
        in_specs=(
            P(None, "freq", "base"),
            P("freq", "base", None),
            P("freq", "base"),
            P("freq", "base"),
            P(None, "freq", "base"),
            P(),
            P("freq", "base"),
            P("base", None),
        ),
        out_specs=(P("freq", "base"), P()),
        check_vma=False,
    )
```

```python
import functools
import math

import jax
import jax.numpy as jnp
from jax import lax
from jax.experimental import pallas as pl
from jax.experimental.pallas import tpu as pltpu
from jax.sharding import PartitionSpec as P

G = 1024
NBINS = 512
KW = 8
OVER = 128
SLOTS = 512
TILES = 16
BLOCKS = 128
GROUP = 4
TAIL = 24
F32 = jnp.float32
BF16 = jnp.bfloat16
I32 = jnp.int32
MESH = pl.DeviceIdType.MESH
VMEM_SPEC = pl.BlockSpec(memory_space=pltpu.VMEM)
LIMIT = 16 * 1024 * 1024
STEPS = sorted(
    ((down, right) for down in range(4) for right in range(4) if down or right),
    key=lambda step: (-sum(min(part, 4 - part) for part in step), step),
)
NORM = 1.0 / (32 * 8192)


def iota(shape, dim):
    return lax.broadcasted_iota(I32, shape, dim)


def cis(phase, period):
    phase = phase & (period - 1)
    phase = jnp.where(phase >= period // 2, phase - period, phase)
    angle = phase.astype(F32) * (2.0 * math.pi / period)
    return jnp.cos(angle), -jnp.sin(angle)


def cmul(ar, ai, br, bi):
    return ar * br - ai * bi, ar * bi + ai * br


def split2(x):
    hi = x.astype(BF16)
    return hi, (x - hi.astype(F32)).astype(BF16)


def dot_nt(a, b):
    return lax.dot_general(a, b, (((1,), (1,)), ((), ())), preferred_element_type=F32)


def dot_nn(a, b):
    return lax.dot_general(a, b, (((1,), (0,)), ((), ())), preferred_element_type=F32)


def take_lanes(table, index):
    return jnp.take_along_axis(table, index, axis=1, mode="promise_in_bounds")


def bin_channel(ch, z, vis_ref, tile_ref, within_ref, vcell_ref, kidx_ref, live, upper):
    tile = tile_ref[ch]
    lane = iota((1, SLOTS), 1)
    is_live = lane < live
    member = (tile == iota((TILES, SLOTS), 0)) & is_live
    before = dot_nn(member.astype(BF16), upper)
    rank = jnp.sum(jnp.where(member, before, 0.0), axis=0, keepdims=True).astype(I32)
    block = tile * 4 + (rank >> 4)
    position = (block >> 3) * 128 + (((block & 7) + z) & 7) * 16 + (rank & 15)
    position = jnp.where(is_live, position, -1)
    row = jnp.minimum(within_ref[ch : ch + 1, :], (G - KW) - tile * 64)
    column = vcell_ref[ch : ch + 1, :]
    parts = []
    for part in range(2):
        value = vis_ref[part, ch : ch + 1, :]
        for _ in range(3):
            piece = value.astype(BF16).astype(F32)
            parts.append(piece)
            value = value - piece
    parts += [
        row.astype(F32),
        (column >> 3).astype(F32),
        (column & 7).astype(F32),
        kidx_ref[0, ch : ch + 1, :].astype(F32),
        kidx_ref[1, ch : ch + 1, :].astype(F32),
        jnp.ones((1, SLOTS), F32),
        jnp.zeros((4, SLOTS), F32),
    ]
    payload = jnp.concatenate(parts, axis=0).astype(BF16)
    out = []
    for part in range(4):
        place = (iota((256, SLOTS), 0) + part * 256 == position).astype(F32).astype(BF16)
        got = dot_nt(payload, place)
        out.append(
            jnp.concatenate(
                [
                    got[0:1] + got[1:2] + got[2:3],
                    got[3:4] + got[4:5] + got[5:6],
                    got[6:7],
                    got[7:8] * 8.0 + got[8:9],
                    got[9:10],
                    got[10:11],
                    got[11:12],
                    jnp.zeros((1, 256), F32),
                ],
                axis=0,
            )
        )
    return out


def places():
    base = lax.axis_index("base")
    return base // 8, base % 8


def gather_kernel(
    live_hbm,
    vis_hbm,
    tile_hbm,
    within_hbm,
    vcell_hbm,
    kidx_hbm,
    kernel_hbm,
    bins_ref,
    out_ref,
    kernel_ref,
    used_ref,
    phase_ref,
    matrix_ref,
    twiddle_ref,
    onehot_ref,
    hit_ref,
    counts_ref,
    packed,
    got,
    bins,
    turned,
    live_ref,
    vis_ref,
    tile_ref,
    within_ref,
    vcell_ref,
    kidx_ref,
    send,
    land,
    relay,
    local,
    fetched,
):
    inputs = (
        (live_hbm, live_ref),
        (tile_hbm, tile_ref),
        (vis_hbm, vis_ref),
        (within_hbm, within_ref),
        (vcell_hbm, vcell_ref),
        (kidx_hbm, kidx_ref),
        (kernel_hbm, kernel_ref),
    )
    loads = [
        pltpu.make_async_copy(source, place, fetched.at[index])
        for index, (source, place) in enumerate(inputs)
    ]
    for load in loads:
        load.start()
    h, z = places()
    freq = lax.axis_index("freq")
    at = pl.multiple_of((freq // 2) * 128, 128)
    fetch = pltpu.make_async_copy(bins_ref.at[:, pl.ds(at, 128)], bins, fetched.at[7])
    fetch.start()
    hops = (1, -1, 2, -2)

    def device(side, step):
        return {"base": side * 8 + (z + step + 8) % 8}

    barrier = pltpu.get_barrier_semaphore()
    for step in hops:
        pl.semaphore_signal(barrier, 1, device_id=device(h, step), device_id_type=MESH)
    for step in (0, 2, -2):
        pl.semaphore_signal(barrier, 1, device_id=device(1 - h, step), device_id_type=MESH)

    upper = (iota((SLOTS, SLOTS), 0) < iota((SLOTS, SLOTS), 1)).astype(F32).astype(BF16)
    for load in loads:
        load.wait()
    for ch in range(2):
        live = live_ref[0:1, ch : ch + 1]
        parts = bin_channel(
            ch, z, vis_ref, tile_ref, within_ref, vcell_ref, kidx_ref, live, upper
        )
        for index, part in enumerate(parts):
            packed[ch, 12 * index : 12 * index + 6] = part[:6, :128]
            packed[ch, 12 * index + 6 : 12 * index + 12] = part[:6, 128:]
    pl.semaphore_wait(barrier, 7)

    def direct(side, step, number):
        return pltpu.make_async_remote_copy(
            src_ref=packed.at[side],
            dst_ref=got.at[z, h],
            send_sem=send.at[number],
            recv_sem=land.at[z, h],
            device_id=device(side, step),
            device_id_type=MESH,
        )

    def arrival(step, side):
        zz = (z + step + 8) % 8
        return pltpu.make_async_remote_copy(
            src_ref=got.at[zz, side],
            dst_ref=got.at[zz, side],
            send_sem=send.at[0],
            recv_sem=land.at[zz, side],
            device_id=device(1 - h, 0),
            device_id_type=MESH,
        )

    copies = []
    for step in (2, -2):
        copies.append(direct(1 - h, step, len(copies)))
        copies.append(direct(h, step, len(copies)))
    copies.insert(2, direct(1 - h, 0, 4))
    for step in (1, -1):
        copies.append(direct(h, step, len(copies)))
    for copy in copies:
        copy.start()
    own = pltpu.make_async_copy(packed.at[h], got.at[z, h], local)
    own.start()

    column_tables(z, kernel_ref, phase_ref)
    row_tables(matrix_ref, twiddle_ref)
    fetch.wait()
    bin_tables(freq % 2, bins, turned, onehot_ref, hit_ref, counts_ref)

    relays = []

    def pass_on(source, side, step):
        zz = (z + source + 8) % 8
        copy = pltpu.make_async_remote_copy(
            src_ref=got.at[zz, side],
            dst_ref=got.at[zz, side],
            send_sem=relay.at[len(relays)],
            recv_sem=land.at[zz, side],
            device_id=device(h, step),
            device_id_type=MESH,
        )
        copy.start()
        relays.append(copy)

    arrival(0, 1 - h).wait_recv()
    pass_on(0, 1 - h, 1)
    pass_on(0, 1 - h, -1)
    arrival(-2, h).wait_recv()
    pass_on(-2, h, 2)
    pass_on(-2, h, 1)
    arrival(2, h).wait_recv()
    pass_on(2, h, -1)
    arrival(2, 1 - h).wait_recv()
    pass_on(2, 1 - h, -2)
    pass_on(2, 1 - h, -1)
    arrival(-2, 1 - h).wait_recv()
    pass_on(-2, 1 - h, 1)
    for step in (1, -1):
        arrival(step, h).wait_recv()
        arrival(step, 1 - h).wait_recv()
    for step in (3, -3, 4):
        arrival(step, h).wait_recv()
        arrival(step, 1 - h).wait_recv()
    own.wait()
    for copy in copies + relays:
        copy.wait_send()
    group = iota((48, 128), 1) >> 4
    for half in range(2):
        for i in range(8):
            block = got[(0 - i) % 8, half]
            for p in range(1, 8):
                block = jnp.where(group == p, got[(p - i) % 8, half], block)
            out_ref[half * 8 + i] = block
    marks = []
    for index in range(16):
        re, im = out_ref[index, pl.ds(0, 8, stride=6), :], out_ref[index, pl.ds(1, 8, stride=6), :]
        marks.append(((re != 0.0) | (im != 0.0)).astype(F32))
    marks = jnp.concatenate(marks, axis=0).astype(BF16)
    used_ref[...] = dot_nt(jnp.ones((8, 128), F32).astype(BF16), marks).astype(I32)


def column_tables(z, kernel_ref, phase_ref):
    l_row = iota((128, 128), 0)
    zr, zi = cis((l_row & 63) + (l_row >> 6) * 512 + z * 64, G)
    kern = kernel_ref[...]
    pr = jnp.broadcast_to(kern[7:8], (128, 128))
    pi = jnp.zeros((128, 128), F32)
    for s in range(6, -1, -1):
        pr, pi = cmul(pr, pi, zr, zi)
        pr = pr + kern[s : s + 1]
    phase_ref[0] = pr
    phase_ref[1] = pi


def row_tables(matrix_ref, twiddle_ref):
    row, lane = iota((128, 128), 0), iota((128, 128), 1)
    fc, fs = cis(row * lane, 128)
    for quarter, value in ((0, fc), (1, -fs), (2, fs), (3, fc)):
        down, right = (quarter >> 1) * 128, (quarter & 1) * 128
        for part, half in enumerate(split2(value)):
            matrix_ref[part, down : down + 128, right : right + 128] = half
    tr, ti = cis(row, G)
    ar, ai = tr, ti
    for k0 in range(1, 8):
        twiddle_ref[k0 - 1, 0] = ar
        twiddle_ref[k0 - 1, 1] = ai
        if k0 < 7:
            ar, ai = cmul(ar, ai, tr, ti)


def bin_tables(core, bins, turned, onehot_ref, hit_ref, counts_ref):
    full = jnp.concatenate([bins[...].astype(F32), jnp.zeros((64, 128), F32)], axis=0)
    turned[...] = pltpu.roll(full, core * 64, 1).T
    row128, high_row, lane8 = iota((128, 128), 0), iota((4, 128), 0), iota((8, 128), 1)
    for k0 in range(4):
        ours = turned[pl.ds(k0, 8, stride=8), :]
        other = turned[pl.ds(k0 + 4, 8, stride=8), :]
        both = jnp.where(lane8 < 64, ours, pltpu.roll(other, 64, 1)).astype(I32)
        for sub in range(8):
            found = both[sub : sub + 1]
            at = slice(128 * (8 * k0 + sub), 128 * (8 * k0 + sub) + 128)
            onehot_ref[:, at] = (row128 == (found & 127)).astype(F32).astype(BF16)
            hit_ref[:, at] = ((found >> 7) == high_row).astype(F32)
    counts_ref[...] = dot_nt(hit_ref[...].astype(BF16), onehot_ref[...])


def gather_call(*args):
    return pl.pallas_call(
        gather_kernel,
        out_shape=(
            jax.ShapeDtypeStruct((16, 48, 128), F32),
            jax.ShapeDtypeStruct((8, 128), F32),
            jax.ShapeDtypeStruct((8, 128), I32),
            jax.ShapeDtypeStruct((2, 128, 128), F32),
            jax.ShapeDtypeStruct((2, 256, 256), BF16),
            jax.ShapeDtypeStruct((7, 2, 128, 128), F32),
            jax.ShapeDtypeStruct((128, 4096), BF16),
            jax.ShapeDtypeStruct((4, 4096), F32),
            jax.ShapeDtypeStruct((4, 128), F32),
        ),
        in_specs=[pl.BlockSpec(memory_space=pltpu.HBM)] * 8,
        out_specs=(VMEM_SPEC,) * 9,
        scratch_shapes=[
            pltpu.VMEM((2, 48, 128), F32),
            pltpu.VMEM((8, 2, 48, 128), F32),
            pltpu.VMEM((64, 128), I32),
            pltpu.VMEM((128, 128), F32),
            pltpu.VMEM((1, 2), I32),
            pltpu.VMEM((2, 2, SLOTS), F32),
            pltpu.VMEM((2, 1, SLOTS), I32),
            pltpu.VMEM((2, SLOTS), I32),
            pltpu.VMEM((2, SLOTS), I32),
            pltpu.VMEM((2, 2, SLOTS), I32),
            pltpu.SemaphoreType.DMA((7,)),
            pltpu.SemaphoreType.DMA((8, 2)),
            pltpu.SemaphoreType.DMA((8,)),
            pltpu.SemaphoreType.DMA,
            pltpu.SemaphoreType.DMA((8,)),
        ],
        compiler_params=pltpu.CompilerParams(
            collective_id=0, has_side_effects=True, vmem_limit_bytes=LIMIT
        ),
    )(*(pltpu.with_memory_space_constraint(x, pltpu.HBM) for x in args))


def gridder(merged, taps_ref, kernel_ref, grid_ref, wbufs, rbufs, rows):
    sub = iota((8, 128), 0)
    lane = iota((8, 128), 1)
    _, z = places()
    sd_r, sd_i = cis(sub * lane, G)
    sc_r, sc_i = cis(sub * lane, 8)
    gd_r, gd_i = cis((z * 64 + sub * 8) * lane, G)
    gc_r, gc_i = cis((z * 64 + sub * 8) * lane, 8)
    grid_ref[...] = jnp.zeros_like(grid_ref)
    for i in range(GROUP):
        for ref in rbufs:
            ref[i, 80:160, 128:256] = jnp.zeros((80, 128), BF16)
    def build(bid, slot, i):
        which = lax.rem(lax.div(bid, 64), 2) * 8 + lax.rem(bid, 8)
        first = lax.rem(lax.div(bid, 8), 8) * 6
        keep = jnp.where(bid < BLOCKS, 1.0, 0.0)

        def field(index):
            return jnp.broadcast_to(merged[which, pl.ds(first + index, 1), :], (8, 128))

        v = field(3).astype(I32)
        index_d = v & 127
        index_c = v >> 7
        index_u = field(4).astype(I32)
        index_v = field(5).astype(I32)
        w = field(2).astype(I32)
        near = [take_lanes(t, index_d) for t in (gd_r, gd_i, sd_r, sd_i)]
        wide = [take_lanes(t, index_c) for t in (gc_r, gc_i, sc_r, sc_i)]
        group = cmul(*near[:2], *wide[:2])
        inner = cmul(*cmul(*near[2:], *wide[2:]), field(0) * keep, field(1) * keep)
        sign = (1 - 2 * (v & 1)).astype(F32)
        rows[i, 0] = group[0]
        rows[i, 1] = group[1]
        for pair in range(4):
            done = []
            for g in (2 * pair, 2 * pair + 1):
                ar, ai = cmul(jnp.broadcast_to(rows[i, 0, g : g + 1], (8, 128)), jnp.broadcast_to(rows[i, 1, g : g + 1], (8, 128)), *inner)
                low, high = slice(8 * g, 8 * g + 8), slice(64 + 8 * g, 72 + 8 * g)
                one = cmul(ar, ai, take_lanes(taps_ref[0, low], index_v), take_lanes(taps_ref[1, low], index_v))
                two = cmul(ar * sign, ai * sign, take_lanes(taps_ref[0, high], index_v), take_lanes(taps_ref[1, high], index_v))
                done.append(one + two)
            for part, start in enumerate((0, 128, 64, 192)):
                hi, lo = split2(jnp.concatenate([done[0][part], done[1][part]], axis=0))
                at = slice(start + 16 * pair, start + 16 * pair + 16)
                wbufs[slot][i, at, 0:128] = hi
                wbufs[slot][i, at, 128:256] = lo
        taps = take_lanes(kernel_ref[...], index_u)
        turned = jnp.take_along_axis(taps, (sub - w) & 7, axis=0, mode="promise_in_bounds")
        high = turned.astype(BF16).astype(F32)
        low = turned - high
        down = (w - sub + 7) >> 3
        zero = jnp.zeros((8, 128), F32)
        for pair in range(5):
            his, los = [], []
            for k in (2 * pair, 2 * pair + 1):
                hit = down == k
                his.append(jnp.where(hit, high, zero))
                los.append(jnp.where(hit, low, zero))
            hi = jnp.concatenate(his, axis=0).astype(BF16)
            at = slice(16 * pair, 16 * pair + 16)
            rbufs[slot][i, at, 0:128] = hi
            rbufs[slot][i, at, 128:256] = hi
            at = slice(80 + 16 * pair, 80 + 16 * pair + 16)
            rbufs[slot][i, at, 0:128] = jnp.concatenate(los, axis=0).astype(BF16)

    def place(bid, slot, i):
        res = dot_nt(rbufs[slot][i], wbufs[slot][i])
        start = pl.multiple_of(lax.rem(lax.div(bid, 4), 16) * 64, 64)
        grid_ref[pl.ds(start, 80), :] += res[:80] + res[80:]

    def open_round(first):
        for i in range(GROUP):
            build(4 * (first + i), 0, i)
        for i in range(GROUP):
            place(4 * (first + i), 0, i)
            build(4 * (first + GROUP + i), 1, i)
        return tuple(jnp.int32(4 * (first + GROUP + i)) for i in range(GROUP))

    return build, place, open_round


def grid_kernel(
    merged, used_ref, taps_ref, kernel_ref, grid_ref, wbuf_a, rbuf_a, wbuf_b, rbuf_b, rows, used, order, sem
):
    copy = pltpu.make_async_copy(used_ref, used, sem)
    copy.start()
    build, place, open_round = gridder(
        merged, taps_ref, kernel_ref, grid_ref, (wbuf_a, wbuf_b), (rbuf_a, rbuf_b), rows
    )
    opened = open_round(TAIL)
    copy.wait()
    total = jnp.int32(0)
    for half in range(2):
        for i in (1, 2, 3, 5, 6, 7):
            for g in range(8):
                order[total] = half * 64 + g * 8 + i
                total = total + jnp.where(used[0, half * 64 + i * 8 + g] > 0, 1, 0)
    for i in range(2 * GROUP):
        order[total + i] = BLOCKS

    def step(it, before):
        first = tuple(order[2 * GROUP * it + i] for i in range(GROUP))
        second = tuple(order[2 * GROUP * it + GROUP + i] for i in range(GROUP))
        for i in range(GROUP):
            place(before[i], 1, i)
            build(first[i], 0, i)
        for i in range(GROUP):
            place(first[i], 0, i)
            build(second[i], 1, i)
        return second

    rounds = (total + 2 * GROUP - 1) // (2 * GROUP)
    last = lax.fori_loop(0, rounds, step, opened)
    for i in range(GROUP):
        place(last[i], 1, i)


def grid_call(merged, used, phase, kernel_t):
    return pl.pallas_call(
        grid_kernel,
        out_shape=jax.ShapeDtypeStruct((1040, 256), F32),
        in_specs=[VMEM_SPEC] * 4,
        out_specs=VMEM_SPEC,
        scratch_shapes=[
            pltpu.VMEM((GROUP, 256, 256), BF16),
            pltpu.VMEM((GROUP, 160, 256), BF16),
            pltpu.VMEM((GROUP, 256, 256), BF16),
            pltpu.VMEM((GROUP, 160, 256), BF16),
            pltpu.VMEM((GROUP, 2, 8, 128), F32),
            pltpu.SMEM((8, 128), I32),
            pltpu.SMEM((BLOCKS + 2 * GROUP,), I32),
            pltpu.SemaphoreType.DMA,
        ],
        compiler_params=pltpu.CompilerParams(vmem_limit_bytes=LIMIT),
    )(merged, used, phase, kernel_t)


def tail_kernel(
    grid_ref, merged, taps_ref, kernel_ref, matrix_ref, tw_ref, onehot, hit_ref, counts, power_ref, spectrum_ref,
    first_ref, wbuf_a, rbuf_a, wbuf_b, rbuf_b, rows_ref, bh_ref, bl_ref, left, piece, partner, summed, landed, counts_in, counts_z, counts_plane,
    totals, totals_in, totals_z, totals_plane, sems,
):
    h, z = places()
    freq = lax.axis_index("freq")
    quad, core = freq // 2, freq % 2
    me = h * 16 + freq
    me_pair = h * 8 + quad
    far_first = (4, 3, 5, 2, 6, 1, 7)
    row, spot = me_pair // 4, me_pair % 4

    def neighbour(down, right):
        return ((row + down) % 4) * 4 + (spot + right) % 4


    def chip(index, to_core):
        return {"freq": (index % 8) * 2 + to_core, "base": (index // 8) * 8 + z}

    def column(step, to_core):
        return {"freq": quad * 2 + to_core, "base": h * 8 + (z + step) % 8}

    barrier = pltpu.get_barrier_semaphore()

    def greet(device):
        pl.semaphore_signal(barrier, 1, device_id=device, device_id_type=MESH)

    for step in far_first:
        for to_core in range(2):
            greet(column(step, to_core))
    for step in STEPS:
        for to_core in range(2):
            greet(chip(neighbour(*step), to_core))
    greet(chip(me_pair, 1 - core))

    build, place, open_round = gridder(
        merged, taps_ref, kernel_ref, first_ref, (wbuf_a, wbuf_b), (rbuf_a, rbuf_b), rows_ref
    )
    open_round(0)

    def step(it, _):
        for i in range(GROUP):
            place(4 * (2 * GROUP * it - GROUP + i), 1, i)
            build(4 * (2 * GROUP * it + i), 0, i)
        for i in range(GROUP):
            place(4 * (2 * GROUP * it + i), 0, i)
            build(4 * (2 * GROUP * it + GROUP + i), 1, i)
        return 0

    lax.fori_loop(1, TAIL // (2 * GROUP), step, 0)
    for i in range(GROUP):
        place(4 * (TAIL - GROUP + i), 1, i)

    root = math.sqrt(0.5)
    slot_of = (0, 2, 4, 6, 1, 3, 5, 7)
    for rows in range(8):
        u = [
            (
                grid_ref[128 * a + 16 * rows : 128 * a + 16 * rows + 16, 0:128]
                + first_ref[128 * a + 16 * rows : 128 * a + 16 * rows + 16, 0:128],
                grid_ref[128 * a + 16 * rows : 128 * a + 16 * rows + 16, 128:256]
                + first_ref[128 * a + 16 * rows : 128 * a + 16 * rows + 16, 128:256],
            )
            for a in range(8)
        ]

        def add(x, y):
            return x[0] + y[0], x[1] + y[1]

        def sub2(x, y):
            return x[0] - y[0], x[1] - y[1]

        def four(a, b, c, d):
            s, t = add(a, c), sub2(a, c)
            p, q = add(b, d), sub2(b, d)
            mq = (q[1], -q[0])
            return add(s, p), add(t, mq), sub2(s, p), sub2(t, mq)

        even = four(u[0], u[2], u[4], u[6])
        odd = four(u[1], u[3], u[5], u[7])
        o1 = ((odd[1][0] + odd[1][1]) * root, (odd[1][1] - odd[1][0]) * root)
        o2 = (odd[2][1], -odd[2][0])
        o3 = ((odd[3][1] - odd[3][0]) * root, -(odd[3][0] + odd[3][1]) * root)
        odd = (odd[0], o1, o2, o3)
        spectrum = [add(even[k], odd[k]) for k in range(4)] + [sub2(even[k], odd[k]) for k in range(4)]
        at = slice(16 * rows, 16 * rows + 16)
        for k0 in range(8):
            xr, xi = spectrum[k0]
            if k0:
                xr, xi = cmul(xr, xi, tw_ref[k0 - 1, 0, at], tw_ref[k0 - 1, 1, at])
            col = slice(128 * slot_of[k0], 128 * slot_of[k0] + 128)
            for base, value in ((0, xr), (128, xi)):
                hi, lo = split2(value)
                bh_ref[base + 16 * rows : base + 16 * rows + 16, col] = hi
                bl_ref[base + 16 * rows : base + 16 * rows + 16, col] = lo
    low_half = iota((128, 128), 1) < 64
    for k0 in range(4):
        col = slice(256 * k0, 256 * k0 + 256)
        full = dot_nn(matrix_ref[0], bh_ref[:, col]) + dot_nn(matrix_ref[0], bl_ref[:, col]) + dot_nn(matrix_ref[1], bh_ref[:, col])
        power = (full[:128] * full[:128] + full[128:] * full[128:]) * NORM
        pa, pb = power[:, :128], power[:, 128:]
        ra, rb = pltpu.roll(pa, 64, 1), pltpu.roll(pb, 64, 1)
        for side, block in ((0, jnp.where(low_half, pa, rb)), (1, jnp.where(low_half, ra, pb))):
            block = block.reshape(8, 2, 8, 128)
            for cc in range(2):
                piece[cc, k0, side] = block[:, cc]

    pl.semaphore_wait(barrier, 45)

    def remote(source, target, number, device):
        return pltpu.make_async_remote_copy(
            src_ref=source, dst_ref=target, send_sem=sems.at[2 * number], recv_sem=sems.at[2 * number + 1],
            device_id=device, device_id_type=MESH,
        )

    def whole(ref, count, number):
        return remote(ref.at[0:count], ref.at[0:count], number, chip(me_pair, 1 - core))

    pair = remote(piece.at[1 - core], partner, 0, chip(me_pair, 1 - core))
    pair.start()

    def plane_send(buf, slots, number):
        @pl.when(core == 0)
        def _():
            remote(buf, slots.at[me], number, chip(me_pair, 1)).start()

        for step in STEPS:
            remote(buf, slots.at[me], number, chip(neighbour(*step), 1)).start()

    def plane_sum(buf, slots, result, number):
        slots[me] = buf[...]
        whole(slots, 31, number).wait_recv()
        total = slots[0]
        for index in range(1, 32):
            total = total + slots[index]
        result[...] = total

    def column_send(buf, slots, number):
        for step in far_first:
            for to_core in range(2):
                remote(buf, slots.at[z], number, column(step, to_core)).start()
        remote(buf, slots.at[z], number, chip(me_pair, 0)).start()

    def column_sum(buf, slots, number):
        @pl.when(core == 0)
        def _():
            whole(slots, 8, number).wait_recv()

        @pl.when(core == 1)
        def _():
            slots[z] = buf[...]
            whole(slots, 7, number).wait_recv()

        total = slots[0]
        for index in range(1, 8):
            total = total + slots[index]
        return total

    def plane_sent(slots, number):
        @pl.when(core == 0)
        def _():
            whole(slots, 16, number).wait_send()

        @pl.when(core == 1)
        def _():
            whole(slots, 15, number).wait_send()

    plane_send(counts, counts_in, 2)
    pair.wait_recv()
    for k0 in range(4):
        for side in range(2):
            for q in range(8):
                summed[side * 8 + q, k0] = piece[core, k0, side, q] + partner[k0, side, q]
    for step in STEPS:
        peer = neighbour(*step)
        remote(summed.at[peer], landed.at[me_pair], 1, chip(peer, core)).start()
    landed[me_pair] = summed[me_pair]

    @pl.when(core == 1)
    def _():
        plane_sum(counts, counts_in, counts_plane, 2)
        column_send(counts_plane, counts_z, 3)

    whole(landed, 15, 1).wait_recv()
    total = landed[0]
    for index in range(1, 16):
        total = total + landed[index]
    for k0 in range(4):
        for sub in range(8):
            at = slice(128 * (8 * k0 + sub), 128 * (8 * k0 + sub) + 128)
            hit = hit_ref[:, at]
            value = total[k0][sub : sub + 1]
            p0 = value.astype(BF16).astype(F32)
            p1 = (value - p0).astype(BF16).astype(F32)
            left[0:4, at] = hit * p0
            left[4:8, at] = hit * p1
            left[8:12, at] = hit * (value - p0 - p1)
            left[12:16, at] = jnp.zeros((4, 128), F32)
    got = dot_nt(left[...].astype(BF16), onehot[...])
    totals[...] = got[0:4] + got[4:8] + got[8:12]
    plane_send(totals, totals_in, 4)
    for k0 in range(8):
        half = (k0 // 4) * 64
        power_ref[pl.ds(k0, 8, stride=8), :] = total[k0 % 4][:, half : half + 64]
    all_counts = column_sum(counts_plane, counts_z, 3)

    @pl.when(core == 1)
    def _():
        plane_sum(totals, totals_in, totals_plane, 4)
        column_send(totals_plane, totals_z, 5)

    pair.wait_send()
    whole(landed, 15, 1).wait_send()
    plane_sent(counts_in, 2)
    plane_sent(totals_in, 4)

    @pl.when(core == 1)
    def _():
        whole(counts_in, 15, 3).wait_send()

    spectrum_ref[...] = column_sum(totals_plane, totals_z, 5) / all_counts

    @pl.when(core == 1)
    def _():
        whole(totals_in, 15, 5).wait_send()


def tail_call(*args):
    small = (4, 128)
    return pl.pallas_call(
        tail_kernel,
        out_shape=(jax.ShapeDtypeStruct((64, 64), F32), jax.ShapeDtypeStruct((4, 128), F32)),
        in_specs=[VMEM_SPEC] * 9,
        out_specs=(VMEM_SPEC,) * 2,
        scratch_shapes=[
            pltpu.VMEM((1040, 256), F32),
            pltpu.VMEM((GROUP, 256, 256), BF16),
            pltpu.VMEM((GROUP, 160, 256), BF16),
            pltpu.VMEM((GROUP, 256, 256), BF16),
            pltpu.VMEM((GROUP, 160, 256), BF16),
            pltpu.VMEM((GROUP, 2, 8, 128), F32),
            pltpu.VMEM((256, 1024), BF16),
            pltpu.VMEM((256, 1024), BF16),
            pltpu.VMEM((16, 4096), F32),
            pltpu.VMEM((2, 4, 2, 8, 8, 128), F32),
            pltpu.VMEM((4, 2, 8, 8, 128), F32),
            pltpu.VMEM((16, 4, 8, 128), F32),
            pltpu.VMEM((16, 4, 8, 128), F32),
            pltpu.VMEM((32,) + small, F32),
            pltpu.VMEM((8,) + small, F32),
            pltpu.VMEM(small, F32),
            pltpu.VMEM(small, F32),
            pltpu.VMEM((32,) + small, F32),
            pltpu.VMEM((8,) + small, F32),
            pltpu.VMEM(small, F32),
            pltpu.SemaphoreType.DMA((12,)),
        ],
        compiler_params=pltpu.CompilerParams(
            collective_id=1, has_side_effects=True, vmem_limit_bytes=LIMIT
        ),
    )(*args)


def store_kernel(power_ref, spectrum_ref, power_out, spectrum_out, sems):
    first = pltpu.make_async_copy(power_ref, power_out, sems.at[0])
    second = pltpu.make_async_copy(spectrum_ref, spectrum_out, sems.at[1])
    first.start()
    second.start()
    first.wait()
    second.wait()


def store_call(power, spectrum):
    return pl.pallas_call(
        store_kernel,
        out_shape=(jax.ShapeDtypeStruct((64, 64), F32), jax.ShapeDtypeStruct((4, 128), F32)),
        in_specs=[VMEM_SPEC] * 2,
        out_specs=(pl.BlockSpec(memory_space=pltpu.HBM),) * 2,
        scratch_shapes=[pltpu.SemaphoreType.DMA((2,))],
        compiler_params=pltpu.CompilerParams(vmem_limit_bytes=LIMIT),
    )(power, spectrum)


def per_device(visibility, tile_of, u_within, v_cell, kernel_index, kernel, live_count, bin_map):
    merged, kernel_rows, used, phase, matrix, twiddle, onehot, hit, counts = gather_call(
        live_count.T,
        visibility,
        tile_of.transpose(0, 2, 1),
        u_within,
        v_cell,
        kernel_index,
        kernel.T,
        bin_map,
    )
    grid = grid_call(merged, used, phase, kernel_rows)
    power, spectrum = tail_call(grid, merged, phase, kernel_rows, matrix, twiddle, onehot, hit, counts)
    power, spectrum = store_call(power, spectrum)
    return power, spectrum.reshape(NBINS)


def solution(mesh):
    return jax.shard_map(
        per_device,
        mesh=mesh,
        in_specs=(
            P(None, "freq", "base"),
            P("freq", "base", None),
            P("freq", "base"),
            P("freq", "base"),
            P(None, "freq", "base"),
            P(),
            P("freq", "base"),
            P("base", None),
        ),
        out_specs=(P("freq", "base"), P()),
        check_vma=False,
    )
```

```python
import functools
import math

import jax
import jax.numpy as jnp
from jax import lax
from jax.experimental import pallas as pl
from jax.experimental.pallas import tpu as pltpu
from jax.sharding import PartitionSpec as P

G = 1024
NBINS = 512
KW = 8
OVER = 128
SLOTS = 512
TILES = 16
BLOCKS = 128
GROUP = 4
TAIL = 24
F32 = jnp.float32
BF16 = jnp.bfloat16
I32 = jnp.int32
MESH = pl.DeviceIdType.MESH
VMEM_SPEC = pl.BlockSpec(memory_space=pltpu.VMEM)
LIMIT = 16 * 1024 * 1024
STEPS = sorted(
    ((down, right) for down in range(4) for right in range(4) if down or right),
    key=lambda step: (-sum(min(part, 4 - part) for part in step), step),
)
NORM = 1.0 / (32 * 8192)


def iota(shape, dim):
    return lax.broadcasted_iota(I32, shape, dim)


def cis(phase, period):
    phase = phase & (period - 1)
    phase = jnp.where(phase >= period // 2, phase - period, phase)
    angle = phase.astype(F32) * (2.0 * math.pi / period)
    return jnp.cos(angle), -jnp.sin(angle)


def cmul(ar, ai, br, bi):
    return ar * br - ai * bi, ar * bi + ai * br


def split2(x):
    hi = x.astype(BF16)
    return hi, (x - hi.astype(F32)).astype(BF16)


def dot_nt(a, b):
    return lax.dot_general(a, b, (((1,), (1,)), ((), ())), preferred_element_type=F32)


def dot_nn(a, b):
    return lax.dot_general(a, b, (((1,), (0,)), ((), ())), preferred_element_type=F32)


def take_lanes(table, index):
    return jnp.take_along_axis(table, index, axis=1, mode="promise_in_bounds")


def bin_channel(ch, z, vis_ref, tile_ref, within_ref, vcell_ref, kidx_ref, live, upper):
    tile = tile_ref[ch]
    lane = iota((1, SLOTS), 1)
    is_live = lane < live
    member = (tile == iota((TILES, SLOTS), 0)) & is_live
    before = dot_nn(member.astype(BF16), upper)
    rank = jnp.sum(jnp.where(member, before, 0.0), axis=0, keepdims=True).astype(I32)
    block = tile * 4 + (rank >> 4)
    position = (block >> 3) * 128 + (((block & 7) + z) & 7) * 16 + (rank & 15)
    position = jnp.where(is_live, position, -1)
    row = jnp.minimum(within_ref[ch : ch + 1, :], (G - KW) - tile * 64)
    column = vcell_ref[ch : ch + 1, :]
    parts = []
    for part in range(2):
        value = vis_ref[part, ch : ch + 1, :]
        for _ in range(3):
            piece = value.astype(BF16).astype(F32)
            parts.append(piece)
            value = value - piece
    parts += [
        row.astype(F32),
        (column >> 3).astype(F32),
        (column & 7).astype(F32),
        kidx_ref[0, ch : ch + 1, :].astype(F32),
        kidx_ref[1, ch : ch + 1, :].astype(F32),
        jnp.ones((1, SLOTS), F32),
        jnp.zeros((4, SLOTS), F32),
    ]
    payload = jnp.concatenate(parts, axis=0).astype(BF16)
    out = []
    for part in range(4):
        place = (iota((256, SLOTS), 0) + part * 256 == position).astype(F32).astype(BF16)
        got = dot_nt(payload, place)
        out.append(
            jnp.concatenate(
                [
                    got[0:1] + got[1:2] + got[2:3],
                    got[3:4] + got[4:5] + got[5:6],
                    got[6:7],
                    got[7:8] * 8.0 + got[8:9],
                    got[9:10],
                    got[10:11],
                    got[11:12],
                    jnp.zeros((1, 256), F32),
                ],
                axis=0,
            )
        )
    return out


def places():
    base = lax.axis_index("base")
    return base // 8, base % 8


def gather_kernel(
    live_hbm,
    vis_hbm,
    tile_hbm,
    within_hbm,
    vcell_hbm,
    kidx_hbm,
    kernel_hbm,
    bins_ref,
    out_ref,
    kernel_ref,
    used_ref,
    phase_ref,
    matrix_ref,
    twiddle_ref,
    onehot_ref,
    hit_ref,
    counts_ref,
    packed,
    got,
    bins,
    turned,
    live_ref,
    vis_ref,
    tile_ref,
    within_ref,
    vcell_ref,
    kidx_ref,
    send,
    land,
    relay,
    local,
    fetched,
):
    inputs = (
        (live_hbm, live_ref),
        (tile_hbm, tile_ref),
        (vis_hbm, vis_ref),
        (within_hbm, within_ref),
        (vcell_hbm, vcell_ref),
        (kidx_hbm, kidx_ref),
        (kernel_hbm, kernel_ref),
    )
    loads = [
        pltpu.make_async_copy(source, place, fetched.at[index])
        for index, (source, place) in enumerate(inputs)
    ]
    for load in loads:
        load.start()
    h, z = places()
    freq = lax.axis_index("freq")
    at = pl.multiple_of((freq // 2) * 128, 128)
    fetch = pltpu.make_async_copy(bins_ref.at[:, pl.ds(at, 128)], bins, fetched.at[7])
    fetch.start()

    def device(side, step):
        return {"base": side * 8 + (z + step + 8) % 8}

    barrier = pltpu.get_barrier_semaphore()
    for side, step in ((1 - h, 2), (1 - h, -2), (h, 2), (h, -2), (1 - h, 0), (h, 1), (h, -1)):
        pl.semaphore_signal(barrier, 1, device_id=device(side, step), device_id_type=MESH)

    upper = (iota((SLOTS, SLOTS), 0) < iota((SLOTS, SLOTS), 1)).astype(F32).astype(BF16)
    for load in loads:
        load.wait()
    for ch in range(2):
        live = live_ref[0:1, ch : ch + 1]
        parts = bin_channel(
            ch, z, vis_ref, tile_ref, within_ref, vcell_ref, kidx_ref, live, upper
        )
        for index, part in enumerate(parts):
            packed[ch, 12 * index : 12 * index + 6] = part[:6, :128]
            packed[ch, 12 * index + 6 : 12 * index + 12] = part[:6, 128:]
    pl.semaphore_wait(barrier, 7)

    def direct(side, step, number):
        return pltpu.make_async_remote_copy(
            src_ref=packed.at[side],
            dst_ref=got.at[z, h],
            send_sem=send.at[number],
            recv_sem=land.at[z, h],
            device_id=device(side, step),
            device_id_type=MESH,
        )

    def arrival(step, side):
        zz = (z + step + 8) % 8
        return pltpu.make_async_remote_copy(
            src_ref=got.at[zz, side],
            dst_ref=got.at[zz, side],
            send_sem=send.at[0],
            recv_sem=land.at[zz, side],
            device_id=device(1 - h, 0),
            device_id_type=MESH,
        )

    copies = []
    for side, step in ((1 - h, 2), (1 - h, -2), (h, 2), (h, -2), (1 - h, 0), (h, 1), (h, -1)):
        copies.append(direct(side, step, len(copies)))
    for copy in copies:
        copy.start()
    own = pltpu.make_async_copy(packed.at[h], got.at[z, h], local)
    own.start()

    column_tables(z, kernel_ref, phase_ref)
    row_tables(matrix_ref, twiddle_ref)
    fetch.wait()
    bin_tables(freq % 2, bins, turned, onehot_ref, hit_ref, counts_ref)

    relays = []

    def pass_on(source, side, step):
        zz = (z + source + 8) % 8
        copy = pltpu.make_async_remote_copy(
            src_ref=got.at[zz, side],
            dst_ref=got.at[zz, side],
            send_sem=relay.at[len(relays)],
            recv_sem=land.at[zz, side],
            device_id=device(h, step),
            device_id_type=MESH,
        )
        copy.start()
        relays.append(copy)

    arrival(0, 1 - h).wait_recv()
    pass_on(0, 1 - h, 1)
    pass_on(0, 1 - h, -1)
    arrival(-2, h).wait_recv()
    pass_on(-2, h, 2)
    pass_on(-2, h, 1)
    arrival(2, h).wait_recv()
    pass_on(2, h, -1)
    arrival(2, 1 - h).wait_recv()
    pass_on(2, 1 - h, -2)
    pass_on(2, 1 - h, -1)
    arrival(-2, 1 - h).wait_recv()
    pass_on(-2, 1 - h, 1)
    for step in (1, -1):
        arrival(step, h).wait_recv()
        arrival(step, 1 - h).wait_recv()
    for step in (3, -3, 4):
        arrival(step, h).wait_recv()
        arrival(step, 1 - h).wait_recv()
    own.wait()
    for copy in copies + relays:
        copy.wait_send()
    group = iota((48, 128), 1) >> 4
    for half in range(2):
        for i in range(8):
            block = got[(0 - i) % 8, half]
            for p in range(1, 8):
                block = jnp.where(group == p, got[(p - i) % 8, half], block)
            out_ref[half * 8 + i] = block
    marks = []
    for index in range(16):
        re, im = out_ref[index, pl.ds(0, 8, stride=6), :], out_ref[index, pl.ds(1, 8, stride=6), :]
        marks.append(((re != 0.0) | (im != 0.0)).astype(F32))
    marks = jnp.concatenate(marks, axis=0).astype(BF16)
    used_ref[...] = dot_nt(jnp.ones((8, 128), F32).astype(BF16), marks).astype(I32)


def column_tables(z, kernel_ref, phase_ref):
    l_row = iota((128, 128), 0)
    zr, zi = cis((l_row & 63) + (l_row >> 6) * 512 + z * 64, G)
    kern = kernel_ref[...]
    pr = jnp.broadcast_to(kern[7:8], (128, 128))
    pi = jnp.zeros((128, 128), F32)
    for s in range(6, -1, -1):
        pr, pi = cmul(pr, pi, zr, zi)
        pr = pr + kern[s : s + 1]
    phase_ref[0] = pr
    phase_ref[1] = pi


def row_tables(matrix_ref, twiddle_ref):
    row, lane = iota((128, 128), 0), iota((128, 128), 1)
    fc, fs = cis(row * lane, 128)
    for quarter, value in ((0, fc), (1, -fs), (2, fs), (3, fc)):
        down, right = (quarter >> 1) * 128, (quarter & 1) * 128
        for part, half in enumerate(split2(value)):
            matrix_ref[part, down : down + 128, right : right + 128] = half
    tr, ti = cis(row, G)
    ar, ai = tr, ti
    for k0 in range(1, 8):
        twiddle_ref[k0 - 1, 0] = ar
        twiddle_ref[k0 - 1, 1] = ai
        if k0 < 7:
            ar, ai = cmul(ar, ai, tr, ti)


def bin_tables(core, bins, turned, onehot_ref, hit_ref, counts_ref):
    full = jnp.concatenate([bins[...].astype(F32), jnp.zeros((64, 128), F32)], axis=0)
    turned[...] = pltpu.roll(full, core * 64, 1).T
    row128, high_row, lane8 = iota((128, 128), 0), iota((4, 128), 0), iota((8, 128), 1)
    for k0 in range(4):
        ours = turned[pl.ds(k0, 8, stride=8), :]
        other = turned[pl.ds(k0 + 4, 8, stride=8), :]
        both = jnp.where(lane8 < 64, ours, pltpu.roll(other, 64, 1)).astype(I32)
        for sub in range(8):
            found = both[sub : sub + 1]
            at = slice(128 * (8 * k0 + sub), 128 * (8 * k0 + sub) + 128)
            onehot_ref[:, at] = (row128 == (found & 127)).astype(F32).astype(BF16)
            hit_ref[:, at] = ((found >> 7) == high_row).astype(F32)
    counts_ref[...] = dot_nt(hit_ref[...].astype(BF16), onehot_ref[...])


def gather_call(*args):
    return pl.pallas_call(
        gather_kernel,
        out_shape=(
            jax.ShapeDtypeStruct((16, 48, 128), F32),
            jax.ShapeDtypeStruct((8, 128), F32),
            jax.ShapeDtypeStruct((8, 128), I32),
            jax.ShapeDtypeStruct((2, 128, 128), F32),
            jax.ShapeDtypeStruct((2, 256, 256), BF16),
            jax.ShapeDtypeStruct((7, 2, 128, 128), F32),
            jax.ShapeDtypeStruct((128, 4096), BF16),
            jax.ShapeDtypeStruct((4, 4096), F32),
            jax.ShapeDtypeStruct((4, 128), F32),
        ),
        in_specs=[pl.BlockSpec(memory_space=pltpu.HBM)] * 8,
        out_specs=(VMEM_SPEC,) * 9,
        scratch_shapes=[
            pltpu.VMEM((2, 48, 128), F32),
            pltpu.VMEM((8, 2, 48, 128), F32),
            pltpu.VMEM((64, 128), I32),
            pltpu.VMEM((128, 128), F32),
            pltpu.VMEM((1, 2), I32),
            pltpu.VMEM((2, 2, SLOTS), F32),
            pltpu.VMEM((2, 1, SLOTS), I32),
            pltpu.VMEM((2, SLOTS), I32),
            pltpu.VMEM((2, SLOTS), I32),
            pltpu.VMEM((2, 2, SLOTS), I32),
            pltpu.SemaphoreType.DMA((7,)),
            pltpu.SemaphoreType.DMA((8, 2)),
            pltpu.SemaphoreType.DMA((8,)),
            pltpu.SemaphoreType.DMA,
            pltpu.SemaphoreType.DMA((8,)),
        ],
        compiler_params=pltpu.CompilerParams(
            collective_id=0, has_side_effects=True, vmem_limit_bytes=LIMIT
        ),
    )(*(pltpu.with_memory_space_constraint(x, pltpu.HBM) for x in args))


def gridder(merged, taps_ref, kernel_ref, grid_ref, wbufs, rbufs, rows):
    sub = iota((8, 128), 0)
    lane = iota((8, 128), 1)
    _, z = places()
    sd_r, sd_i = cis(sub * lane, G)
    sc_r, sc_i = cis(sub * lane, 8)
    gd_r, gd_i = cis((z * 64 + sub * 8) * lane, G)
    gc_r, gc_i = cis((z * 64 + sub * 8) * lane, 8)
    grid_ref[...] = jnp.zeros_like(grid_ref)
    for i in range(GROUP):
        for ref in rbufs:
            ref[i, 80:160, 128:256] = jnp.zeros((80, 128), BF16)
    def build(bid, slot, i):
        which = lax.rem(lax.div(bid, 64), 2) * 8 + lax.rem(bid, 8)
        first = lax.rem(lax.div(bid, 8), 8) * 6
        keep = jnp.where(bid < BLOCKS, 1.0, 0.0)

        def field(index):
            return jnp.broadcast_to(merged[which, pl.ds(first + index, 1), :], (8, 128))

        v = field(3).astype(I32)
        index_d = v & 127
        index_c = v >> 7
        index_u = field(4).astype(I32)
        index_v = field(5).astype(I32)
        w = field(2).astype(I32)
        near = [take_lanes(t, index_d) for t in (gd_r, gd_i, sd_r, sd_i)]
        wide = [take_lanes(t, index_c) for t in (gc_r, gc_i, sc_r, sc_i)]
        group = cmul(*near[:2], *wide[:2])
        inner = cmul(*cmul(*near[2:], *wide[2:]), field(0) * keep, field(1) * keep)
        sign = (1 - 2 * (v & 1)).astype(F32)
        rows[i, 0] = group[0]
        rows[i, 1] = group[1]
        for pair in range(4):
            done = []
            for g in (2 * pair, 2 * pair + 1):
                ar, ai = cmul(jnp.broadcast_to(rows[i, 0, g : g + 1], (8, 128)), jnp.broadcast_to(rows[i, 1, g : g + 1], (8, 128)), *inner)
                low, high = slice(8 * g, 8 * g + 8), slice(64 + 8 * g, 72 + 8 * g)
                one = cmul(ar, ai, take_lanes(taps_ref[0, low], index_v), take_lanes(taps_ref[1, low], index_v))
                two = cmul(ar * sign, ai * sign, take_lanes(taps_ref[0, high], index_v), take_lanes(taps_ref[1, high], index_v))
                done.append(one + two)
            for part, start in enumerate((0, 128, 64, 192)):
                hi, lo = split2(jnp.concatenate([done[0][part], done[1][part]], axis=0))
                at = slice(start + 16 * pair, start + 16 * pair + 16)
                wbufs[slot][i, at, 0:128] = hi
                wbufs[slot][i, at, 128:256] = lo
        taps = take_lanes(kernel_ref[...], index_u)
        turned = jnp.take_along_axis(taps, (sub - w) & 7, axis=0, mode="promise_in_bounds")
        high = turned.astype(BF16).astype(F32)
        low = turned - high
        down = (w - sub + 7) >> 3
        zero = jnp.zeros((8, 128), F32)
        for pair in range(5):
            his, los = [], []
            for k in (2 * pair, 2 * pair + 1):
                hit = down == k
                his.append(jnp.where(hit, high, zero))
                los.append(jnp.where(hit, low, zero))
            hi = jnp.concatenate(his, axis=0).astype(BF16)
            at = slice(16 * pair, 16 * pair + 16)
            rbufs[slot][i, at, 0:128] = hi
            rbufs[slot][i, at, 128:256] = hi
            at = slice(80 + 16 * pair, 80 + 16 * pair + 16)
            rbufs[slot][i, at, 0:128] = jnp.concatenate(los, axis=0).astype(BF16)

    def place(bid, slot, i):
        res = dot_nt(rbufs[slot][i], wbufs[slot][i])
        start = pl.multiple_of(lax.rem(lax.div(bid, 4), 16) * 64, 64)
        grid_ref[pl.ds(start, 80), :] += res[:80] + res[80:]

    def open_round(first):
        for i in range(GROUP):
            build(4 * (first + i), 0, i)
        for i in range(GROUP):
            place(4 * (first + i), 0, i)
            build(4 * (first + GROUP + i), 1, i)
        return tuple(jnp.int32(4 * (first + GROUP + i)) for i in range(GROUP))

    return build, place, open_round


def grid_kernel(
    merged, used_ref, taps_ref, kernel_ref, grid_ref, wbuf_a, rbuf_a, wbuf_b, rbuf_b, rows, used, order, sem
):
    copy = pltpu.make_async_copy(used_ref, used, sem)
    copy.start()
    build, place, open_round = gridder(
        merged, taps_ref, kernel_ref, grid_ref, (wbuf_a, wbuf_b), (rbuf_a, rbuf_b), rows
    )
    opened = open_round(TAIL)
    copy.wait()
    total = jnp.int32(0)
    for half in range(2):
        for i in (1, 2, 3, 5, 6, 7):
            for g in range(8):
                order[total] = half * 64 + g * 8 + i
                total = total + jnp.where(used[0, half * 64 + i * 8 + g] > 0, 1, 0)
    for i in range(2 * GROUP):
        order[total + i] = BLOCKS

    def step(it, before):
        first = tuple(order[2 * GROUP * it + i] for i in range(GROUP))
        second = tuple(order[2 * GROUP * it + GROUP + i] for i in range(GROUP))
        for i in range(GROUP):
            place(before[i], 1, i)
            build(first[i], 0, i)
        for i in range(GROUP):
            place(first[i], 0, i)
            build(second[i], 1, i)
        return second

    rounds = (total + 2 * GROUP - 1) // (2 * GROUP)
    last = lax.fori_loop(0, rounds, step, opened)
    for i in range(GROUP):
        place(last[i], 1, i)


def grid_call(merged, used, phase, kernel_t):
    return pl.pallas_call(
        grid_kernel,
        out_shape=jax.ShapeDtypeStruct((1040, 256), F32),
        in_specs=[VMEM_SPEC] * 4,
        out_specs=VMEM_SPEC,
        scratch_shapes=[
            pltpu.VMEM((GROUP, 256, 256), BF16),
            pltpu.VMEM((GROUP, 160, 256), BF16),
            pltpu.VMEM((GROUP, 256, 256), BF16),
            pltpu.VMEM((GROUP, 160, 256), BF16),
            pltpu.VMEM((GROUP, 2, 8, 128), F32),
            pltpu.SMEM((8, 128), I32),
            pltpu.SMEM((BLOCKS + 2 * GROUP,), I32),
            pltpu.SemaphoreType.DMA,
        ],
        compiler_params=pltpu.CompilerParams(vmem_limit_bytes=LIMIT),
    )(merged, used, phase, kernel_t)


def tail_kernel(
    grid_ref, merged, taps_ref, kernel_ref, matrix_ref, tw_ref, onehot, hit_ref, counts, power_ref, spectrum_ref,
    first_ref, wbuf_a, rbuf_a, wbuf_b, rbuf_b, rows_ref, bh_ref, bl_ref, left, piece, partner, summed, landed, counts_in, counts_z, counts_plane,
    totals, totals_in, totals_z, totals_plane, sems,
):
    h, z = places()
    freq = lax.axis_index("freq")
    quad, core = freq // 2, freq % 2
    me = h * 16 + freq
    me_pair = h * 8 + quad
    far_first = (4, 3, 5, 2, 6, 1, 7)
    row, spot = me_pair // 4, me_pair % 4

    def neighbour(down, right):
        return ((row + down) % 4) * 4 + (spot + right) % 4


    def chip(index, to_core):
        return {"freq": (index % 8) * 2 + to_core, "base": (index // 8) * 8 + z}

    def column(step, to_core):
        return {"freq": quad * 2 + to_core, "base": h * 8 + (z + step) % 8}

    barrier = pltpu.get_barrier_semaphore()

    def greet(device):
        pl.semaphore_signal(barrier, 1, device_id=device, device_id_type=MESH)

    for step in far_first:
        for to_core in range(2):
            greet(column(step, to_core))
    for step in STEPS:
        for to_core in range(2):
            greet(chip(neighbour(*step), to_core))
    greet(chip(me_pair, 1 - core))

    build, place, open_round = gridder(
        merged, taps_ref, kernel_ref, first_ref, (wbuf_a, wbuf_b), (rbuf_a, rbuf_b), rows_ref
    )
    open_round(0)

    def step(it, _):
        for i in range(GROUP):
            place(4 * (2 * GROUP * it - GROUP + i), 1, i)
            build(4 * (2 * GROUP * it + i), 0, i)
        for i in range(GROUP):
            place(4 * (2 * GROUP * it + i), 0, i)
            build(4 * (2 * GROUP * it + GROUP + i), 1, i)
        return 0

    lax.fori_loop(1, TAIL // (2 * GROUP), step, 0)
    for i in range(GROUP):
        place(4 * (TAIL - GROUP + i), 1, i)

    root = math.sqrt(0.5)
    slot_of = (0, 2, 4, 6, 1, 3, 5, 7)
    for rows in range(8):
        u = [
            (
                grid_ref[128 * a + 16 * rows : 128 * a + 16 * rows + 16, 0:128]
                + first_ref[128 * a + 16 * rows : 128 * a + 16 * rows + 16, 0:128],
                grid_ref[128 * a + 16 * rows : 128 * a + 16 * rows + 16, 128:256]
                + first_ref[128 * a + 16 * rows : 128 * a + 16 * rows + 16, 128:256],
            )
            for a in range(8)
        ]

        def add(x, y):
            return x[0] + y[0], x[1] + y[1]

        def sub2(x, y):
            return x[0] - y[0], x[1] - y[1]

        def four(a, b, c, d):
            s, t = add(a, c), sub2(a, c)
            p, q = add(b, d), sub2(b, d)
            mq = (q[1], -q[0])
            return add(s, p), add(t, mq), sub2(s, p), sub2(t, mq)

        even = four(u[0], u[2], u[4], u[6])
        odd = four(u[1], u[3], u[5], u[7])
        o1 = ((odd[1][0] + odd[1][1]) * root, (odd[1][1] - odd[1][0]) * root)
        o2 = (odd[2][1], -odd[2][0])
        o3 = ((odd[3][1] - odd[3][0]) * root, -(odd[3][0] + odd[3][1]) * root)
        odd = (odd[0], o1, o2, o3)
        spectrum = [add(even[k], odd[k]) for k in range(4)] + [sub2(even[k], odd[k]) for k in range(4)]
        at = slice(16 * rows, 16 * rows + 16)
        for k0 in range(8):
            xr, xi = spectrum[k0]
            if k0:
                xr, xi = cmul(xr, xi, tw_ref[k0 - 1, 0, at], tw_ref[k0 - 1, 1, at])
            col = slice(128 * slot_of[k0], 128 * slot_of[k0] + 128)
            for base, value in ((0, xr), (128, xi)):
                hi, lo = split2(value)
                bh_ref[base + 16 * rows : base + 16 * rows + 16, col] = hi
                bl_ref[base + 16 * rows : base + 16 * rows + 16, col] = lo
    low_half = iota((128, 128), 1) < 64
    for k0 in range(4):
        col = slice(256 * k0, 256 * k0 + 256)
        full = dot_nn(matrix_ref[0], bh_ref[:, col]) + dot_nn(matrix_ref[0], bl_ref[:, col]) + dot_nn(matrix_ref[1], bh_ref[:, col])
        power = (full[:128] * full[:128] + full[128:] * full[128:]) * NORM
        pa, pb = power[:, :128], power[:, 128:]
        ra, rb = pltpu.roll(pa, 64, 1), pltpu.roll(pb, 64, 1)
        for side, block in ((0, jnp.where(low_half, pa, rb)), (1, jnp.where(low_half, ra, pb))):
            block = block.reshape(8, 2, 8, 128)
            for cc in range(2):
                piece[cc, k0, side] = block[:, cc]

    pl.semaphore_wait(barrier, 45)

    def remote(source, target, number, device):
        return pltpu.make_async_remote_copy(
            src_ref=source, dst_ref=target, send_sem=sems.at[2 * number], recv_sem=sems.at[2 * number + 1],
            device_id=device, device_id_type=MESH,
        )

    def whole(ref, count, number):
        return remote(ref.at[0:count], ref.at[0:count], number, chip(me_pair, 1 - core))

    pair = remote(piece.at[1 - core], partner, 0, chip(me_pair, 1 - core))
    pair.start()

    def plane_send(buf, slots, number):
        @pl.when(core == 0)
        def _():
            remote(buf, slots.at[me], number, chip(me_pair, 1)).start()

        for step in STEPS:
            remote(buf, slots.at[me], number, chip(neighbour(*step), 1)).start()

    def plane_sum(buf, slots, result, number):
        slots[me] = buf[...]
        whole(slots, 31, number).wait_recv()
        total = slots[0]
        for index in range(1, 32):
            total = total + slots[index]
        result[...] = total

    def column_send(buf, slots, number):
        for step in far_first:
            for to_core in range(2):
                remote(buf, slots.at[z], number, column(step, to_core)).start()
        remote(buf, slots.at[z], number, chip(me_pair, 0)).start()

    def column_sum(buf, slots, number):
        @pl.when(core == 0)
        def _():
            whole(slots, 8, number).wait_recv()

        @pl.when(core == 1)
        def _():
            slots[z] = buf[...]
            whole(slots, 7, number).wait_recv()

        total = slots[0]
        for index in range(1, 8):
            total = total + slots[index]
        return total

    def plane_sent(slots, number):
        @pl.when(core == 0)
        def _():
            whole(slots, 16, number).wait_send()

        @pl.when(core == 1)
        def _():
            whole(slots, 15, number).wait_send()

    plane_send(counts, counts_in, 2)
    pair.wait_recv()
    for k0 in range(4):
        for side in range(2):
            for q in range(8):
                summed[side * 8 + q, k0] = piece[core, k0, side, q] + partner[k0, side, q]
    for step in STEPS:
        peer = neighbour(*step)
        remote(summed.at[peer], landed.at[me_pair], 1, chip(peer, core)).start()
    landed[me_pair] = summed[me_pair]

    @pl.when(core == 1)
    def _():
        plane_sum(counts, counts_in, counts_plane, 2)
        column_send(counts_plane, counts_z, 3)

    whole(landed, 15, 1).wait_recv()
    total = landed[0]
    for index in range(1, 16):
        total = total + landed[index]
    for k0 in range(4):
        for sub in range(8):
            at = slice(128 * (8 * k0 + sub), 128 * (8 * k0 + sub) + 128)
            hit = hit_ref[:, at]
            value = total[k0][sub : sub + 1]
            p0 = value.astype(BF16).astype(F32)
            p1 = (value - p0).astype(BF16).astype(F32)
            left[0:4, at] = hit * p0
            left[4:8, at] = hit * p1
            left[8:12, at] = hit * (value - p0 - p1)
            left[12:16, at] = jnp.zeros((4, 128), F32)
    got = dot_nt(left[...].astype(BF16), onehot[...])
    totals[...] = got[0:4] + got[4:8] + got[8:12]
    plane_send(totals, totals_in, 4)
    for k0 in range(8):
        half = (k0 // 4) * 64
        power_ref[pl.ds(k0, 8, stride=8), :] = total[k0 % 4][:, half : half + 64]
    all_counts = column_sum(counts_plane, counts_z, 3)

    @pl.when(core == 1)
    def _():
        plane_sum(totals, totals_in, totals_plane, 4)
        column_send(totals_plane, totals_z, 5)

    pair.wait_send()
    whole(landed, 15, 1).wait_send()
    plane_sent(counts_in, 2)
    plane_sent(totals_in, 4)

    @pl.when(core == 1)
    def _():
        whole(counts_in, 15, 3).wait_send()

    spectrum_ref[...] = column_sum(totals_plane, totals_z, 5) / all_counts

    @pl.when(core == 1)
    def _():
        whole(totals_in, 15, 5).wait_send()


def tail_call(*args):
    small = (4, 128)
    return pl.pallas_call(
        tail_kernel,
        out_shape=(jax.ShapeDtypeStruct((64, 64), F32), jax.ShapeDtypeStruct((4, 128), F32)),
        in_specs=[VMEM_SPEC] * 9,
        out_specs=(VMEM_SPEC,) * 2,
        scratch_shapes=[
            pltpu.VMEM((1040, 256), F32),
            pltpu.VMEM((GROUP, 256, 256), BF16),
            pltpu.VMEM((GROUP, 160, 256), BF16),
            pltpu.VMEM((GROUP, 256, 256), BF16),
            pltpu.VMEM((GROUP, 160, 256), BF16),
            pltpu.VMEM((GROUP, 2, 8, 128), F32),
            pltpu.VMEM((256, 1024), BF16),
            pltpu.VMEM((256, 1024), BF16),
            pltpu.VMEM((16, 4096), F32),
            pltpu.VMEM((2, 4, 2, 8, 8, 128), F32),
            pltpu.VMEM((4, 2, 8, 8, 128), F32),
            pltpu.VMEM((16, 4, 8, 128), F32),
            pltpu.VMEM((16, 4, 8, 128), F32),
            pltpu.VMEM((32,) + small, F32),
            pltpu.VMEM((8,) + small, F32),
            pltpu.VMEM(small, F32),
            pltpu.VMEM(small, F32),
            pltpu.VMEM((32,) + small, F32),
            pltpu.VMEM((8,) + small, F32),
            pltpu.VMEM(small, F32),
            pltpu.SemaphoreType.DMA((12,)),
        ],
        compiler_params=pltpu.CompilerParams(
            collective_id=1, has_side_effects=True, vmem_limit_bytes=LIMIT
        ),
    )(*args)


def store_kernel(power_ref, spectrum_ref, power_out, spectrum_out, sems):
    first = pltpu.make_async_copy(power_ref, power_out, sems.at[0])
    second = pltpu.make_async_copy(spectrum_ref, spectrum_out, sems.at[1])
    first.start()
    second.start()
    first.wait()
    second.wait()


def store_call(power, spectrum):
    return pl.pallas_call(
        store_kernel,
        out_shape=(jax.ShapeDtypeStruct((64, 64), F32), jax.ShapeDtypeStruct((4, 128), F32)),
        in_specs=[VMEM_SPEC] * 2,
        out_specs=(pl.BlockSpec(memory_space=pltpu.HBM),) * 2,
        scratch_shapes=[pltpu.SemaphoreType.DMA((2,))],
        compiler_params=pltpu.CompilerParams(vmem_limit_bytes=LIMIT),
    )(power, spectrum)


def per_device(visibility, tile_of, u_within, v_cell, kernel_index, kernel, live_count, bin_map):
    merged, kernel_rows, used, phase, matrix, twiddle, onehot, hit, counts = gather_call(
        live_count.T,
        visibility,
        tile_of.transpose(0, 2, 1),
        u_within,
        v_cell,
        kernel_index,
        kernel.T,
        bin_map,
    )
    grid = grid_call(merged, used, phase, kernel_rows)
    power, spectrum = tail_call(grid, merged, phase, kernel_rows, matrix, twiddle, onehot, hit, counts)
    power, spectrum = store_call(power, spectrum)
    return power, spectrum.reshape(NBINS)


def solution(mesh):
    return jax.shard_map(
        per_device,
        mesh=mesh,
        in_specs=(
            P(None, "freq", "base"),
            P("freq", "base", None),
            P("freq", "base"),
            P("freq", "base"),
            P(None, "freq", "base"),
            P(),
            P("freq", "base"),
            P("base", None),
        ),
        out_specs=(P("freq", "base"), P()),
        check_vma=False,
    )
```
